32 devices in a mesh: dp: 1 (over z), tp: 4 (over y), sp: 8 (over x, core).
Axes of the slice: x: 4, y: 4, z: 1, core: 2. Of those that a mesh axis runs over, the one named last changes fastest.
The devices are a block of a 4x4x8 slice.
Arguments:
- hidden: bfloat16 [128, 5120], P('dp')
- seq_lens: int32 [128], P('dp')
- rope_cos: float32 [128, 64], P('dp')
- rope_sin: float32 [128, 64], P('dp')
- k_cache: bfloat16 [128, 512, 8, 128], P('dp', 'sp', 'tp')
- v_cache: bfloat16 [128, 512, 8, 128], P('dp', 'sp', 'tp')
- norm_gain: bfloat16 [5120], replicated
- w_qkv: bfloat16 [5120, 8, 1280], P(None, 'tp')
- b_qkv: bfloat16 [8, 1280], P('tp')
- sink_logits: float32 [64], P('tp')
- w_o: bfloat16 [8192, 5120], P('tp')
- b_o: bfloat16 [5120], replicated
Outputs:
- output 1: bfloat16 [128, 5120], P('dp')
- output 2: bfloat16 [128, 512, 8, 128], P('dp', 'sp', 'tp')
- output 3: bfloat16 [128, 512, 8, 128], P('dp', 'sp', 'tp')
All inputs are finite; a program needn't handle non-finite values.
Results may differ from the reference program's by a relative error of at most 0.00575541.
Values sent between devices are 32-bit elements.
A program may use at most 768 MiB of HBM per device.

```python
import math
import jax
import jax.numpy as jnp
from jax import lax

D_MODEL = 5120
Q_HEADS = 64
KV_HEADS = 8
HEAD_DIM = 128
SEQ_COUNT = 128
CTX_LEN = 512
ROPE_BASE = 150000
NORM_EPS = 1e-5


def rotate_half(heads_in, cos_part, sin_part):
    half_dim = heads_in.shape[-1] // 2
    first_half = heads_in[..., :half_dim]
    second_half = heads_in[..., half_dim:]
    return jnp.concatenate([first_half * cos_part - second_half * sin_part, second_half * cos_part + first_half * sin_part], axis=-1)


def setup_inputs(seed: int = 0, part: int = 0) -> dict:
    shared_keys = jax.random.split(jax.random.key(seed), 6)
    part_keys = jax.random.split(jax.random.fold_in(jax.random.key(seed + 1), part), 5)
    group_size = Q_HEADS // KV_HEADS
    qkv_width = (group_size + 2) * HEAD_DIM
    key_scale = math.sqrt(math.log(CTX_LEN) / 2.0)
    sink_center = math.log(CTX_LEN / 2.0) + 0.6 * key_scale * key_scale - 1.0
    hidden = (0.5 * jax.random.normal(part_keys[0], (SEQ_COUNT, D_MODEL), jnp.float32)).astype(jnp.bfloat16)
    drawn_lens = jax.random.randint(part_keys[1], (SEQ_COUNT,), 0, CTX_LEN, jnp.int32)
    full_row = jax.random.randint(part_keys[2], (), 0, SEQ_COUNT, jnp.int32)
    seq_lens = jnp.where(jnp.arange(SEQ_COUNT) == full_row, CTX_LEN - 1, drawn_lens).astype(jnp.int32)
    inv_freq = jnp.exp(jnp.arange(HEAD_DIM // 2, dtype=jnp.float32) * (-2.0 * math.log(ROPE_BASE) / HEAD_DIM))
    angles = seq_lens.astype(jnp.float32)[:, None] * inv_freq[None, :]
    cache_shape = (SEQ_COUNT, CTX_LEN, KV_HEADS, HEAD_DIM)
    k_cache = (key_scale * jax.random.normal(part_keys[3], cache_shape, jnp.float32)).astype(jnp.bfloat16)
    v_cache = jax.random.normal(part_keys[4], cache_shape, jnp.float32).astype(jnp.bfloat16)
    norm_gain = (1.0 + 0.2 * jax.random.normal(shared_keys[0], (D_MODEL,), jnp.float32)).astype(jnp.bfloat16)
    w_qkv = (D_MODEL ** -0.5 * jax.random.normal(shared_keys[1], (D_MODEL, KV_HEADS, qkv_width), jnp.float32)).astype(jnp.bfloat16)
    b_qkv = (0.5 * jax.random.normal(shared_keys[2], (KV_HEADS, qkv_width), jnp.float32)).astype(jnp.bfloat16)
    sink_logits = sink_center + jax.random.normal(shared_keys[3], (Q_HEADS,), jnp.float32)
    w_o = (4.0 * (Q_HEADS * HEAD_DIM) ** -0.5 * jax.random.normal(shared_keys[4], (Q_HEADS * HEAD_DIM, D_MODEL), jnp.float32)).astype(jnp.bfloat16)
    b_o = (0.3 * jax.random.normal(shared_keys[5], (D_MODEL,), jnp.float32)).astype(jnp.bfloat16)
    return {"hidden": hidden, "seq_lens": seq_lens, "rope_cos": jnp.cos(angles), "rope_sin": jnp.sin(angles), "k_cache": k_cache, "v_cache": v_cache, "norm_gain": norm_gain, "w_qkv": w_qkv, "b_qkv": b_qkv, "sink_logits": sink_logits, "w_o": w_o, "b_o": b_o}


def reference(hidden, seq_lens, rope_cos, rope_sin, k_cache, v_cache, norm_gain, w_qkv, b_qkv, sink_logits, w_o, b_o):
    group_size = Q_HEADS // KV_HEADS
    x_wide = hidden.astype(jnp.float32)
    inv_rms = lax.rsqrt(jnp.mean(x_wide * x_wide, axis=-1, keepdims=True) + NORM_EPS)
    normed = (x_wide * inv_rms * norm_gain.astype(jnp.float32)).astype(jnp.bfloat16)
    qkv_all = jnp.dot(normed, w_qkv.reshape(D_MODEL, KV_HEADS * (group_size + 2) * HEAD_DIM), preferred_element_type=jnp.float32)
    qkv_all = (qkv_all + b_qkv.astype(jnp.float32).reshape(-1)).reshape(SEQ_COUNT, KV_HEADS, group_size + 2, HEAD_DIM)
    q_rot = rotate_half(qkv_all[:, :, :group_size], rope_cos[:, None, None, :], rope_sin[:, None, None, :]).astype(jnp.bfloat16)
    k_new = rotate_half(qkv_all[:, :, group_size], rope_cos[:, None, :], rope_sin[:, None, :]).astype(jnp.bfloat16)
    v_new = qkv_all[:, :, group_size + 1].astype(jnp.bfloat16)
    positions = jnp.arange(CTX_LEN)
    is_new = (positions[None, :] == seq_lens[:, None])[:, :, None, None]
    k_out = jnp.where(is_new, k_new[:, None], k_cache)
    v_out = jnp.where(is_new, v_new[:, None], v_cache)
    sink_kg = sink_logits.reshape(KV_HEADS, group_size)
    logit_scale = HEAD_DIM ** -0.5

    def one_sequence(per_seq):
        q_seq, k_seq, v_seq, len_seq = per_seq
        logits = jnp.einsum("kgd,lkd->kgl", q_seq.astype(jnp.float32), k_seq.astype(jnp.float32)) * logit_scale
        logits = jnp.where((positions <= len_seq)[None, None, :], logits, -jnp.inf)
        row_max = jnp.maximum(jnp.max(logits, axis=-1), sink_kg)
        weights = jnp.exp(logits - row_max[..., None])
        denominator = jnp.sum(weights, axis=-1) + jnp.exp(sink_kg - row_max)
        weighted = jnp.einsum("kgl,lkd->kgd", weights.astype(jnp.bfloat16).astype(jnp.float32), v_seq.astype(jnp.float32))
        return weighted / denominator[..., None]

    head_out = lax.map(one_sequence, (q_rot, k_out, v_out, seq_lens))
    attn_out = jnp.dot(head_out.astype(jnp.bfloat16).reshape(SEQ_COUNT, Q_HEADS * HEAD_DIM), w_o, preferred_element_type=jnp.float32)
    out_hidden = (x_wide + attn_out + b_o.astype(jnp.float32)).astype(jnp.bfloat16)
    return out_hidden, k_out, v_out
```

```python
import functools

import jax
import jax.numpy as jnp
from jax import lax
from jax.experimental import pallas as pl
from jax.experimental.pallas import tpu as pltpu
from jax.sharding import PartitionSpec as P

NORM_EPS = 1e-5
MESH = pl.DeviceIdType.MESH
LANES = 128
HALF = LANES // 2
SUBS = 2
CORES = 2
RING = 4


def lane_column(tile, index):
    return tile[:, index : index + 1]


def merge_parts(parts, seqs):
    stats = [part[seqs] for part in parts]
    top = functools.reduce(jnp.maximum, stats)
    scales = [jnp.exp(stat - top) for stat in stats]
    total = sum(pltpu.roll(scale, HALF, 1) * stat for scale, stat in zip(scales, stats))
    return top, total, scales


def merge_into(dst, parts, seqs):
    top, total, scales = merge_parts(parts, seqs)
    for i in range(seqs):
        dst[i] = sum(lane_column(scale, i) * part[i] for scale, part in zip(scales, parts))
    lane = lax.broadcasted_iota(jnp.int32, top.shape, 1)
    dst[seqs] = jnp.where(lane < HALF, top, total)


def combine_kernel(
    seqs, p_ref, sink_ref, x_hbm, bo_ref, wo_hbm, out_ref,
    ra, cb, rl, rm, rd, own_o, other_o, wbuf, xbuf, z, yrl, ym, yrm, yrd, g, gp,
    w_sem, x_sem, a_send, a_recv, b_send, rl_recv, rm_recv, rd_recv, o_send, o_recv,
    d_send, yrl_recv, yrm_recv, yrd_recv, g_send, g_recv, gp_send, gp_recv,
):
    y = lax.axis_index("tp")
    sp = lax.axis_index("sp")
    x = sp // CORES
    c = sp % CORES
    step = 1 - 2 * c
    xn, xp, xo = (x + step + RING) % RING, (x - step + RING) % RING, (x + 2) % RING
    yn, yp, yo = (y + step + RING) % RING, (y - step + RING) % RING, (y + 2) % RING
    partner = {"sp": x * CORES + 1 - c}
    to_xn, to_xp = {"sp": xn * CORES + c}, {"sp": xp * CORES + c}
    to_yn, to_yp = {"tp": yn}, {"tp": yp}

    rows_half = wo_hbm.shape[0] // 2
    cols_core = wo_hbm.shape[1] // CORES
    cols_sub = cols_core // SUBS
    heads = p_ref.shape[4]
    block_rows = z.shape[2]

    w_copies = []
    for k in range(2):
        rows = (c if k == 0 else 1 - c) * rows_half
        copy = pltpu.make_async_copy(
            wo_hbm.at[pl.ds(pl.multiple_of(rows, LANES), rows_half), pl.ds(pl.multiple_of(c * cols_core, LANES), cols_core)],
            wbuf.at[k], w_sem.at[k])
        copy.start()
        w_copies.append(copy)
    row0 = pl.multiple_of((x * RING + y) * block_rows, block_rows)
    x_copy = pltpu.make_async_copy(
        x_hbm.at[pl.ds(row0, block_rows), pl.ds(pl.multiple_of(c * cols_core, LANES), cols_core)], xbuf, x_sem.at[0])
    x_copy.start()

    barrier = pltpu.get_barrier_semaphore()
    for where in (partner, to_xn, to_xp, to_yn, to_yp):
        pl.semaphore_signal(barrier, inc=1, device_id=where, device_id_type=MESH)
    pl.semaphore_wait(barrier, 5)

    sends = []

    def send(src, dst, send_sem, recv_sem, where):
        copy = pltpu.make_async_remote_copy(
            src_ref=src, dst_ref=dst, send_sem=send_sem, recv_sem=recv_sem, device_id=where, device_id_type=MESH)
        copy.start()
        sends.append(copy)

    def arrived(dst, recv_sem):
        pltpu.make_async_remote_copy(
            src_ref=dst, dst_ref=dst, send_sem=recv_sem, recv_sem=recv_sem, device_id=partner, device_id_type=MESH).wait_recv()

    for k, b in enumerate((xo, xp, xn, x)):
        for s in range(SUBS):
            send(p_ref.at[b, s, 1 - c], ra.at[b, s], a_send.at[k, s], a_recv.at[b, s], partner)

    for s in range(SUBS):
        arrived(ra.at[xo, s], a_recv.at[xo, s])
        merge_into(cb.at[0, s], (p_ref.at[xo, s, c], ra.at[xo, s]), seqs)
        send(cb.at[0, s], rl.at[s], b_send.at[0, s], rl_recv.at[s], to_xn)
    for s in range(SUBS):
        arrived(ra.at[xp, s], a_recv.at[xp, s])
        merge_into(cb.at[1, s], (p_ref.at[xp, s, c], ra.at[xp, s]), seqs)
        send(cb.at[1, s], rd.at[s], b_send.at[1, s], rd_recv.at[s], to_xp)
    for s in range(SUBS):
        arrived(ra.at[xn, s], a_recv.at[xn, s])
        arrived(rl.at[s], rl_recv.at[s])
        merge_into(cb.at[2, s], (p_ref.at[xn, s, c], ra.at[xn, s], rl.at[s]), seqs)
        send(cb.at[2, s], rm.at[s], b_send.at[2, s], rm_recv.at[s], to_xn)
    for s in range(SUBS):
        arrived(ra.at[x, s], a_recv.at[x, s])
        merge_into(cb.at[3, s], (p_ref.at[x, s, c], ra.at[x, s]), seqs)
    sink = sink_ref[pl.ds(pl.multiple_of(c * heads, heads), heads), :]
    for s in range(SUBS):
        arrived(rd.at[s], rd_recv.at[s])
        arrived(rm.at[s], rm_recv.at[s])
        parts = (cb.at[3, s], rd.at[s], rm.at[s])
        top, total, scales = merge_parts(parts, seqs)
        inverse = 1.0 / (pltpu.roll(total, HALF, 1) + jnp.exp(sink - top))
        for i in range(seqs):
            summed = sum(lane_column(scale, i) * part[i] for scale, part in zip(scales, parts))
            head_out = summed * lane_column(inverse, i)
            own_o[s, pl.ds(i * heads, heads), :] = head_out.astype(jnp.bfloat16).astype(jnp.float32)
        send(own_o.at[s], other_o.at[s], o_send.at[s], o_recv.at[s], partner)

    def head_rows(ref):
        columns = []
        for h in range(heads):
            columns.append(jnp.concatenate(
                [ref[s, pl.ds(h, seqs, stride=heads), :] for s in range(SUBS)], axis=0).astype(jnp.bfloat16))
        return jnp.concatenate(columns, axis=1)

    own_rows = head_rows(own_o)
    w_copies[0].wait()
    for q in range(SUBS):
        part = jnp.dot(own_rows, wbuf[0, :, pl.ds(q * cols_sub, cols_sub)], preferred_element_type=jnp.float32)
        for r in range(RING):
            z[q, r] = part[r * block_rows : (r + 1) * block_rows]
    for s in range(SUBS):
        arrived(other_o.at[s], o_recv.at[s])
    other_rows = head_rows(other_o)
    w_copies[1].wait()
    for q in range(SUBS):
        part = jnp.dot(other_rows, wbuf[1, :, pl.ds(q * cols_sub, cols_sub)], preferred_element_type=jnp.float32)
        for r in range(RING):
            z[q, r] += part[r * block_rows : (r + 1) * block_rows]
        send(z.at[q, yo], yrl.at[q], d_send.at[0, q], yrl_recv.at[q], to_yn)
        send(z.at[q, yp], yrd.at[q], d_send.at[1, q], yrd_recv.at[q], to_yp)
    for q in range(SUBS):
        arrived(yrl.at[q], yrl_recv.at[q])
        ym[q] = z[q, yn] + yrl[q]
        send(ym.at[q], yrm.at[q], d_send.at[2, q], yrm_recv.at[q], to_yn)
    x_copy.wait()

    def store(q, xx, yy, core, value):
        rows = pl.ds(pl.multiple_of((xx * RING + yy) * block_rows, block_rows), block_rows)
        cols = pl.ds(pl.multiple_of(core * cols_core + q * cols_sub, LANES), cols_sub)
        out_ref[rows, cols] = value.astype(jnp.bfloat16)

    def slot(q, first, second):
        return (first, second) if q == 0 else (second, first)

    ahead = ((to_xn, to_xp), (to_yn, to_yp))
    first_now, first_n, first_p, first_o = (x, y), (xn, yn), (xp, yp), (xo, yo)

    def push(q, first, second, kind, where):
        xx, yy = slot(q, first, second)
        send(g.at[q, xx, yy], g.at[q, xx, yy], g_send.at[q, xx, yy, kind], g_recv.at[q, xx, yy], where)

    def share(q, first, second):
        xx, yy = slot(q, first, second)
        send(g.at[q, xx, yy], gp.at[q, xx, yy], gp_send.at[q, xx, yy], gp_recv.at[q, xx, yy], partner)

    def receive(q, first, second):
        xx, yy = slot(q, first, second)
        arrived(g.at[q, xx, yy], g_recv.at[q, xx, yy])

    def keep(q, first, second):
        xx, yy = slot(q, first, second)
        store(q, xx, yy, c, g[q, xx, yy])

    for q in range(SUBS):
        arrived(yrd.at[q], yrd_recv.at[q])
        arrived(yrm.at[q], yrm_recv.at[q])
        cols = pl.ds(q * cols_sub, cols_sub)
        bias = bo_ref[:, pl.ds(pl.multiple_of(c * cols_core + q * cols_sub, LANES), cols_sub)]
        summed = z[q, y] + yrd[q] + yrm[q]
        final = xbuf[:, cols].astype(jnp.float32) + summed + bias.astype(jnp.float32)
        g[q, x, y] = final.astype(jnp.bfloat16).astype(jnp.float32)
        for axis in (q, 1 - q):
            for kind in range(2):
                push(q, first_now[q], first_now[1 - q], 2 * (axis != q) + kind, ahead[axis][kind])
        share(q, first_now[q], first_now[1 - q])

    def spread(q, first, forward):
        other = 1 - q
        receive(q, first, first_now[other])
        if forward:
            push(q, first, first_now[other], 0, ahead[q][0])
        for kind in range(2):
            push(q, first, first_now[other], 2 + kind, ahead[other][kind])
        share(q, first, first_now[other])
        keep(q, first, first_now[other])

    def settle(q, first, second, forward):
        receive(q, first, second)
        if forward:
            push(q, first, second, 2, ahead[1 - q][0])
        share(q, first, second)
        keep(q, first, second)

    both = range(SUBS)
    for q in both:
        spread(q, first_p[q], True)
    for q in both:
        spread(q, first_n[q], False)
    for q in both:
        keep(q, first_now[q], first_now[1 - q])
    for q in both:
        settle(q, first_now[q], first_p[1 - q], True)
    for q in both:
        settle(q, first_now[q], first_n[1 - q], False)
    for q in both:
        spread(q, first_o[q], False)
    for first in (first_p, first_n):
        for q in both:
            settle(q, first[q], first_p[1 - q], True)
        for q in both:
            settle(q, first[q], first_n[1 - q], False)
    for q in both:
        settle(q, first_now[q], first_o[1 - q], False)
    for q in both:
        settle(q, first_o[q], first_p[1 - q], True)
    for q in both:
        settle(q, first_o[q], first_n[1 - q], False)
    for first in (first_p, first_n, first_o):
        for q in both:
            settle(q, first[q], first_o[1 - q], False)
    orders = [first_now, first_p, first_n, first_o]
    for xi in range(RING):
        for yi in range(RING):
            for q in both:
                xx, yy = slot(q, orders[xi][q], orders[yi][1 - q])
                arrived(gp.at[q, xx, yy], gp_recv.at[q, xx, yy])
                store(q, xx, yy, 1 - c, gp[q, xx, yy])
    for copy in sends:
        copy.wait_send()


def combine(p, sinks, hidden, b_o, w_o):
    seqs = p.shape[3] - 1
    heads = p.shape[4]
    num_seqs, d_model = hidden.shape
    cols_core = d_model // CORES
    cols_sub = cols_core // SUBS
    block_rows = num_seqs // (RING * RING)
    part = (seqs + 1, heads, LANES)
    f32, bf16 = jnp.float32, jnp.bfloat16
    dma = pltpu.SemaphoreType.DMA
    vmem = pl.BlockSpec(memory_space=pltpu.VMEM)
    hbm = pl.BlockSpec(memory_space=pl.ANY)
    chunk = (block_rows, cols_sub)
    return pl.pallas_call(
        functools.partial(combine_kernel, seqs),
        out_shape=jax.ShapeDtypeStruct((num_seqs, d_model), bf16),
        in_specs=[vmem, vmem, hbm, vmem, hbm],
        out_specs=vmem,
        scratch_shapes=[
            pltpu.VMEM((RING, SUBS) + part, f32),
            pltpu.VMEM((RING, SUBS) + part, f32),
            pltpu.VMEM((SUBS,) + part, f32),
            pltpu.VMEM((SUBS,) + part, f32),
            pltpu.VMEM((SUBS,) + part, f32),
            pltpu.VMEM((SUBS, seqs * heads, LANES), f32),
            pltpu.VMEM((SUBS, seqs * heads, LANES), f32),
            pltpu.VMEM((2, w_o.shape[0] // 2, cols_core), bf16),
            pltpu.VMEM((block_rows, cols_core), bf16),
            pltpu.VMEM((SUBS, RING) + chunk, f32),
            pltpu.VMEM((SUBS,) + chunk, f32),
            pltpu.VMEM((SUBS,) + chunk, f32),
            pltpu.VMEM((SUBS,) + chunk, f32),
            pltpu.VMEM((SUBS,) + chunk, f32),
            pltpu.VMEM((SUBS, RING, RING) + chunk, f32),
            pltpu.VMEM((SUBS, RING, RING) + chunk, f32),
            dma((2,)), dma((1,)), dma((RING, SUBS)), dma((RING, SUBS)), dma((3, SUBS)),
            dma((SUBS,)), dma((SUBS,)), dma((SUBS,)), dma((SUBS,)), dma((SUBS,)),
            dma((3, SUBS)), dma((SUBS,)), dma((SUBS,)), dma((SUBS,)),
            dma((SUBS, RING, RING, 4)), dma((SUBS, RING, RING)), dma((SUBS, RING, RING)), dma((SUBS, RING, RING)),
        ],
        compiler_params=pltpu.CompilerParams(collective_id=0, has_side_effects=True, vmem_limit_bytes=48 * 2**20),
        cost_estimate=pl.CostEstimate(flops=2 * num_seqs // RING * w_o.shape[0] * cols_core, bytes_accessed=30 * 2**20, transcendentals=0),
        name="combine",
    )(p, sinks, hidden, b_o, w_o)


def rotate_half(heads_in, cos_part, sin_part):
    half_dim = heads_in.shape[-1] // 2
    first_half = heads_in[..., :half_dim]
    second_half = heads_in[..., half_dim:]
    return jnp.concatenate([first_half * cos_part - second_half * sin_part, second_half * cos_part + first_half * sin_part], axis=-1)


def local_partials(hidden, seq_lens, rope_cos, rope_sin, k_cache, v_cache, norm_gain, w_qkv, b_qkv, sink_logits):
    num_seqs, ctx_local, kv_local, head_dim = k_cache.shape
    group_size = w_qkv.shape[2] // head_dim - 2
    x_wide = hidden.astype(jnp.float32)
    inv_rms = lax.rsqrt(jnp.mean(x_wide * x_wide, axis=-1, keepdims=True) + NORM_EPS)
    normed = (x_wide * inv_rms * norm_gain.astype(jnp.float32)).astype(jnp.bfloat16)
    qkv_all = jnp.einsum("bd,dkc->bkc", normed, w_qkv, preferred_element_type=jnp.float32) + b_qkv.astype(jnp.float32)
    qkv_all = qkv_all.reshape(num_seqs, kv_local, group_size + 2, head_dim)
    q_rot = rotate_half(qkv_all[:, :, :group_size], rope_cos[:, None, None, :], rope_sin[:, None, None, :]).astype(jnp.bfloat16)
    k_new = rotate_half(qkv_all[:, :, group_size], rope_cos[:, None, :], rope_sin[:, None, :]).astype(jnp.bfloat16)
    v_new = qkv_all[:, :, group_size + 1].astype(jnp.bfloat16)
    positions = lax.axis_index("sp") * ctx_local + jnp.arange(ctx_local)
    is_new = (positions[None, :] == seq_lens[:, None])[:, :, None, None]
    k_out = jnp.where(is_new, k_new[:, None], k_cache)
    v_out = jnp.where(is_new, v_new[:, None], v_cache)
    logits = jnp.einsum("bkgd,blkd->bkgl", q_rot, k_out, preferred_element_type=jnp.float32) * head_dim ** -0.5
    logits = jnp.where((positions[None, :] <= seq_lens[:, None])[:, None, None, :], logits, -jnp.inf)
    row_max = jnp.maximum(jnp.max(logits, axis=-1), sink_logits.reshape(kv_local, group_size))
    weights = jnp.exp(logits - row_max[..., None])
    row_sum = jnp.sum(weights, axis=-1)
    weighted = jnp.einsum("bkgl,blkd->bkgd", weights.astype(jnp.bfloat16), v_out, preferred_element_type=jnp.float32)
    seqs = num_seqs // (RING * SUBS)
    numer = weighted.reshape(RING, SUBS, seqs, kv_local, group_size, head_dim).transpose(0, 1, 3, 2, 4, 5)
    stat = lambda a: a.reshape(RING, SUBS, seqs, kv_local, group_size).transpose(0, 1, 3, 4, 2)
    pad = jnp.zeros((RING, SUBS, kv_local, group_size, HALF - seqs), jnp.float32)
    stats = jnp.concatenate([stat(row_max), pad, stat(row_sum), pad], axis=-1)
    return jnp.concatenate([numer, stats[:, :, :, None]], axis=3), k_out, v_out


def solution(mesh):
    cache_spec = P("dp", "sp", "tp", None)

    def block_step(hidden, seq_lens, rope_cos, rope_sin, k_cache, v_cache, norm_gain, w_qkv, b_qkv, sink_logits, w_o, b_o):
        packed, k_out, v_out = local_partials(hidden, seq_lens, rope_cos, rope_sin, k_cache, v_cache, norm_gain, w_qkv, b_qkv, sink_logits)
        sinks = jnp.broadcast_to(sink_logits[:, None], (sink_logits.shape[0], LANES))
        out_hidden = combine(packed, sinks, hidden, b_o[None, :], w_o)
        return out_hidden, k_out, v_out

    return jax.shard_map(block_step, mesh=mesh, in_specs=(P("dp", None), P("dp"), P("dp", None), P("dp", None), cache_spec, cache_spec, P(None), P(None, "tp", None), P("tp", None), P("tp"), P("tp", None), P(None)), out_specs=(P("dp", None), cache_spec, cache_spec), check_vma=False)
```

```python
import functools

import jax
import jax.numpy as jnp
from jax import lax
from jax.experimental import pallas as pl
from jax.experimental.pallas import tpu as pltpu
from jax.sharding import PartitionSpec as P

NORM_EPS = 1e-5
MESH = pl.DeviceIdType.MESH
LANES = 128
HALF = LANES // 2
SUBS = 2
CORES = 2
RING = 4


def lane_column(tile, index):
    return tile[:, index : index + 1]


def merge_parts(parts, seqs):
    stats = [part[seqs] for part in parts]
    top = functools.reduce(jnp.maximum, stats)
    scales = [jnp.exp(stat - top) for stat in stats]
    total = sum(pltpu.roll(scale, HALF, 1) * stat for scale, stat in zip(scales, stats))
    return top, total, scales


def merge_into(dst, parts, seqs):
    top, total, scales = merge_parts(parts, seqs)
    for i in range(seqs):
        dst[i] = sum(lane_column(scale, i) * part[i] for scale, part in zip(scales, parts))
    lane = lax.broadcasted_iota(jnp.int32, top.shape, 1)
    dst[seqs] = jnp.where(lane < HALF, top, total)


def combine_kernel(
    seqs, p_ref, sink_ref, x_hbm, bo_ref, wo_hbm, out_ref,
    ra, cb, rl, rm, rd, own_o, other_o, wbuf, xbuf, z, yrl, ym, yrm, yrd, g, gp,
    w_sem, x_sem, a_send, a_recv, b_send, rl_recv, rm_recv, rd_recv, o_send, o_recv,
    d_send, yrl_recv, yrm_recv, yrd_recv, g_send, g_recv, gp_send, gp_recv,
):
    y = lax.axis_index("tp")
    sp = lax.axis_index("sp")
    x = sp // CORES
    c = sp % CORES
    step = 1 - 2 * c
    xn, xp, xo = (x + step + RING) % RING, (x - step + RING) % RING, (x + 2) % RING
    yn, yp, yo = (y + step + RING) % RING, (y - step + RING) % RING, (y + 2) % RING
    partner = {"sp": x * CORES + 1 - c}
    to_xn, to_xp = {"sp": xn * CORES + c}, {"sp": xp * CORES + c}
    to_yn, to_yp = {"tp": yn}, {"tp": yp}

    rows_half = wo_hbm.shape[0] // 2
    cols_core = wo_hbm.shape[1] // CORES
    cols_sub = cols_core // SUBS
    heads = p_ref.shape[4]
    block_rows = z.shape[2]

    w_copies = []
    for k in range(2):
        rows = (c if k == 0 else 1 - c) * rows_half
        copy = pltpu.make_async_copy(
            wo_hbm.at[pl.ds(pl.multiple_of(rows, LANES), rows_half), pl.ds(pl.multiple_of(c * cols_core, LANES), cols_core)],
            wbuf.at[k], w_sem.at[k])
        copy.start()
        w_copies.append(copy)
    row0 = pl.multiple_of((x * RING + y) * block_rows, block_rows)
    x_copy = pltpu.make_async_copy(
        x_hbm.at[pl.ds(row0, block_rows), pl.ds(pl.multiple_of(c * cols_core, LANES), cols_core)], xbuf, x_sem.at[0])
    x_copy.start()

    barrier = pltpu.get_barrier_semaphore()
    for where in (partner, to_xn, to_xp, to_yn, to_yp):
        pl.semaphore_signal(barrier, inc=1, device_id=where, device_id_type=MESH)
    pl.semaphore_wait(barrier, 5)

    sends = []

    def send(src, dst, send_sem, recv_sem, where):
        copy = pltpu.make_async_remote_copy(
            src_ref=src, dst_ref=dst, send_sem=send_sem, recv_sem=recv_sem, device_id=where, device_id_type=MESH)
        copy.start()
        sends.append(copy)

    def arrived(dst, recv_sem):
        pltpu.make_async_remote_copy(
            src_ref=dst, dst_ref=dst, send_sem=recv_sem, recv_sem=recv_sem, device_id=partner, device_id_type=MESH).wait_recv()

    for k, b in enumerate((xo, xp, xn, x)):
        for s in range(SUBS):
            send(p_ref.at[b, s, 1 - c], ra.at[b, s], a_send.at[k, s], a_recv.at[b, s], partner)

    for s in range(SUBS):
        arrived(ra.at[xo, s], a_recv.at[xo, s])
        merge_into(cb.at[0, s], (p_ref.at[xo, s, c], ra.at[xo, s]), seqs)
        send(cb.at[0, s], rl.at[s], b_send.at[0, s], rl_recv.at[s], to_xn)
    for s in range(SUBS):
        arrived(ra.at[xp, s], a_recv.at[xp, s])
        merge_into(cb.at[1, s], (p_ref.at[xp, s, c], ra.at[xp, s]), seqs)
        send(cb.at[1, s], rd.at[s], b_send.at[1, s], rd_recv.at[s], to_xp)
    for s in range(SUBS):
        arrived(ra.at[xn, s], a_recv.at[xn, s])
        arrived(rl.at[s], rl_recv.at[s])
        merge_into(cb.at[2, s], (p_ref.at[xn, s, c], ra.at[xn, s], rl.at[s]), seqs)
        send(cb.at[2, s], rm.at[s], b_send.at[2, s], rm_recv.at[s], to_xn)
    for s in range(SUBS):
        arrived(ra.at[x, s], a_recv.at[x, s])
        merge_into(cb.at[3, s], (p_ref.at[x, s, c], ra.at[x, s]), seqs)
    sink = sink_ref[pl.ds(pl.multiple_of(c * heads, heads), heads), :]
    for s in range(SUBS):
        arrived(rd.at[s], rd_recv.at[s])
        arrived(rm.at[s], rm_recv.at[s])
        parts = (cb.at[3, s], rd.at[s], rm.at[s])
        top, total, scales = merge_parts(parts, seqs)
        inverse = 1.0 / (pltpu.roll(total, HALF, 1) + jnp.exp(sink - top))
        for i in range(seqs):
            summed = sum(lane_column(scale, i) * part[i] for scale, part in zip(scales, parts))
            head_out = summed * lane_column(inverse, i)
            own_o[s, pl.ds(i * heads, heads), :] = head_out.astype(jnp.bfloat16).astype(jnp.float32)
        send(own_o.at[s], other_o.at[s], o_send.at[s], o_recv.at[s], partner)

    def head_rows(ref):
        columns = []
        for h in range(heads):
            columns.append(jnp.concatenate(
                [ref[s, pl.ds(h, seqs, stride=heads), :] for s in range(SUBS)], axis=0).astype(jnp.bfloat16))
        return jnp.concatenate(columns, axis=1)

    own_rows = head_rows(own_o)
    w_copies[0].wait()
    for q in range(SUBS):
        part = jnp.dot(own_rows, wbuf[0, :, pl.ds(q * cols_sub, cols_sub)], preferred_element_type=jnp.float32)
        for r in range(RING):
            z[q, r] = part[r * block_rows : (r + 1) * block_rows]
    for s in range(SUBS):
        arrived(other_o.at[s], o_recv.at[s])
    other_rows = head_rows(other_o)
    w_copies[1].wait()
    for q in range(SUBS):
        part = jnp.dot(other_rows, wbuf[1, :, pl.ds(q * cols_sub, cols_sub)], preferred_element_type=jnp.float32)
        for r in range(RING):
            z[q, r] += part[r * block_rows : (r + 1) * block_rows]
        send(z.at[q, yo], yrl.at[q], d_send.at[0, q], yrl_recv.at[q], to_yn)
        send(z.at[q, yp], yrd.at[q], d_send.at[1, q], yrd_recv.at[q], to_yp)
    for q in range(SUBS):
        arrived(yrl.at[q], yrl_recv.at[q])
        ym[q] = z[q, yn] + yrl[q]
        send(ym.at[q], yrm.at[q], d_send.at[2, q], yrm_recv.at[q], to_yn)
    x_copy.wait()

    def store(q, xx, yy, core, value):
        rows = pl.ds(pl.multiple_of((xx * RING + yy) * block_rows, block_rows), block_rows)
        cols = pl.ds(pl.multiple_of(core * cols_core + q * cols_sub, LANES), cols_sub)
        out_ref[rows, cols] = value.astype(jnp.bfloat16)

    def slot(q, first, second):
        return (first, second) if q == 0 else (second, first)

    ahead = ((to_xn, to_xp), (to_yn, to_yp))
    first_now, first_n, first_p, first_o = (x, y), (xn, yn), (xp, yp), (xo, yo)

    def push(q, first, second, kind, where):
        xx, yy = slot(q, first, second)
        send(g.at[q, xx, yy], g.at[q, xx, yy], g_send.at[q, xx, yy, kind], g_recv.at[q, xx, yy], where)

    def share(q, first, second):
        xx, yy = slot(q, first, second)
        send(g.at[q, xx, yy], gp.at[q, xx, yy], gp_send.at[q, xx, yy], gp_recv.at[q, xx, yy], partner)

    def receive(q, first, second):
        xx, yy = slot(q, first, second)
        arrived(g.at[q, xx, yy], g_recv.at[q, xx, yy])

    def keep(q, first, second):
        xx, yy = slot(q, first, second)
        store(q, xx, yy, c, g[q, xx, yy])

    for q in range(SUBS):
        arrived(yrd.at[q], yrd_recv.at[q])
        arrived(yrm.at[q], yrm_recv.at[q])
        cols = pl.ds(q * cols_sub, cols_sub)
        bias = bo_ref[:, pl.ds(pl.multiple_of(c * cols_core + q * cols_sub, LANES), cols_sub)]
        summed = z[q, y] + yrd[q] + yrm[q]
        final = xbuf[:, cols].astype(jnp.float32) + summed + bias.astype(jnp.float32)
        g[q, x, y] = final.astype(jnp.bfloat16).astype(jnp.float32)
        for axis in (q, 1 - q):
            for kind in range(2):
                push(q, first_now[q], first_now[1 - q], 2 * (axis != q) + kind, ahead[axis][kind])
        share(q, first_now[q], first_now[1 - q])

    def spread(q, first, forward):
        other = 1 - q
        receive(q, first, first_now[other])
        if forward:
            push(q, first, first_now[other], 0, ahead[q][0])
        for kind in range(2):
            push(q, first, first_now[other], 2 + kind, ahead[other][kind])
        share(q, first, first_now[other])
        keep(q, first, first_now[other])

    def settle(q, first, second, forward):
        receive(q, first, second)
        if forward:
            push(q, first, second, 2, ahead[1 - q][0])
        share(q, first, second)
        keep(q, first, second)

    both = range(SUBS)
    for q in both:
        spread(q, first_p[q], True)
    for q in both:
        spread(q, first_n[q], False)
    for q in both:
        keep(q, first_now[q], first_now[1 - q])
    for q in both:
        settle(q, first_now[q], first_p[1 - q], True)
    for q in both:
        settle(q, first_now[q], first_n[1 - q], False)
    for q in both:
        spread(q, first_o[q], False)
    for first in (first_p, first_n):
        for q in both:
            settle(q, first[q], first_p[1 - q], True)
        for q in both:
            settle(q, first[q], first_n[1 - q], False)
    for q in both:
        settle(q, first_now[q], first_o[1 - q], False)
    for q in both:
        settle(q, first_o[q], first_p[1 - q], True)
    for q in both:
        settle(q, first_o[q], first_n[1 - q], False)
    for first in (first_p, first_n, first_o):
        for q in both:
            settle(q, first[q], first_o[1 - q], False)
    orders = [first_now, first_p, first_n, first_o]
    for xi in range(RING):
        for yi in range(RING):
            for q in both:
                xx, yy = slot(q, orders[xi][q], orders[yi][1 - q])
                arrived(gp.at[q, xx, yy], gp_recv.at[q, xx, yy])
                store(q, xx, yy, 1 - c, gp[q, xx, yy])
    for copy in sends:
        copy.wait_send()


def combine(p, sinks, hidden, b_o, w_o):
    seqs = p.shape[3] - 1
    heads = p.shape[4]
    num_seqs, d_model = hidden.shape
    cols_core = d_model // CORES
    cols_sub = cols_core // SUBS
    block_rows = num_seqs // (RING * RING)
    part = (seqs + 1, heads, LANES)
    f32, bf16 = jnp.float32, jnp.bfloat16
    dma = pltpu.SemaphoreType.DMA
    vmem = pl.BlockSpec(memory_space=pltpu.VMEM)
    hbm = pl.BlockSpec(memory_space=pl.ANY)
    chunk = (block_rows, cols_sub)
    return pl.pallas_call(
        functools.partial(combine_kernel, seqs),
        out_shape=jax.ShapeDtypeStruct((num_seqs, d_model), bf16),
        in_specs=[vmem, vmem, hbm, vmem, hbm],
        out_specs=vmem,
        scratch_shapes=[
            pltpu.VMEM((RING, SUBS) + part, f32),
            pltpu.VMEM((RING, SUBS) + part, f32),
            pltpu.VMEM((SUBS,) + part, f32),
            pltpu.VMEM((SUBS,) + part, f32),
            pltpu.VMEM((SUBS,) + part, f32),
            pltpu.VMEM((SUBS, seqs * heads, LANES), f32),
            pltpu.VMEM((SUBS, seqs * heads, LANES), f32),
            pltpu.VMEM((2, w_o.shape[0] // 2, cols_core), bf16),
            pltpu.VMEM((block_rows, cols_core), bf16),
            pltpu.VMEM((SUBS, RING) + chunk, f32),
            pltpu.VMEM((SUBS,) + chunk, f32),
            pltpu.VMEM((SUBS,) + chunk, f32),
            pltpu.VMEM((SUBS,) + chunk, f32),
            pltpu.VMEM((SUBS,) + chunk, f32),
            pltpu.VMEM((SUBS, RING, RING) + chunk, f32),
            pltpu.VMEM((SUBS, RING, RING) + chunk, f32),
            dma((2,)), dma((1,)), dma((RING, SUBS)), dma((RING, SUBS)), dma((3, SUBS)),
            dma((SUBS,)), dma((SUBS,)), dma((SUBS,)), dma((SUBS,)), dma((SUBS,)),
            dma((3, SUBS)), dma((SUBS,)), dma((SUBS,)), dma((SUBS,)),
            dma((SUBS, RING, RING, 4)), dma((SUBS, RING, RING)), dma((SUBS, RING, RING)), dma((SUBS, RING, RING)),
        ],
        compiler_params=pltpu.CompilerParams(collective_id=0, has_side_effects=True, vmem_limit_bytes=48 * 2**20),
        cost_estimate=pl.CostEstimate(flops=2 * num_seqs // RING * w_o.shape[0] * cols_core, bytes_accessed=30 * 2**20, transcendentals=0),
        name="combine",
    )(p, sinks, hidden, b_o, w_o)


def front_kernel(
    logit_scale, x_hbm, len_hbm, cos_hbm, sin_hbm, k_hbm, v_hbm, gain_hbm, w_hbm, bias_hbm, sink_hbm,
    p_ref, k_out, v_out,
    xbuf, lens, cos, sin, gain, bias, sinks, hexp, wbuf, acc, qs, kn, vn, kbuf, vbuf,
    in_sem, w_sem, k_sem, v_sem, ko_sem, vo_sem,
):
    num_seqs, d_model = x_hbm.shape
    kv = w_hbm.shape[1]
    qkv = w_hbm.shape[2]
    tiles = qkv // LANES
    heads = tiles - 2
    slots, _, depth2, _ = wbuf.shape
    chunks = d_model * kv // depth2
    blocks, _, seqs1 = p_ref.shape[0], p_ref.shape[1], p_ref.shape[2]
    seqs = seqs1 - 1
    ctx2 = k_hbm.shape[1]
    w_rows = w_hbm.reshape(d_model * kv, qkv)

    def w_copy(chunk, slot, t):
        return pltpu.make_async_copy(
            w_rows.at[pl.ds(pl.multiple_of(chunk * depth2, depth2), depth2), pl.ds(t * LANES, LANES)],
            wbuf.at[slot, t], w_sem.at[slot])

    def w_start(chunk, slot):
        for t in range(tiles):
            w_copy(chunk, slot, t).start()

    small = [
        pltpu.make_async_copy(src, dst, in_sem.at[i])
        for i, (src, dst) in enumerate((
            (x_hbm, xbuf), (gain_hbm, gain), (len_hbm, lens), (cos_hbm, cos), (sin_hbm, sin), (bias_hbm, bias), (sink_hbm, sinks)))
    ]
    for copy in small:
        copy.start()
    for slot in range(slots - 1):
        w_start(slot, slot)

    def cache_copy(hbm, buf, sem, block, out):
        rows = pl.ds(block * seqs, seqs)
        src, dst = hbm.at[rows], buf.at[rows]
        return pltpu.make_async_copy(dst, src, sem.at[block]) if out else pltpu.make_async_copy(src, dst, sem.at[block])

    small[0].wait()
    small[1].wait()
    row = lax.broadcasted_iota(jnp.int32, (LANES, kv * LANES), 0)
    col = lax.broadcasted_iota(jnp.int32, (LANES, kv * LANES), 1)
    picks = [(col == row * kv + k).astype(jnp.bfloat16) for k in range(kv)]
    square = jnp.zeros((num_seqs, LANES), jnp.float32)
    for t in range(d_model // LANES):
        xt = xbuf[:, t * LANES : (t + 1) * LANES].astype(jnp.float32)
        square += xt * xt
    inv_rms = lax.rsqrt(jnp.sum(square, axis=-1, keepdims=True) / d_model + NORM_EPS)
    per_chunk = depth2 // (kv * LANES)
    for t in range(d_model // LANES):
        xt = xbuf[:, t * LANES : (t + 1) * LANES].astype(jnp.float32)
        ht = (xt * inv_rms * gain[:, t * LANES : (t + 1) * LANES].astype(jnp.float32)).astype(jnp.bfloat16)
        for k in range(kv):
            spread = jnp.dot(ht, picks[k], preferred_element_type=jnp.float32).astype(jnp.bfloat16)
            place = t % per_chunk * kv * LANES
            hexp[t // per_chunk, k * num_seqs : (k + 1) * num_seqs, place : place + kv * LANES] = spread
    acc[...] = jnp.zeros_like(acc)

    @pl.loop(0, chunks)
    def _(chunk):
        slot = lax.rem(chunk, slots)

        @pl.when(chunk + slots - 1 < chunks)
        def _():
            w_start(chunk + slots - 1, lax.rem(chunk + slots - 1, slots))

        @pl.when(chunk == chunks - slots)
        def _():
            for block in range(blocks):
                cache_copy(k_hbm, kbuf, k_sem, block, False).start()
                cache_copy(v_hbm, vbuf, v_sem, block, False).start()

        for t in range(tiles):
            w_copy(chunk, slot, t).wait()
        lhs = hexp.at[chunk]
        for t in range(0, tiles, 2):
            rhs = jnp.concatenate([wbuf[slot, t], wbuf[slot, t + 1]], axis=1)
            cols = slice(t * LANES, (t + 2) * LANES)
            acc[:, cols] += jnp.dot(lhs[...], rhs, preferred_element_type=jnp.float32)

    for copy in small[2:]:
        copy.wait()
    cos_t = jnp.transpose(jnp.concatenate([cos[...], cos[...]], axis=0))
    sin_t = jnp.transpose(jnp.concatenate([-sin[...], sin[...]], axis=0))

    def rotate(t):
        return t * cos_t + pltpu.roll(t, HALF, 1) * sin_t

    def rounded(t):
        return t.astype(jnp.bfloat16).astype(jnp.float32)

    for k in range(kv):
        for t in range(tiles):
            cols = slice(t * LANES, (t + 1) * LANES)
            value = acc[k * num_seqs : (k + 1) * num_seqs, cols] + bias[k : k + 1, cols].astype(jnp.float32)
            if t < heads:
                qs[pl.ds(k * heads + t, num_seqs, stride=kv * heads), :] = rotate(value)
            elif t == heads:
                kn[pl.ds(k, num_seqs, stride=kv), :] = rotate(value)
            else:
                vn[pl.ds(k, num_seqs, stride=kv), :] = value

    q_rows = kv * heads
    base = lax.axis_index("sp") * (ctx2 // kv)
    row = lax.broadcasted_iota(jnp.int32, (q_rows, LANES), 0)
    lane = lax.broadcasted_iota(jnp.int32, (q_rows, LANES), 1)
    assert ctx2 == LANES
    position = jnp.where(lane % kv == row // heads, lane // kv + base, jnp.iinfo(jnp.int32).max)
    sink = jnp.zeros((q_rows, LANES), jnp.float32)
    for i in range(q_rows):
        sink = jnp.where(row == i, sinks[i], sink)
    sink_col = jnp.max(sink, axis=-1, keepdims=True)
    group = 16
    group_row = lax.broadcasted_iota(jnp.int32, (group, LANES), 0)

    @pl.loop(0, blocks)
    def _(block):
        cache_copy(k_hbm, kbuf, k_sem, block, False).wait()
        cache_copy(v_hbm, vbuf, v_sem, block, False).wait()
        stats = jnp.zeros((q_rows, LANES), jnp.float32)
        for i in range(seqs):
            b = block * seqs + i
            n = lens[b]
            local = n - base
            here = jnp.logical_and(local >= 0, local < ctx2 // kv)
            place = jnp.where(here, local * kv, 0)
            start = pl.multiple_of(place // group * group, group)
            target = jnp.where(here, place - start, group)
            for buf, new in ((kbuf, kn), (vbuf, vn)):
                fresh = new[pl.ds(b * kv, kv), :]
                value = buf[b, pl.ds(start, group), :].astype(jnp.float32)
                for k in range(kv):
                    value = jnp.where(group_row == target + k, fresh[k : k + 1], value)
                buf[b, pl.ds(start, group), :] = value.astype(jnp.bfloat16)
        for i in range(seqs):
            b = block * seqs + i
            q = qs[pl.ds(pl.multiple_of(b * q_rows, q_rows), q_rows), :].astype(jnp.bfloat16)
            logits = lax.dot_general(q, kbuf[b], (((1,), (1,)), ((), ())), preferred_element_type=jnp.float32) * logit_scale
            logits = jnp.where(position <= lens[b], logits, -jnp.inf)
            top = jnp.maximum(jnp.max(logits, axis=-1, keepdims=True), sink_col)
            weights = jnp.exp(logits - top)
            total = jnp.sum(weights, axis=-1, keepdims=True)
            numer = jnp.dot(weights.astype(jnp.bfloat16), vbuf[b], preferred_element_type=jnp.float32)
            for k in range(kv):
                p_ref[block, k, i] = numer[k * heads : (k + 1) * heads]
            stats = jnp.where(lane == i, top, jnp.where(lane == HALF + i, total, stats))
        for k in range(kv):
            p_ref[block, k, seqs] = stats[k * heads : (k + 1) * heads]
        cache_copy(k_out, kbuf, ko_sem, block, True).start()
        cache_copy(v_out, vbuf, vo_sem, block, True).start()

    for block in range(blocks):
        cache_copy(k_out, kbuf, ko_sem, block, True).wait()
        cache_copy(v_out, vbuf, vo_sem, block, True).wait()


def front(hidden, seq_lens, cos_t, sin_t, k_cache, v_cache, gain, w_qkv, b_qkv, sinks):
    num_seqs, d_model = hidden.shape
    kv, qkv = w_qkv.shape[1:]
    tiles = qkv // LANES
    heads = tiles - 2
    seqs = num_seqs // (RING * SUBS)
    ctx2 = k_cache.shape[1]
    depth2 = 1024
    chunks = d_model * kv // depth2
    slots = 4
    f32, bf16 = jnp.float32, jnp.bfloat16
    dma = pltpu.SemaphoreType.DMA
    hbm = pl.BlockSpec(memory_space=pl.ANY)
    cache = jax.ShapeDtypeStruct(k_cache.shape, bf16)
    return pl.pallas_call(
        functools.partial(front_kernel, LANES ** -0.5),
        out_shape=(jax.ShapeDtypeStruct((RING * SUBS, kv, seqs + 1, heads, LANES), f32), cache, cache),
        in_specs=[hbm] * 10,
        out_specs=(pl.BlockSpec(memory_space=pltpu.VMEM), hbm, hbm),
        scratch_shapes=[
            pltpu.VMEM(hidden.shape, bf16),
            pltpu.SMEM(seq_lens.shape, jnp.int32),
            pltpu.VMEM(cos_t.shape, f32),
            pltpu.VMEM(sin_t.shape, f32),
            pltpu.VMEM(gain.shape, bf16),
            pltpu.VMEM(b_qkv.shape, bf16),
            pltpu.SMEM(sinks.shape, f32),
            pltpu.VMEM((chunks, kv * num_seqs, depth2), bf16),
            pltpu.VMEM((slots, tiles, depth2, LANES), bf16),
            pltpu.VMEM((kv * num_seqs, qkv), f32),
            pltpu.VMEM((num_seqs * kv * heads, LANES), f32),
            pltpu.VMEM((num_seqs * kv, LANES), f32),
            pltpu.VMEM((num_seqs * kv, LANES), f32),
            pltpu.VMEM(k_cache.shape, bf16),
            pltpu.VMEM(v_cache.shape, bf16),
            dma((7,)), dma((slots,)), dma((RING * SUBS,)), dma((RING * SUBS,)), dma((RING * SUBS,)), dma((RING * SUBS,)),
        ],
        compiler_params=pltpu.CompilerParams(vmem_limit_bytes=44 * 2**20),
        cost_estimate=pl.CostEstimate(flops=4 * num_seqs * d_model * kv * qkv, bytes_accessed=50 * 2**20, transcendentals=0),
        name="front",
    )(hidden, seq_lens, cos_t, sin_t, k_cache, v_cache, gain, w_qkv, b_qkv, sinks)


def solution(mesh):
    cache_spec = P("dp", "sp", "tp", None)

    def block_step(hidden, seq_lens, rope_cos, rope_sin, k_cache, v_cache, norm_gain, w_qkv, b_qkv, sink_logits, w_o, b_o):
        num_seqs, ctx, kv, head_dim = k_cache.shape
        assert head_dim == LANES and mesh.shape["tp"] == RING and mesh.shape["sp"] == RING * CORES
        flat = (num_seqs, ctx * kv, head_dim)
        packed, k_out, v_out = front(
            hidden, seq_lens, rope_cos.T, rope_sin.T, k_cache.reshape(flat), v_cache.reshape(flat), norm_gain[None, :], w_qkv, b_qkv, sink_logits)
        packed = packed.reshape((RING, SUBS) + packed.shape[1:])
        sinks = jnp.broadcast_to(sink_logits[:, None], (sink_logits.shape[0], LANES))
        out_hidden = combine(packed, sinks, hidden, b_o[None, :], w_o)
        return out_hidden, k_out.reshape(k_cache.shape), v_out.reshape(v_cache.shape)

    return jax.shard_map(block_step, mesh=mesh, in_specs=(P("dp", None), P("dp"), P("dp", None), P("dp", None), cache_spec, cache_spec, P(None), P(None, "tp", None), P("tp", None), P("tp"), P("tp", None), P(None)), out_specs=(P("dp", None), cache_spec, cache_spec), check_vma=False)
```

```python
import functools

import jax
import jax.numpy as jnp
from jax import lax
from jax.experimental import pallas as pl
from jax.experimental.pallas import tpu as pltpu
from jax.sharding import PartitionSpec as P

NORM_EPS = 1e-5
MESH = pl.DeviceIdType.MESH
LANES = 128
HALF = LANES // 2
SUBS = 2
CORES = 2
RING = 4


def lane_column(tile, index):
    return tile[:, index : index + 1]


def merge_parts(parts, seqs):
    stats = [part[seqs] for part in parts]
    top = functools.reduce(jnp.maximum, stats)
    scales = [jnp.exp(stat - top) for stat in stats]
    total = sum(pltpu.roll(scale, HALF, 1) * stat for scale, stat in zip(scales, stats))
    return top, total, scales


def merge_into(dst, parts, seqs):
    top, total, scales = merge_parts(parts, seqs)
    for i in range(seqs):
        dst[i] = sum(lane_column(scale, i) * part[i] for scale, part in zip(scales, parts))
    lane = lax.broadcasted_iota(jnp.int32, top.shape, 1)
    dst[seqs] = jnp.where(lane < HALF, top, total)


def combine_kernel(
    seqs, p_ref, sink_ref, x_hbm, bo_ref, wo_hbm, out_ref,
    ra, cb, rl, rm, rd, own_o, other_o, wbuf, xbuf, z, yrl, ym, yrm, yrd, g, gp,
    w_sem, x_sem, a_send, a_recv, b_send, rl_recv, rm_recv, rd_recv, o_send, o_recv,
    d_send, yrl_recv, yrm_recv, yrd_recv, g_send, g_recv, gp_send, gp_recv,
):
    y = lax.axis_index("tp")
    sp = lax.axis_index("sp")
    x = sp // CORES
    c = sp % CORES
    step = 1 - 2 * c
    xn, xp, xo = (x + step + RING) % RING, (x - step + RING) % RING, (x + 2) % RING
    yn, yp, yo = (y + step + RING) % RING, (y - step + RING) % RING, (y + 2) % RING
    partner = {"sp": x * CORES + 1 - c}
    to_xn, to_xp = {"sp": xn * CORES + c}, {"sp": xp * CORES + c}
    to_yn, to_yp = {"tp": yn}, {"tp": yp}

    rows_half = wo_hbm.shape[0] // 2
    cols_core = wo_hbm.shape[1] // CORES
    cols_sub = cols_core // SUBS
    heads = p_ref.shape[4]
    block_rows = z.shape[2]

    w_copies = []
    for k in range(2):
        rows = (c if k == 0 else 1 - c) * rows_half
        copy = pltpu.make_async_copy(
            wo_hbm.at[pl.ds(pl.multiple_of(rows, LANES), rows_half), pl.ds(pl.multiple_of(c * cols_core, LANES), cols_core)],
            wbuf.at[k], w_sem.at[k])
        copy.start()
        w_copies.append(copy)
    row0 = pl.multiple_of((x * RING + y) * block_rows, block_rows)
    x_copy = pltpu.make_async_copy(
        x_hbm.at[pl.ds(row0, block_rows), pl.ds(pl.multiple_of(c * cols_core, LANES), cols_core)], xbuf, x_sem.at[0])
    x_copy.start()

    barrier = pltpu.get_barrier_semaphore()
    for where in (partner, to_xn, to_xp, to_yn, to_yp):
        pl.semaphore_signal(barrier, inc=1, device_id=where, device_id_type=MESH)
    pl.semaphore_wait(barrier, 5)

    sends = []

    def send(src, dst, send_sem, recv_sem, where):
        copy = pltpu.make_async_remote_copy(
            src_ref=src, dst_ref=dst, send_sem=send_sem, recv_sem=recv_sem, device_id=where, device_id_type=MESH)
        copy.start()
        sends.append(copy)

    def arrived(dst, recv_sem):
        pltpu.make_async_remote_copy(
            src_ref=dst, dst_ref=dst, send_sem=recv_sem, recv_sem=recv_sem, device_id=partner, device_id_type=MESH).wait_recv()

    for k, b in enumerate((xo, xp, xn, x)):
        for s in range(SUBS):
            send(p_ref.at[b, s, 1 - c], ra.at[b, s], a_send.at[k, s], a_recv.at[b, s], partner)

    for s in range(SUBS):
        arrived(ra.at[xo, s], a_recv.at[xo, s])
        merge_into(cb.at[0, s], (p_ref.at[xo, s, c], ra.at[xo, s]), seqs)
        send(cb.at[0, s], rl.at[s], b_send.at[0, s], rl_recv.at[s], to_xn)
    for s in range(SUBS):
        arrived(ra.at[xp, s], a_recv.at[xp, s])
        merge_into(cb.at[1, s], (p_ref.at[xp, s, c], ra.at[xp, s]), seqs)
        send(cb.at[1, s], rd.at[s], b_send.at[1, s], rd_recv.at[s], to_xp)
    for s in range(SUBS):
        arrived(ra.at[xn, s], a_recv.at[xn, s])
        arrived(rl.at[s], rl_recv.at[s])
        merge_into(cb.at[2, s], (p_ref.at[xn, s, c], ra.at[xn, s], rl.at[s]), seqs)
        send(cb.at[2, s], rm.at[s], b_send.at[2, s], rm_recv.at[s], to_xn)
    for s in range(SUBS):
        arrived(ra.at[x, s], a_recv.at[x, s])
        merge_into(cb.at[3, s], (p_ref.at[x, s, c], ra.at[x, s]), seqs)
    sink = sink_ref[pl.ds(pl.multiple_of(c * heads, heads), heads), :]
    for s in range(SUBS):
        arrived(rd.at[s], rd_recv.at[s])
        arrived(rm.at[s], rm_recv.at[s])
        parts = (cb.at[3, s], rd.at[s], rm.at[s])
        top, total, scales = merge_parts(parts, seqs)
        inverse = 1.0 / (pltpu.roll(total, HALF, 1) + jnp.exp(sink - top))
        for i in range(seqs):
            summed = sum(lane_column(scale, i) * part[i] for scale, part in zip(scales, parts))
            head_out = summed * lane_column(inverse, i)
            own_o[s, pl.ds(i * heads, heads), :] = head_out.astype(jnp.bfloat16).astype(jnp.float32)
        send(own_o.at[s], other_o.at[s], o_send.at[s], o_recv.at[s], partner)

    def head_rows(ref):
        columns = []
        for h in range(heads):
            columns.append(jnp.concatenate(
                [ref[s, pl.ds(h, seqs, stride=heads), :] for s in range(SUBS)], axis=0).astype(jnp.bfloat16))
        return jnp.concatenate(columns, axis=1)

    own_rows = head_rows(own_o)
    w_copies[0].wait()
    for q in range(SUBS):
        part = jnp.dot(own_rows, wbuf[0, :, pl.ds(q * cols_sub, cols_sub)], preferred_element_type=jnp.float32)
        for r in range(RING):
            z[q, r] = part[r * block_rows : (r + 1) * block_rows]
    for s in range(SUBS):
        arrived(other_o.at[s], o_recv.at[s])
    other_rows = head_rows(other_o)
    w_copies[1].wait()
    for q in range(SUBS):
        part = jnp.dot(other_rows, wbuf[1, :, pl.ds(q * cols_sub, cols_sub)], preferred_element_type=jnp.float32)
        for r in range(RING):
            z[q, r] += part[r * block_rows : (r + 1) * block_rows]
        send(z.at[q, yo], yrl.at[q], d_send.at[0, q], yrl_recv.at[q], to_yn)
        send(z.at[q, yp], yrd.at[q], d_send.at[1, q], yrd_recv.at[q], to_yp)
    for q in range(SUBS):
        arrived(yrl.at[q], yrl_recv.at[q])
        ym[q] = z[q, yn] + yrl[q]
        send(ym.at[q], yrm.at[q], d_send.at[2, q], yrm_recv.at[q], to_yn)
    x_copy.wait()

    def store(q, xx, yy, core, value):
        rows = pl.ds(pl.multiple_of((xx * RING + yy) * block_rows, block_rows), block_rows)
        cols = pl.ds(pl.multiple_of(core * cols_core + q * cols_sub, LANES), cols_sub)
        out_ref[rows, cols] = value.astype(jnp.bfloat16)

    def slot(q, first, second):
        return (first, second) if q == 0 else (second, first)

    ahead = ((to_xn, to_xp), (to_yn, to_yp))
    first_now, first_n, first_p, first_o = (x, y), (xn, yn), (xp, yp), (xo, yo)

    def push(q, first, second, kind, where):
        xx, yy = slot(q, first, second)
        send(g.at[q, xx, yy], g.at[q, xx, yy], g_send.at[q, xx, yy, kind], g_recv.at[q, xx, yy], where)

    def share(q, first, second):
        xx, yy = slot(q, first, second)
        send(g.at[q, xx, yy], gp.at[q, xx, yy], gp_send.at[q, xx, yy], gp_recv.at[q, xx, yy], partner)

    def receive(q, first, second):
        xx, yy = slot(q, first, second)
        arrived(g.at[q, xx, yy], g_recv.at[q, xx, yy])

    def keep(q, first, second):
        xx, yy = slot(q, first, second)
        store(q, xx, yy, c, g[q, xx, yy])

    for q in range(SUBS):
        arrived(yrd.at[q], yrd_recv.at[q])
        arrived(yrm.at[q], yrm_recv.at[q])
        cols = pl.ds(q * cols_sub, cols_sub)
        bias = bo_ref[:, pl.ds(pl.multiple_of(c * cols_core + q * cols_sub, LANES), cols_sub)]
        summed = z[q, y] + yrd[q] + yrm[q]
        final = xbuf[:, cols].astype(jnp.float32) + summed + bias.astype(jnp.float32)
        g[q, x, y] = final.astype(jnp.bfloat16).astype(jnp.float32)
        for axis in (q, 1 - q):
            for kind in range(2):
                push(q, first_now[q], first_now[1 - q], 2 * (axis != q) + kind, ahead[axis][kind])
        share(q, first_now[q], first_now[1 - q])

    def spread(q, first, forward):
        other = 1 - q
        receive(q, first, first_now[other])
        if forward:
            push(q, first, first_now[other], 0, ahead[q][0])
        for kind in range(2):
            push(q, first, first_now[other], 2 + kind, ahead[other][kind])
        share(q, first, first_now[other])
        keep(q, first, first_now[other])

    def settle(q, first, second, forward):
        receive(q, first, second)
        if forward:
            push(q, first, second, 2, ahead[1 - q][0])
        share(q, first, second)
        keep(q, first, second)

    both = range(SUBS)
    for q in both:
        spread(q, first_p[q], True)
    for q in both:
        spread(q, first_n[q], False)
    for q in both:
        keep(q, first_now[q], first_now[1 - q])
    for q in both:
        settle(q, first_now[q], first_p[1 - q], True)
    for q in both:
        settle(q, first_now[q], first_n[1 - q], False)
    for q in both:
        spread(q, first_o[q], False)
    for first in (first_p, first_n):
        for q in both:
            settle(q, first[q], first_p[1 - q], True)
        for q in both:
            settle(q, first[q], first_n[1 - q], False)
    for q in both:
        settle(q, first_now[q], first_o[1 - q], False)
    for q in both:
        settle(q, first_o[q], first_p[1 - q], True)
    for q in both:
        settle(q, first_o[q], first_n[1 - q], False)
    for first in (first_p, first_n, first_o):
        for q in both:
            settle(q, first[q], first_o[1 - q], False)
    orders = [first_now, first_p, first_n, first_o]
    for xi in range(RING):
        for yi in range(RING):
            for q in both:
                xx, yy = slot(q, orders[xi][q], orders[yi][1 - q])
                arrived(gp.at[q, xx, yy], gp_recv.at[q, xx, yy])
                store(q, xx, yy, 1 - c, gp[q, xx, yy])
    for copy in sends:
        copy.wait_send()


def combine(p, sinks, hidden, b_o, w_o):
    seqs = p.shape[3] - 1
    heads = p.shape[4]
    num_seqs, d_model = hidden.shape
    cols_core = d_model // CORES
    cols_sub = cols_core // SUBS
    block_rows = num_seqs // (RING * RING)
    part = (seqs + 1, heads, LANES)
    f32, bf16 = jnp.float32, jnp.bfloat16
    dma = pltpu.SemaphoreType.DMA
    vmem = pl.BlockSpec(memory_space=pltpu.VMEM)
    hbm = pl.BlockSpec(memory_space=pl.ANY)
    chunk = (block_rows, cols_sub)
    return pl.pallas_call(
        functools.partial(combine_kernel, seqs),
        out_shape=jax.ShapeDtypeStruct((num_seqs, d_model), bf16),
        in_specs=[vmem, vmem, hbm, vmem, hbm],
        out_specs=vmem,
        scratch_shapes=[
            pltpu.VMEM((RING, SUBS) + part, f32),
            pltpu.VMEM((RING, SUBS) + part, f32),
            pltpu.VMEM((SUBS,) + part, f32),
            pltpu.VMEM((SUBS,) + part, f32),
            pltpu.VMEM((SUBS,) + part, f32),
            pltpu.VMEM((SUBS, seqs * heads, LANES), f32),
            pltpu.VMEM((SUBS, seqs * heads, LANES), f32),
            pltpu.VMEM((2, w_o.shape[0] // 2, cols_core), bf16),
            pltpu.VMEM((block_rows, cols_core), bf16),
            pltpu.VMEM((SUBS, RING) + chunk, f32),
            pltpu.VMEM((SUBS,) + chunk, f32),
            pltpu.VMEM((SUBS,) + chunk, f32),
            pltpu.VMEM((SUBS,) + chunk, f32),
            pltpu.VMEM((SUBS,) + chunk, f32),
            pltpu.VMEM((SUBS, RING, RING) + chunk, f32),
            pltpu.VMEM((SUBS, RING, RING) + chunk, f32),
            dma((2,)), dma((1,)), dma((RING, SUBS)), dma((RING, SUBS)), dma((3, SUBS)),
            dma((SUBS,)), dma((SUBS,)), dma((SUBS,)), dma((SUBS,)), dma((SUBS,)),
            dma((3, SUBS)), dma((SUBS,)), dma((SUBS,)), dma((SUBS,)),
            dma((SUBS, RING, RING, 4)), dma((SUBS, RING, RING)), dma((SUBS, RING, RING)), dma((SUBS, RING, RING)),
        ],
        compiler_params=pltpu.CompilerParams(collective_id=0, has_side_effects=True, vmem_limit_bytes=48 * 2**20),
        cost_estimate=pl.CostEstimate(flops=2 * num_seqs // RING * w_o.shape[0] * cols_core, bytes_accessed=30 * 2**20, transcendentals=0),
        name="combine",
    )(p, sinks, hidden, b_o, w_o)


def front_kernel(
    logit_scale, x_hbm, len_hbm, cos_hbm, sin_hbm, k_hbm, v_hbm, gain_hbm, w_hbm, bias_hbm, sink_hbm,
    p_ref, k_out, v_out,
    xbuf, lens, cos, sin, gain, bias, sinks, hexp, wbuf, acc, qs, kn, vn, kbuf, vbuf,
    in_sem, w_sem, k_sem, v_sem, ko_sem, vo_sem,
):
    num_seqs, d_model = x_hbm.shape
    kv = w_hbm.shape[1]
    qkv = w_hbm.shape[2]
    tiles = qkv // LANES
    heads = tiles - 2
    slots, depth2, _ = wbuf.shape
    chunks = d_model * kv // depth2
    blocks, _, seqs1 = p_ref.shape[0], p_ref.shape[1], p_ref.shape[2]
    seqs = seqs1 - 1
    ctx2 = k_hbm.shape[1]
    w_rows = w_hbm.reshape(d_model * kv, qkv)

    def w_copy(chunk, slot):
        return pltpu.make_async_copy(
            w_rows.at[pl.ds(pl.multiple_of(chunk * depth2, depth2), depth2), :], wbuf.at[slot], w_sem.at[slot])

    def w_start(chunk, slot):
        w_copy(chunk, slot).start()

    small = [
        pltpu.make_async_copy(src, dst, in_sem.at[i])
        for i, (src, dst) in enumerate((
            (x_hbm, xbuf), (gain_hbm, gain), (len_hbm, lens), (cos_hbm, cos), (sin_hbm, sin), (bias_hbm, bias), (sink_hbm, sinks)))
    ]
    for copy in small:
        copy.start()
    for slot in range(slots - 1):
        w_start(slot, slot)

    def cache_copy(hbm, buf, sem, block, out):
        rows = pl.ds(block * seqs, seqs)
        src, dst = hbm.at[rows], buf.at[rows]
        return pltpu.make_async_copy(dst, src, sem.at[block]) if out else pltpu.make_async_copy(src, dst, sem.at[block])

    small[0].wait()
    small[1].wait()
    row = lax.broadcasted_iota(jnp.int32, (LANES, kv * LANES), 0)
    col = lax.broadcasted_iota(jnp.int32, (LANES, kv * LANES), 1)
    picks = [(col == row * kv + k).astype(jnp.bfloat16) for k in range(kv)]
    square = jnp.zeros((num_seqs, LANES), jnp.float32)
    for t in range(d_model // LANES):
        xt = xbuf[:, t * LANES : (t + 1) * LANES].astype(jnp.float32)
        square += xt * xt
    inv_rms = lax.rsqrt(jnp.sum(square, axis=-1, keepdims=True) / d_model + NORM_EPS)
    per_chunk = depth2 // (kv * LANES)
    for t in range(d_model // LANES):
        xt = xbuf[:, t * LANES : (t + 1) * LANES].astype(jnp.float32)
        ht = (xt * inv_rms * gain[:, t * LANES : (t + 1) * LANES].astype(jnp.float32)).astype(jnp.bfloat16)
        for k in range(kv):
            spread = jnp.dot(ht, picks[k], preferred_element_type=jnp.float32).astype(jnp.bfloat16)
            place = t % per_chunk * kv * LANES
            hexp[t // per_chunk, k * num_seqs : (k + 1) * num_seqs, place : place + kv * LANES] = spread
    acc[...] = jnp.zeros_like(acc)

    @pl.loop(0, chunks)
    def _(chunk):
        slot = lax.rem(chunk, slots)

        @pl.when(chunk + slots - 1 < chunks)
        def _():
            w_start(chunk + slots - 1, lax.rem(chunk + slots - 1, slots))

        @pl.when(chunk == chunks - slots)
        def _():
            for block in range(blocks):
                cache_copy(k_hbm, kbuf, k_sem, block, False).start()
                cache_copy(v_hbm, vbuf, v_sem, block, False).start()

        w_copy(chunk, slot).wait()
        lhs = hexp.at[chunk]
        for t in range(0, tiles, 2):
            cols = slice(t * LANES, (t + 2) * LANES)
            acc[:, cols] += jnp.dot(lhs[...], wbuf[slot, :, cols], preferred_element_type=jnp.float32)

    for copy in small[2:]:
        copy.wait()
    cos_t = jnp.transpose(jnp.concatenate([cos[...], cos[...]], axis=0))
    sin_t = jnp.transpose(jnp.concatenate([-sin[...], sin[...]], axis=0))

    def rotate(t):
        return t * cos_t + pltpu.roll(t, HALF, 1) * sin_t

    def rounded(t):
        return t.astype(jnp.bfloat16).astype(jnp.float32)

    for k in range(kv):
        for t in range(tiles):
            cols = slice(t * LANES, (t + 1) * LANES)
            value = acc[k * num_seqs : (k + 1) * num_seqs, cols] + bias[k : k + 1, cols].astype(jnp.float32)
            if t < heads:
                qs[pl.ds(k * heads + t, num_seqs, stride=kv * heads), :] = rotate(value)
            elif t == heads:
                kn[pl.ds(k, num_seqs, stride=kv), :] = rotate(value)
            else:
                vn[pl.ds(k, num_seqs, stride=kv), :] = value

    q_rows = kv * heads
    base = lax.axis_index("sp") * (ctx2 // kv)
    row = lax.broadcasted_iota(jnp.int32, (q_rows, LANES), 0)
    lane = lax.broadcasted_iota(jnp.int32, (q_rows, LANES), 1)
    assert ctx2 == LANES
    position = jnp.where(lane % kv == row // heads, lane // kv + base, jnp.iinfo(jnp.int32).max)
    sink = jnp.zeros((q_rows, LANES), jnp.float32)
    for i in range(q_rows):
        sink = jnp.where(row == i, sinks[i], sink)
    sink_col = jnp.max(sink, axis=-1, keepdims=True)
    group = 16
    group_row = lax.broadcasted_iota(jnp.int32, (group, LANES), 0)

    @pl.loop(0, blocks)
    def _(block):
        cache_copy(k_hbm, kbuf, k_sem, block, False).wait()
        cache_copy(v_hbm, vbuf, v_sem, block, False).wait()
        stats = jnp.zeros((q_rows, LANES), jnp.float32)
        for i in range(seqs):
            b = block * seqs + i
            n = lens[b]
            local = n - base
            here = jnp.logical_and(local >= 0, local < ctx2 // kv)
            place = jnp.where(here, local * kv, 0)
            start = pl.multiple_of(place // group * group, group)
            target = jnp.where(here, place - start, group)
            for buf, new in ((kbuf, kn), (vbuf, vn)):
                fresh = new[pl.ds(b * kv, kv), :]
                value = buf[b, pl.ds(start, group), :].astype(jnp.float32)
                for k in range(kv):
                    value = jnp.where(group_row == target + k, fresh[k : k + 1], value)
                buf[b, pl.ds(start, group), :] = value.astype(jnp.bfloat16)
        for i in range(seqs):
            b = block * seqs + i
            q = qs[pl.ds(pl.multiple_of(b * q_rows, q_rows), q_rows), :].astype(jnp.bfloat16)
            logits = lax.dot_general(q, kbuf[b], (((1,), (1,)), ((), ())), preferred_element_type=jnp.float32) * logit_scale
            logits = jnp.where(position <= lens[b], logits, -jnp.inf)
            top = jnp.maximum(jnp.max(logits, axis=-1, keepdims=True), sink_col)
            weights = jnp.exp(logits - top)
            total = jnp.sum(weights, axis=-1, keepdims=True)
            numer = jnp.dot(weights.astype(jnp.bfloat16), vbuf[b], preferred_element_type=jnp.float32)
            for k in range(kv):
                p_ref[block, k, i] = numer[k * heads : (k + 1) * heads]
            stats = jnp.where(lane == i, top, jnp.where(lane == HALF + i, total, stats))
        for k in range(kv):
            p_ref[block, k, seqs] = stats[k * heads : (k + 1) * heads]
        cache_copy(k_out, kbuf, ko_sem, block, True).start()
        cache_copy(v_out, vbuf, vo_sem, block, True).start()

    for block in range(blocks):
        cache_copy(k_out, kbuf, ko_sem, block, True).wait()
        cache_copy(v_out, vbuf, vo_sem, block, True).wait()


def front(hidden, seq_lens, cos_t, sin_t, k_cache, v_cache, gain, w_qkv, b_qkv, sinks):
    num_seqs, d_model = hidden.shape
    kv, qkv = w_qkv.shape[1:]
    tiles = qkv // LANES
    heads = tiles - 2
    seqs = num_seqs // (RING * SUBS)
    ctx2 = k_cache.shape[1]
    depth2 = 1024
    chunks = d_model * kv // depth2
    slots = 4
    f32, bf16 = jnp.float32, jnp.bfloat16
    dma = pltpu.SemaphoreType.DMA
    hbm = pl.BlockSpec(memory_space=pl.ANY)
    cache = jax.ShapeDtypeStruct(k_cache.shape, bf16)
    return pl.pallas_call(
        functools.partial(front_kernel, LANES ** -0.5),
        out_shape=(jax.ShapeDtypeStruct((RING * SUBS, kv, seqs + 1, heads, LANES), f32), cache, cache),
        in_specs=[hbm] * 10,
        out_specs=(pl.BlockSpec(memory_space=pltpu.VMEM), hbm, hbm),
        scratch_shapes=[
            pltpu.VMEM(hidden.shape, bf16),
            pltpu.SMEM(seq_lens.shape, jnp.int32),
            pltpu.VMEM(cos_t.shape, f32),
            pltpu.VMEM(sin_t.shape, f32),
            pltpu.VMEM(gain.shape, bf16),
            pltpu.VMEM(b_qkv.shape, bf16),
            pltpu.SMEM(sinks.shape, f32),
            pltpu.VMEM((chunks, kv * num_seqs, depth2), bf16),
            pltpu.VMEM((slots, depth2, qkv), bf16),
            pltpu.VMEM((kv * num_seqs, qkv), f32),
            pltpu.VMEM((num_seqs * kv * heads, LANES), f32),
            pltpu.VMEM((num_seqs * kv, LANES), f32),
            pltpu.VMEM((num_seqs * kv, LANES), f32),
            pltpu.VMEM(k_cache.shape, bf16),
            pltpu.VMEM(v_cache.shape, bf16),
            dma((7,)), dma((slots,)), dma((RING * SUBS,)), dma((RING * SUBS,)), dma((RING * SUBS,)), dma((RING * SUBS,)),
        ],
        compiler_params=pltpu.CompilerParams(vmem_limit_bytes=44 * 2**20),
        cost_estimate=pl.CostEstimate(flops=4 * num_seqs * d_model * kv * qkv, bytes_accessed=50 * 2**20, transcendentals=0),
        name="front",
    )(*(pltpu.with_memory_space_constraint(a, pltpu.HBM) for a in (hidden, seq_lens, cos_t, sin_t, k_cache, v_cache, gain, w_qkv, b_qkv, sinks)))


def solution(mesh):
    cache_spec = P("dp", "sp", "tp", None)

    def block_step(hidden, seq_lens, rope_cos, rope_sin, k_cache, v_cache, norm_gain, w_qkv, b_qkv, sink_logits, w_o, b_o):
        num_seqs, ctx, kv, head_dim = k_cache.shape
        assert head_dim == LANES and mesh.shape["tp"] == RING and mesh.shape["sp"] == RING * CORES
        flat = (num_seqs, ctx * kv, head_dim)
        packed, k_out, v_out = front(
            hidden, seq_lens, rope_cos.T, rope_sin.T, k_cache.reshape(flat), v_cache.reshape(flat), norm_gain[None, :], w_qkv, b_qkv, sink_logits)
        packed = packed.reshape((RING, SUBS) + packed.shape[1:])
        sinks = jnp.broadcast_to(sink_logits[:, None], (sink_logits.shape[0], LANES))
        out_hidden = combine(packed, sinks, hidden, b_o[None, :], w_o)
        return out_hidden, k_out.reshape(k_cache.shape), v_out.reshape(v_cache.shape)

    return jax.shard_map(block_step, mesh=mesh, in_specs=(P("dp", None), P("dp"), P("dp", None), P("dp", None), cache_spec, cache_spec, P(None), P(None, "tp", None), P("tp", None), P("tp"), P("tp", None), P(None)), out_specs=(P("dp", None), cache_spec, cache_spec), check_vma=False)
```

```python
import functools

import jax
import jax.numpy as jnp
from jax import lax
from jax.experimental import pallas as pl
from jax.experimental.pallas import tpu as pltpu
from jax.sharding import PartitionSpec as P

NORM_EPS = 1e-5
MESH = pl.DeviceIdType.MESH
LANES = 128
HALF = LANES // 2
SUBS = 2
CORES = 2
RING = 4


def lane_column(tile, index):
    return tile[:, index : index + 1]


def merge_parts(parts, seqs):
    stats = [part[seqs] for part in parts]
    top = functools.reduce(jnp.maximum, stats)
    scales = [jnp.exp(stat - top) for stat in stats]
    total = sum(pltpu.roll(scale, HALF, 1) * stat for scale, stat in zip(scales, stats))
    return top, total, scales


def merge_into(dst, parts, seqs):
    top, total, scales = merge_parts(parts, seqs)
    for i in range(seqs):
        dst[i] = sum(lane_column(scale, i) * part[i] for scale, part in zip(scales, parts))
    lane = lax.broadcasted_iota(jnp.int32, top.shape, 1)
    dst[seqs] = jnp.where(lane < HALF, top, total)


def combine_kernel(
    seqs, p_ref, sink_ref, x_hbm, bo_ref, wo_hbm, out_ref,
    ra, cb, rl, rm, rd, own_o, other_o, wbuf, xbuf, z, yrl, ym, yrm, yrd, g, gp,
    w_sem, x_sem, a_send, a_recv, b_send, rl_recv, rm_recv, rd_recv, o_send, o_recv,
    d_send, yrl_recv, yrm_recv, yrd_recv, g_send, g_recv, gp_send, gp_recv,
):
    y = lax.axis_index("tp")
    sp = lax.axis_index("sp")
    x = sp // CORES
    c = sp % CORES
    step = 1 - 2 * c
    xn, xp, xo = (x + step + RING) % RING, (x - step + RING) % RING, (x + 2) % RING
    yn, yp, yo = (y + step + RING) % RING, (y - step + RING) % RING, (y + 2) % RING
    partner = {"sp": x * CORES + 1 - c}
    to_xn, to_xp = {"sp": xn * CORES + c}, {"sp": xp * CORES + c}
    to_yn, to_yp = {"tp": yn}, {"tp": yp}

    rows_half = wo_hbm.shape[0] // 2
    cols_core = wo_hbm.shape[1] // CORES
    cols_sub = cols_core // SUBS
    heads = p_ref.shape[4]
    block_rows = z.shape[2]

    w_copies = []
    for k in range(2):
        rows = (c if k == 0 else 1 - c) * rows_half
        copy = pltpu.make_async_copy(
            wo_hbm.at[pl.ds(pl.multiple_of(rows, LANES), rows_half), pl.ds(pl.multiple_of(c * cols_core, LANES), cols_core)],
            wbuf.at[k], w_sem.at[k])
        copy.start()
        w_copies.append(copy)
    row0 = pl.multiple_of((x * RING + y) * block_rows, block_rows)
    x_copy = pltpu.make_async_copy(
        x_hbm.at[pl.ds(row0, block_rows), pl.ds(pl.multiple_of(c * cols_core, LANES), cols_core)], xbuf, x_sem.at[0])
    x_copy.start()

    barrier = pltpu.get_barrier_semaphore()
    for where in (partner, to_xn, to_xp, to_yn, to_yp):
        pl.semaphore_signal(barrier, inc=1, device_id=where, device_id_type=MESH)
    pl.semaphore_wait(barrier, 5)

    sends = []

    def send(src, dst, send_sem, recv_sem, where):
        copy = pltpu.make_async_remote_copy(
            src_ref=src, dst_ref=dst, send_sem=send_sem, recv_sem=recv_sem, device_id=where, device_id_type=MESH)
        copy.start()
        sends.append(copy)

    def arrived(dst, recv_sem):
        pltpu.make_async_remote_copy(
            src_ref=dst, dst_ref=dst, send_sem=recv_sem, recv_sem=recv_sem, device_id=partner, device_id_type=MESH).wait_recv()

    for k, b in enumerate((xo, xp, xn, x)):
        for s in range(SUBS):
            send(p_ref.at[b, s, 1 - c], ra.at[b, s], a_send.at[k, s], a_recv.at[b, s], partner)

    for s in range(SUBS):
        arrived(ra.at[xo, s], a_recv.at[xo, s])
        merge_into(cb.at[0, s], (p_ref.at[xo, s, c], ra.at[xo, s]), seqs)
        send(cb.at[0, s], rl.at[s], b_send.at[0, s], rl_recv.at[s], to_xn)
    for s in range(SUBS):
        arrived(ra.at[xp, s], a_recv.at[xp, s])
        merge_into(cb.at[1, s], (p_ref.at[xp, s, c], ra.at[xp, s]), seqs)
        send(cb.at[1, s], rd.at[s], b_send.at[1, s], rd_recv.at[s], to_xp)
    for s in range(SUBS):
        arrived(ra.at[xn, s], a_recv.at[xn, s])
        arrived(rl.at[s], rl_recv.at[s])
        merge_into(cb.at[2, s], (p_ref.at[xn, s, c], ra.at[xn, s], rl.at[s]), seqs)
        send(cb.at[2, s], rm.at[s], b_send.at[2, s], rm_recv.at[s], to_xn)
    for s in range(SUBS):
        arrived(ra.at[x, s], a_recv.at[x, s])
        merge_into(cb.at[3, s], (p_ref.at[x, s, c], ra.at[x, s]), seqs)
    sink = sink_ref[pl.ds(pl.multiple_of(c * heads, heads), heads), :]
    for s in range(SUBS):
        arrived(rd.at[s], rd_recv.at[s])
        arrived(rm.at[s], rm_recv.at[s])
        parts = (cb.at[3, s], rd.at[s], rm.at[s])
        top, total, scales = merge_parts(parts, seqs)
        inverse = 1.0 / (pltpu.roll(total, HALF, 1) + jnp.exp(sink - top))
        for i in range(seqs):
            summed = sum(lane_column(scale, i) * part[i] for scale, part in zip(scales, parts))
            head_out = summed * lane_column(inverse, i)
            own_o[s, pl.ds(i * heads, heads), :] = head_out.astype(jnp.bfloat16).astype(jnp.float32)
        send(own_o.at[s], other_o.at[s], o_send.at[s], o_recv.at[s], partner)

    def head_rows(ref):
        columns = []
        for h in range(heads):
            columns.append(jnp.concatenate(
                [ref[s, pl.ds(h, seqs, stride=heads), :] for s in range(SUBS)], axis=0).astype(jnp.bfloat16))
        return jnp.concatenate(columns, axis=1)

    own_rows = head_rows(own_o)
    w_copies[0].wait()
    for q in range(SUBS):
        part = jnp.dot(own_rows, wbuf[0, :, pl.ds(q * cols_sub, cols_sub)], preferred_element_type=jnp.float32)
        for r in range(RING):
            z[q, r] = part[r * block_rows : (r + 1) * block_rows]
    for s in range(SUBS):
        arrived(other_o.at[s], o_recv.at[s])
    other_rows = head_rows(other_o)
    w_copies[1].wait()
    for q in range(SUBS):
        part = jnp.dot(other_rows, wbuf[1, :, pl.ds(q * cols_sub, cols_sub)], preferred_element_type=jnp.float32)
        for r in range(RING):
            z[q, r] += part[r * block_rows : (r + 1) * block_rows]
        send(z.at[q, yo], yrl.at[q], d_send.at[0, q], yrl_recv.at[q], to_yn)
        send(z.at[q, yp], yrd.at[q], d_send.at[1, q], yrd_recv.at[q], to_yp)
    for q in range(SUBS):
        arrived(yrl.at[q], yrl_recv.at[q])
        ym[q] = z[q, yn] + yrl[q]
        send(ym.at[q], yrm.at[q], d_send.at[2, q], yrm_recv.at[q], to_yn)
    x_copy.wait()

    def store(q, xx, yy, core, value):
        rows = pl.ds(pl.multiple_of((xx * RING + yy) * block_rows, block_rows), block_rows)
        cols = pl.ds(pl.multiple_of(core * cols_core + q * cols_sub, LANES), cols_sub)
        out_ref[rows, cols] = value.astype(jnp.bfloat16)

    def slot(q, first, second):
        return (first, second) if q == 0 else (second, first)

    ahead = ((to_xn, to_xp), (to_yn, to_yp))
    first_now, first_n, first_p, first_o = (x, y), (xn, yn), (xp, yp), (xo, yo)

    def push(q, first, second, kind, where):
        xx, yy = slot(q, first, second)
        send(g.at[q, xx, yy], g.at[q, xx, yy], g_send.at[q, xx, yy, kind], g_recv.at[q, xx, yy], where)

    def share(q, first, second):
        xx, yy = slot(q, first, second)
        send(g.at[q, xx, yy], gp.at[q, xx, yy], gp_send.at[q, xx, yy], gp_recv.at[q, xx, yy], partner)

    def receive(q, first, second):
        xx, yy = slot(q, first, second)
        arrived(g.at[q, xx, yy], g_recv.at[q, xx, yy])

    def keep(q, first, second):
        xx, yy = slot(q, first, second)
        store(q, xx, yy, c, g[q, xx, yy])

    for q in range(SUBS):
        arrived(yrd.at[q], yrd_recv.at[q])
        arrived(yrm.at[q], yrm_recv.at[q])
        cols = pl.ds(q * cols_sub, cols_sub)
        bias = bo_ref[:, pl.ds(pl.multiple_of(c * cols_core + q * cols_sub, LANES), cols_sub)]
        summed = z[q, y] + yrd[q] + yrm[q]
        final = xbuf[:, cols].astype(jnp.float32) + summed + bias.astype(jnp.float32)
        g[q, x, y] = final.astype(jnp.bfloat16).astype(jnp.float32)
        for axis in (q, 1 - q):
            for kind in range(2):
                push(q, first_now[q], first_now[1 - q], 2 * (axis != q) + kind, ahead[axis][kind])
        share(q, first_now[q], first_now[1 - q])

    def spread(q, first, forward):
        other = 1 - q
        receive(q, first, first_now[other])
        if forward:
            push(q, first, first_now[other], 0, ahead[q][0])
        for kind in range(2):
            push(q, first, first_now[other], 2 + kind, ahead[other][kind])
        share(q, first, first_now[other])
        keep(q, first, first_now[other])

    def settle(q, first, second, forward):
        receive(q, first, second)
        if forward:
            push(q, first, second, 2, ahead[1 - q][0])
        share(q, first, second)
        keep(q, first, second)

    both = range(SUBS)
    for q in both:
        spread(q, first_p[q], True)
    for q in both:
        spread(q, first_n[q], False)
    for q in both:
        keep(q, first_now[q], first_now[1 - q])
    for q in both:
        settle(q, first_now[q], first_p[1 - q], True)
    for q in both:
        settle(q, first_now[q], first_n[1 - q], False)
    for q in both:
        spread(q, first_o[q], False)
    for first in (first_p, first_n):
        for q in both:
            settle(q, first[q], first_p[1 - q], True)
        for q in both:
            settle(q, first[q], first_n[1 - q], False)
    for q in both:
        settle(q, first_now[q], first_o[1 - q], False)
    for q in both:
        settle(q, first_o[q], first_p[1 - q], True)
    for q in both:
        settle(q, first_o[q], first_n[1 - q], False)
    for first in (first_p, first_n, first_o):
        for q in both:
            settle(q, first[q], first_o[1 - q], False)
    orders = [first_now, first_p, first_n, first_o]
    for xi in range(RING):
        for yi in range(RING):
            for q in both:
                xx, yy = slot(q, orders[xi][q], orders[yi][1 - q])
                arrived(gp.at[q, xx, yy], gp_recv.at[q, xx, yy])
                store(q, xx, yy, 1 - c, gp[q, xx, yy])
    for copy in sends:
        copy.wait_send()


def combine(p, sinks, hidden, b_o, w_o):
    seqs = p.shape[3] - 1
    heads = p.shape[4]
    num_seqs, d_model = hidden.shape
    cols_core = d_model // CORES
    cols_sub = cols_core // SUBS
    block_rows = num_seqs // (RING * RING)
    part = (seqs + 1, heads, LANES)
    f32, bf16 = jnp.float32, jnp.bfloat16
    dma = pltpu.SemaphoreType.DMA
    vmem = pl.BlockSpec(memory_space=pltpu.VMEM)
    hbm = pl.BlockSpec(memory_space=pl.ANY)
    chunk = (block_rows, cols_sub)
    return pl.pallas_call(
        functools.partial(combine_kernel, seqs),
        out_shape=jax.ShapeDtypeStruct((num_seqs, d_model), bf16),
        in_specs=[vmem, vmem, hbm, vmem, hbm],
        out_specs=vmem,
        scratch_shapes=[
            pltpu.VMEM((RING, SUBS) + part, f32),
            pltpu.VMEM((RING, SUBS) + part, f32),
            pltpu.VMEM((SUBS,) + part, f32),
            pltpu.VMEM((SUBS,) + part, f32),
            pltpu.VMEM((SUBS,) + part, f32),
            pltpu.VMEM((SUBS, seqs * heads, LANES), f32),
            pltpu.VMEM((SUBS, seqs * heads, LANES), f32),
            pltpu.VMEM((2, w_o.shape[0] // 2, cols_core), bf16),
            pltpu.VMEM((block_rows, cols_core), bf16),
            pltpu.VMEM((SUBS, RING) + chunk, f32),
            pltpu.VMEM((SUBS,) + chunk, f32),
            pltpu.VMEM((SUBS,) + chunk, f32),
            pltpu.VMEM((SUBS,) + chunk, f32),
            pltpu.VMEM((SUBS,) + chunk, f32),
            pltpu.VMEM((SUBS, RING, RING) + chunk, f32),
            pltpu.VMEM((SUBS, RING, RING) + chunk, f32),
            dma((2,)), dma((1,)), dma((RING, SUBS)), dma((RING, SUBS)), dma((3, SUBS)),
            dma((SUBS,)), dma((SUBS,)), dma((SUBS,)), dma((SUBS,)), dma((SUBS,)),
            dma((3, SUBS)), dma((SUBS,)), dma((SUBS,)), dma((SUBS,)),
            dma((SUBS, RING, RING, 4)), dma((SUBS, RING, RING)), dma((SUBS, RING, RING)), dma((SUBS, RING, RING)),
        ],
        compiler_params=pltpu.CompilerParams(collective_id=0, has_side_effects=True, vmem_limit_bytes=48 * 2**20),
        cost_estimate=pl.CostEstimate(flops=2 * num_seqs // RING * w_o.shape[0] * cols_core, bytes_accessed=30 * 2**20, transcendentals=0),
        name="combine",
    )(p, sinks, hidden, b_o, w_o)


def front_kernel(
    logit_scale, x_hbm, len_hbm, cos_hbm, sin_hbm, k_hbm, v_hbm, gain_hbm, w_hbm, bias_hbm, sink_hbm,
    p_ref, k_out, v_out,
    xbuf, lens, cos, sin, gain, bias, sinks, hbuf, wide, narrow, wide_even, narrow_even, wide_odd, narrow_odd,
    acc, qs, kn, vn, kbuf, vbuf,
    in_sem, w_sem, n_sem, k_sem, v_sem, ko_sem, vo_sem,
):
    num_seqs, d_model = x_hbm.shape
    kv = w_hbm.shape[1]
    tiles = w_hbm.shape[2] // LANES
    heads = tiles - 2
    slots, depth = wide.shape[:2]
    quarter = depth // 4
    chunks = d_model // depth
    blocks, seqs = p_ref.shape[0], p_ref.shape[2] - 1
    ctx2 = k_hbm.shape[1]
    split = heads * LANES

    def w_copies(chunk, slot):
        first = pl.multiple_of(chunk * depth, depth)
        copies = [pltpu.make_async_copy(w_hbm.at[pl.ds(first, depth), :, pl.ds(0, split)], wide.at[slot], w_sem.at[slot])]
        for j in range(4):
            copies.append(pltpu.make_async_copy(
                w_hbm.at[pl.ds(first + j * quarter, quarter), :, pl.ds(split, 2 * LANES)],
                narrow.at[slot, :, :, pl.ds(j * 2 * LANES, 2 * LANES)], n_sem.at[slot]))
        return copies

    def w_start(chunk, slot):
        for copy in w_copies(chunk, slot):
            copy.start()

    def w_wait(chunk, slot):
        for copy in w_copies(chunk, slot):
            copy.wait()

    small = [
        pltpu.make_async_copy(src, dst, in_sem.at[i])
        for i, (src, dst) in enumerate((
            (x_hbm, xbuf), (gain_hbm, gain), (len_hbm, lens), (cos_hbm, cos), (sin_hbm, sin), (bias_hbm, bias), (sink_hbm, sinks)))
    ]
    for copy in small:
        copy.start()
    for slot in range(slots):
        w_start(slot, slot)

    def cache_copy(hbm, buf, sem, block, out):
        rows = pl.ds(block * seqs, seqs)
        src, dst = hbm.at[rows], buf.at[rows]
        return pltpu.make_async_copy(dst, src, sem.at[block]) if out else pltpu.make_async_copy(src, dst, sem.at[block])

    small[0].wait()
    small[1].wait()
    square = jnp.zeros((num_seqs, LANES), jnp.float32)
    for t in range(d_model // LANES):
        xt = xbuf[:, t * LANES : (t + 1) * LANES].astype(jnp.float32)
        square += xt * xt
    inv_rms = lax.rsqrt(jnp.sum(square, axis=-1, keepdims=True) / d_model + NORM_EPS)
    for t in range(d_model // LANES):
        xt = xbuf[:, t * LANES : (t + 1) * LANES].astype(jnp.float32)
        ht = (xt * inv_rms * gain[:, t * LANES : (t + 1) * LANES].astype(jnp.float32)).astype(jnp.bfloat16)
        place = t * LANES % depth
        hbuf[t * LANES // depth, :, place : place + LANES] = ht
    acc[...] = jnp.zeros_like(acc)

    def relayout(slot, wide_rows, narrow_rows):
        for ref, rows, count in ((wide, wide_rows, depth), (narrow, narrow_rows, quarter)):
            for i in range(count):
                value = ref[slot, i].astype(jnp.float32)
                for k in range(kv):
                    rows[k, pl.ds(i, heads, stride=count + 1), :] = value[k : k + 1].reshape(heads, LANES)

    def multiply(chunk, wide_rows, narrow_rows):
        lhs = hbuf[chunk]
        for k in range(kv):
            for t in range(0, tiles, 2):
                if t < heads:
                    pair = [wide_rows[k, pl.ds((t + j) * (depth + 1), depth), :] for j in range(2)]
                else:
                    pair = [jnp.concatenate([
                        narrow_rows[k, pl.ds((2 * i + j) * (quarter + 1), quarter), :] for i in range(4)], axis=0) for j in range(2)]
                rhs = jnp.concatenate(pair, axis=1).astype(jnp.bfloat16)
                cols = slice(t * LANES, (t + 2) * LANES)
                acc[k, :, cols] += jnp.dot(lhs, rhs, preferred_element_type=jnp.float32)

    w_wait(0, 0)
    relayout(0, wide_even, narrow_even)

    @pl.loop(0, chunks // 2)
    def _(i):
        even = 2 * i

        @pl.when(even + slots < chunks)
        def _():
            w_start(even + slots, lax.rem(even, slots))

        odd = even + 1
        w_wait(odd, lax.rem(odd, slots))
        relayout(lax.rem(odd, slots), wide_odd, narrow_odd)
        multiply(even, wide_even, narrow_even)

        @pl.when(odd + slots < chunks)
        def _():
            w_start(odd + slots, lax.rem(odd, slots))

        @pl.when(even + 2 + slots == chunks)
        def _():
            for block in range(blocks):
                cache_copy(k_hbm, kbuf, k_sem, block, False).start()
                cache_copy(v_hbm, vbuf, v_sem, block, False).start()

        later = lax.rem(even + 2, slots)

        @pl.when(even + 2 < chunks)
        def _():
            w_wait(even + 2, later)

        relayout(later, wide_even, narrow_even)
        multiply(odd, wide_odd, narrow_odd)

    for copy in small[2:]:
        copy.wait()
    cos_t = jnp.transpose(jnp.concatenate([cos[...], cos[...]], axis=0))
    sin_t = jnp.transpose(jnp.concatenate([-sin[...], sin[...]], axis=0))

    def rotate(t):
        return t * cos_t + pltpu.roll(t, HALF, 1) * sin_t

    def rounded(t):
        return t.astype(jnp.bfloat16).astype(jnp.float32)

    for k in range(kv):
        for t in range(tiles):
            cols = slice(t * LANES, (t + 1) * LANES)
            value = acc[k, :, cols] + bias[k : k + 1, cols].astype(jnp.float32)
            if t < heads:
                qs[pl.ds(k * heads + t, num_seqs, stride=kv * heads + 1), :] = rotate(value)
            elif t == heads:
                kn[pl.ds(k, num_seqs, stride=kv), :] = rotate(value)
            else:
                vn[pl.ds(k, num_seqs, stride=kv), :] = value

    q_rows = kv * heads
    base = lax.axis_index("sp") * (ctx2 // kv)
    row = lax.broadcasted_iota(jnp.int32, (q_rows, LANES), 0)
    lane = lax.broadcasted_iota(jnp.int32, (q_rows, LANES), 1)
    assert ctx2 == LANES
    position = jnp.where(lane % kv == row // heads, lane // kv + base, jnp.iinfo(jnp.int32).max)
    sink = jnp.zeros((q_rows, LANES), jnp.float32)
    for i in range(q_rows):
        sink = jnp.where(row == i, sinks[i], sink)
    sink_col = jnp.max(sink, axis=-1, keepdims=True)
    group = 16
    group_row = lax.broadcasted_iota(jnp.int32, (group, LANES), 0)

    @pl.loop(0, blocks)
    def _(block):
        cache_copy(k_hbm, kbuf, k_sem, block, False).wait()
        cache_copy(v_hbm, vbuf, v_sem, block, False).wait()
        stats = jnp.zeros((q_rows, LANES), jnp.float32)
        for i in range(seqs):
            b = block * seqs + i
            n = lens[b]
            local = n - base
            here = jnp.logical_and(local >= 0, local < ctx2 // kv)
            place = jnp.where(here, local * kv, 0)
            start = pl.multiple_of(place // group * group, group)
            target = jnp.where(here, place - start, group)
            for buf, new in ((kbuf, kn), (vbuf, vn)):
                fresh = new[pl.ds(b * kv, kv), :]
                value = buf[b, pl.ds(start, group), :].astype(jnp.float32)
                for k in range(kv):
                    value = jnp.where(group_row == target + k, fresh[k : k + 1], value)
                buf[b, pl.ds(start, group), :] = value.astype(jnp.bfloat16)
        for i in range(seqs):
            b = block * seqs + i
            q = qs[pl.ds(b * (q_rows + 1), q_rows), :].astype(jnp.bfloat16)
            logits = lax.dot_general(q, kbuf[b], (((1,), (1,)), ((), ())), preferred_element_type=jnp.float32) * logit_scale
            logits = jnp.where(position <= lens[b], logits, -jnp.inf)
            top = jnp.maximum(jnp.max(logits, axis=-1, keepdims=True), sink_col)
            weights = jnp.exp(logits - top)
            total = jnp.sum(weights, axis=-1, keepdims=True)
            numer = jnp.dot(weights.astype(jnp.bfloat16), vbuf[b], preferred_element_type=jnp.float32)
            for k in range(kv):
                p_ref[block, k, i] = numer[k * heads : (k + 1) * heads]
            stats = jnp.where(lane == i, top, jnp.where(lane == HALF + i, total, stats))
        for k in range(kv):
            p_ref[block, k, seqs] = stats[k * heads : (k + 1) * heads]
        cache_copy(k_out, kbuf, ko_sem, block, True).start()
        cache_copy(v_out, vbuf, vo_sem, block, True).start()

    for block in range(blocks):
        cache_copy(k_out, kbuf, ko_sem, block, True).wait()
        cache_copy(v_out, vbuf, vo_sem, block, True).wait()


def front(hidden, seq_lens, cos_t, sin_t, k_cache, v_cache, gain, w_qkv, b_qkv, sinks):
    num_seqs, d_model = hidden.shape
    kv, qkv = w_qkv.shape[1:]
    tiles = qkv // LANES
    heads = tiles - 2
    seqs = num_seqs // (RING * SUBS)
    ctx2 = k_cache.shape[1]
    depth, slots = 256, 6
    quarter = depth // 4
    f32, bf16 = jnp.float32, jnp.bfloat16
    dma = pltpu.SemaphoreType.DMA
    hbm = pl.BlockSpec(memory_space=pl.ANY)
    cache = jax.ShapeDtypeStruct(k_cache.shape, bf16)
    return pl.pallas_call(
        functools.partial(front_kernel, LANES ** -0.5),
        out_shape=(jax.ShapeDtypeStruct((RING * SUBS, kv, seqs + 1, heads, LANES), f32), cache, cache),
        in_specs=[hbm] * 10,
        out_specs=(pl.BlockSpec(memory_space=pltpu.VMEM), hbm, hbm),
        scratch_shapes=[
            pltpu.VMEM(hidden.shape, bf16),
            pltpu.SMEM(seq_lens.shape, jnp.int32),
            pltpu.VMEM(cos_t.shape, f32),
            pltpu.VMEM(sin_t.shape, f32),
            pltpu.VMEM(gain.shape, bf16),
            pltpu.VMEM(b_qkv.shape, bf16),
            pltpu.SMEM(sinks.shape, f32),
            pltpu.VMEM((d_model // depth, num_seqs, depth), bf16),
            pltpu.VMEM((slots, depth, kv, heads * LANES), bf16),
            pltpu.VMEM((slots, quarter, kv, heads * LANES), bf16),
            pltpu.VMEM((kv, heads * (depth + 1), LANES), f32),
            pltpu.VMEM((kv, heads * (quarter + 1), LANES), f32),
            pltpu.VMEM((kv, heads * (depth + 1), LANES), f32),
            pltpu.VMEM((kv, heads * (quarter + 1), LANES), f32),
            pltpu.VMEM((kv, num_seqs, qkv), f32),
            pltpu.VMEM((num_seqs * (kv * heads + 1), LANES), f32),
            pltpu.VMEM((num_seqs * kv, LANES), f32),
            pltpu.VMEM((num_seqs * kv, LANES), f32),
            pltpu.VMEM(k_cache.shape, bf16),
            pltpu.VMEM(v_cache.shape, bf16),
            dma((7,)), dma((slots,)), dma((slots,)), dma((RING * SUBS,)), dma((RING * SUBS,)), dma((RING * SUBS,)), dma((RING * SUBS,)),
        ],
        compiler_params=pltpu.CompilerParams(vmem_limit_bytes=44 * 2**20),
        cost_estimate=pl.CostEstimate(flops=4 * num_seqs * d_model * kv * qkv, bytes_accessed=50 * 2**20, transcendentals=0),
        name="front",
    )(*(pltpu.with_memory_space_constraint(a, pltpu.HBM) for a in (hidden, seq_lens, cos_t, sin_t, k_cache, v_cache, gain, w_qkv, b_qkv, sinks)))


def solution(mesh):
    cache_spec = P("dp", "sp", "tp", None)

    def block_step(hidden, seq_lens, rope_cos, rope_sin, k_cache, v_cache, norm_gain, w_qkv, b_qkv, sink_logits, w_o, b_o):
        num_seqs, ctx, kv, head_dim = k_cache.shape
        assert head_dim == LANES and mesh.shape["tp"] == RING and mesh.shape["sp"] == RING * CORES
        flat = (num_seqs, ctx * kv, head_dim)
        packed, k_out, v_out = front(
            hidden, seq_lens, rope_cos.T, rope_sin.T, k_cache.reshape(flat), v_cache.reshape(flat), norm_gain[None, :], w_qkv, b_qkv, sink_logits)
        packed = packed.reshape((RING, SUBS) + packed.shape[1:])
        sinks = jnp.broadcast_to(sink_logits[:, None], (sink_logits.shape[0], LANES))
        out_hidden = combine(packed, sinks, hidden, b_o[None, :], w_o)
        return out_hidden, k_out.reshape(k_cache.shape), v_out.reshape(v_cache.shape)

    return jax.shard_map(block_step, mesh=mesh, in_specs=(P("dp", None), P("dp"), P("dp", None), P("dp", None), cache_spec, cache_spec, P(None), P(None, "tp", None), P("tp", None), P("tp"), P("tp", None), P(None)), out_specs=(P("dp", None), cache_spec, cache_spec), check_vma=False)
```

```python
import functools

import jax
import jax.numpy as jnp
from jax import lax
from jax.experimental import pallas as pl
from jax.experimental.pallas import tpu as pltpu
from jax.sharding import PartitionSpec as P

NORM_EPS = 1e-5
MESH = pl.DeviceIdType.MESH
LANES = 128
HALF = LANES // 2
SUBS = 2
CORES = 2
RING = 4


def lane_column(tile, index):
    return tile[:, index : index + 1]


def merge_parts(parts, seqs):
    stats = [part[seqs] for part in parts]
    top = functools.reduce(jnp.maximum, stats)
    scales = [jnp.exp(stat - top) for stat in stats]
    total = sum(pltpu.roll(scale, HALF, 1) * stat for scale, stat in zip(scales, stats))
    return top, total, scales


def weighted_sums(columns, parts, seqs):
    loaded = [[part[i] for part in parts] for i in range(seqs)]
    scaled = [[column * value for column, value in zip(cols, values)] for cols, values in zip(columns, loaded)]
    return [functools.reduce(jnp.add, terms) for terms in scaled]


def merge_into(dst, parts, seqs):
    top, total, scales = merge_parts(parts, seqs)
    columns = [[lane_column(scale, i) for scale in scales] for i in range(seqs)]
    sums = weighted_sums(columns, parts, seqs)
    lane = lax.broadcasted_iota(jnp.int32, top.shape, 1)
    stats = jnp.where(lane < HALF, top, total)
    for i in range(seqs):
        dst[i] = sums[i]
    dst[seqs] = stats


def combine_kernel(
    seqs, p_ref, sink_ref, x_hbm, bo_ref, wo_hbm, out_ref,
    ra, cb, rl, rm, rd, own_o, other_o, wbuf, xbuf, z, yrl, ym, yrm, yrd, g, gp,
    w_sem, x_sem, a_send, a_recv, b_send, rl_recv, rm_recv, rd_recv, o_send, o_recv,
    d_send, yrl_recv, yrm_recv, yrd_recv, g_send, g_recv, gp_send, gp_recv,
):
    y = lax.axis_index("tp")
    sp = lax.axis_index("sp")
    x = sp // CORES
    c = sp % CORES
    step = 1 - 2 * c
    xn, xp, xo = (x + step + RING) % RING, (x - step + RING) % RING, (x + 2) % RING
    yn, yp, yo = (y + step + RING) % RING, (y - step + RING) % RING, (y + 2) % RING
    partner = {"sp": x * CORES + 1 - c}
    to_xn, to_xp = {"sp": xn * CORES + c}, {"sp": xp * CORES + c}
    to_yn, to_yp = {"tp": yn}, {"tp": yp}

    rows_half = wo_hbm.shape[0] // 2
    cols_core = wo_hbm.shape[1] // CORES
    cols_sub = cols_core // SUBS
    heads = p_ref.shape[4]
    block_rows = z.shape[2]

    w_copies = []
    for k in range(2):
        rows = (c if k == 0 else 1 - c) * rows_half
        copy = pltpu.make_async_copy(
            wo_hbm.at[pl.ds(pl.multiple_of(rows, LANES), rows_half), pl.ds(pl.multiple_of(c * cols_core, LANES), cols_core)],
            wbuf.at[k], w_sem.at[k])
        copy.start()
        w_copies.append(copy)
    row0 = pl.multiple_of((x * RING + y) * block_rows, block_rows)
    x_copy = pltpu.make_async_copy(
        x_hbm.at[pl.ds(row0, block_rows), pl.ds(pl.multiple_of(c * cols_core, LANES), cols_core)], xbuf, x_sem.at[0])
    x_copy.start()

    barrier = pltpu.get_barrier_semaphore()
    for where in (partner, to_xn, to_xp, to_yn, to_yp):
        pl.semaphore_signal(barrier, inc=1, device_id=where, device_id_type=MESH)
    pl.semaphore_wait(barrier, 5)

    sends = []

    def send(src, dst, send_sem, recv_sem, where):
        copy = pltpu.make_async_remote_copy(
            src_ref=src, dst_ref=dst, send_sem=send_sem, recv_sem=recv_sem, device_id=where, device_id_type=MESH)
        copy.start()
        sends.append(copy)

    def arrived(dst, recv_sem):
        pltpu.make_async_remote_copy(
            src_ref=dst, dst_ref=dst, send_sem=recv_sem, recv_sem=recv_sem, device_id=partner, device_id_type=MESH).wait_recv()

    for k, b in enumerate((xo, xp, xn, x)):
        for s in range(SUBS):
            send(p_ref.at[b, s, 1 - c], ra.at[b, s], a_send.at[k, s], a_recv.at[b, s], partner)

    for s in range(SUBS):
        arrived(ra.at[xo, s], a_recv.at[xo, s])
        merge_into(cb.at[0, s], (p_ref.at[xo, s, c], ra.at[xo, s]), seqs)
        send(cb.at[0, s], rl.at[s], b_send.at[0, s], rl_recv.at[s], to_xn)
    for s in range(SUBS):
        arrived(ra.at[xp, s], a_recv.at[xp, s])
        merge_into(cb.at[1, s], (p_ref.at[xp, s, c], ra.at[xp, s]), seqs)
        send(cb.at[1, s], rd.at[s], b_send.at[1, s], rd_recv.at[s], to_xp)
    for s in range(SUBS):
        arrived(ra.at[xn, s], a_recv.at[xn, s])
        arrived(rl.at[s], rl_recv.at[s])
        merge_into(cb.at[2, s], (p_ref.at[xn, s, c], ra.at[xn, s], rl.at[s]), seqs)
        send(cb.at[2, s], rm.at[s], b_send.at[2, s], rm_recv.at[s], to_xn)
    for s in range(SUBS):
        arrived(ra.at[x, s], a_recv.at[x, s])
        merge_into(cb.at[3, s], (p_ref.at[x, s, c], ra.at[x, s]), seqs)
    sink = sink_ref[pl.ds(pl.multiple_of(c * heads, heads), heads), :]
    for s in range(SUBS):
        arrived(rd.at[s], rd_recv.at[s])
        arrived(rm.at[s], rm_recv.at[s])
        parts = (cb.at[3, s], rd.at[s], rm.at[s])
        top, total, scales = merge_parts(parts, seqs)
        inverse = 1.0 / (pltpu.roll(total, HALF, 1) + jnp.exp(sink - top))
        columns = [[lane_column(scale * inverse, i) for scale in scales] for i in range(seqs)]
        outs = [out.astype(jnp.bfloat16).astype(jnp.float32) for out in weighted_sums(columns, parts, seqs)]
        for i in range(seqs):
            own_o[s, pl.ds(i * heads, heads), :] = outs[i]
        send(own_o.at[s], other_o.at[s], o_send.at[s], o_recv.at[s], partner)

    def head_rows(ref):
        columns = []
        for h in range(heads):
            columns.append(jnp.concatenate(
                [ref[s, pl.ds(h, seqs, stride=heads), :] for s in range(SUBS)], axis=0).astype(jnp.bfloat16))
        return jnp.concatenate(columns, axis=1)

    own_rows = head_rows(own_o)
    w_copies[0].wait()
    for q in range(SUBS):
        part = jnp.dot(own_rows, wbuf[0, :, pl.ds(q * cols_sub, cols_sub)], preferred_element_type=jnp.float32)
        for r in range(RING):
            z[q, r] = part[r * block_rows : (r + 1) * block_rows]
    for s in range(SUBS):
        arrived(other_o.at[s], o_recv.at[s])
    other_rows = head_rows(other_o)
    w_copies[1].wait()
    for q in range(SUBS):
        part = jnp.dot(other_rows, wbuf[1, :, pl.ds(q * cols_sub, cols_sub)], preferred_element_type=jnp.float32)
        for r in range(RING):
            z[q, r] += part[r * block_rows : (r + 1) * block_rows]
        send(z.at[q, yo], yrl.at[q], d_send.at[0, q], yrl_recv.at[q], to_yn)
        send(z.at[q, yp], yrd.at[q], d_send.at[1, q], yrd_recv.at[q], to_yp)
    for q in range(SUBS):
        arrived(yrl.at[q], yrl_recv.at[q])
        ym[q] = z[q, yn] + yrl[q]
        send(ym.at[q], yrm.at[q], d_send.at[2, q], yrm_recv.at[q], to_yn)
    x_copy.wait()

    def store(q, xx, yy, core, value):
        rows = pl.ds(pl.multiple_of((xx * RING + yy) * block_rows, block_rows), block_rows)
        cols = pl.ds(pl.multiple_of(core * cols_core + q * cols_sub, LANES), cols_sub)
        out_ref[rows, cols] = value.astype(jnp.bfloat16)

    def slot(q, first, second):
        return (first, second) if q == 0 else (second, first)

    ahead = ((to_xn, to_xp), (to_yn, to_yp))
    first_now, first_n, first_p, first_o = (x, y), (xn, yn), (xp, yp), (xo, yo)

    def push(q, first, second, kind, where):
        xx, yy = slot(q, first, second)
        send(g.at[q, xx, yy], g.at[q, xx, yy], g_send.at[q, xx, yy, kind], g_recv.at[q, xx, yy], where)

    def share(q, first, second):
        xx, yy = slot(q, first, second)
        send(g.at[q, xx, yy], gp.at[q, xx, yy], gp_send.at[q, xx, yy], gp_recv.at[q, xx, yy], partner)

    def receive(q, first, second):
        xx, yy = slot(q, first, second)
        arrived(g.at[q, xx, yy], g_recv.at[q, xx, yy])

    def keep(q, first, second):
        xx, yy = slot(q, first, second)
        store(q, xx, yy, c, g[q, xx, yy])

    for q in range(SUBS):
        arrived(yrd.at[q], yrd_recv.at[q])
        arrived(yrm.at[q], yrm_recv.at[q])
        cols = pl.ds(q * cols_sub, cols_sub)
        bias = bo_ref[:, pl.ds(pl.multiple_of(c * cols_core + q * cols_sub, LANES), cols_sub)]
        summed = z[q, y] + yrd[q] + yrm[q]
        final = xbuf[:, cols].astype(jnp.float32) + summed + bias.astype(jnp.float32)
        g[q, x, y] = final.astype(jnp.bfloat16).astype(jnp.float32)
        for axis in (q, 1 - q):
            for kind in range(2):
                push(q, first_now[q], first_now[1 - q], 2 * (axis != q) + kind, ahead[axis][kind])
        share(q, first_now[q], first_now[1 - q])

    def spread(q, first, forward):
        other = 1 - q
        receive(q, first, first_now[other])
        if forward:
            push(q, first, first_now[other], 0, ahead[q][0])
        for kind in range(2):
            push(q, first, first_now[other], 2 + kind, ahead[other][kind])
        share(q, first, first_now[other])
        keep(q, first, first_now[other])

    def settle(q, first, second, forward):
        receive(q, first, second)
        if forward:
            push(q, first, second, 2, ahead[1 - q][0])
        share(q, first, second)
        keep(q, first, second)

    both = range(SUBS)
    for q in both:
        spread(q, first_p[q], True)
    for q in both:
        spread(q, first_n[q], False)
    for q in both:
        keep(q, first_now[q], first_now[1 - q])
    for q in both:
        settle(q, first_now[q], first_p[1 - q], True)
    for q in both:
        settle(q, first_now[q], first_n[1 - q], False)
    for q in both:
        spread(q, first_o[q], False)
    for first in (first_p, first_n):
        for q in both:
            settle(q, first[q], first_p[1 - q], True)
        for q in both:
            settle(q, first[q], first_n[1 - q], False)
    for q in both:
        settle(q, first_now[q], first_o[1 - q], False)
    for q in both:
        settle(q, first_o[q], first_p[1 - q], True)
    for q in both:
        settle(q, first_o[q], first_n[1 - q], False)
    for first in (first_p, first_n, first_o):
        for q in both:
            settle(q, first[q], first_o[1 - q], False)
    orders = [first_now, first_p, first_n, first_o]
    for xi in range(RING):
        for yi in range(RING):
            for q in both:
                xx, yy = slot(q, orders[xi][q], orders[yi][1 - q])
                arrived(gp.at[q, xx, yy], gp_recv.at[q, xx, yy])
                store(q, xx, yy, 1 - c, gp[q, xx, yy])
    for copy in sends:
        copy.wait_send()


def combine(p, sinks, hidden, b_o, w_o):
    seqs = p.shape[3] - 1
    heads = p.shape[4]
    num_seqs, d_model = hidden.shape
    cols_core = d_model // CORES
    cols_sub = cols_core // SUBS
    block_rows = num_seqs // (RING * RING)
    part = (seqs + 1, heads, LANES)
    f32, bf16 = jnp.float32, jnp.bfloat16
    dma = pltpu.SemaphoreType.DMA
    vmem = pl.BlockSpec(memory_space=pltpu.VMEM)
    hbm = pl.BlockSpec(memory_space=pl.ANY)
    chunk = (block_rows, cols_sub)
    return pl.pallas_call(
        functools.partial(combine_kernel, seqs),
        out_shape=jax.ShapeDtypeStruct((num_seqs, d_model), bf16),
        in_specs=[vmem, vmem, hbm, vmem, hbm],
        out_specs=vmem,
        scratch_shapes=[
            pltpu.VMEM((RING, SUBS) + part, f32),
            pltpu.VMEM((RING, SUBS) + part, f32),
            pltpu.VMEM((SUBS,) + part, f32),
            pltpu.VMEM((SUBS,) + part, f32),
            pltpu.VMEM((SUBS,) + part, f32),
            pltpu.VMEM((SUBS, seqs * heads, LANES), f32),
            pltpu.VMEM((SUBS, seqs * heads, LANES), f32),
            pltpu.VMEM((2, w_o.shape[0] // 2, cols_core), bf16),
            pltpu.VMEM((block_rows, cols_core), bf16),
            pltpu.VMEM((SUBS, RING) + chunk, f32),
            pltpu.VMEM((SUBS,) + chunk, f32),
            pltpu.VMEM((SUBS,) + chunk, f32),
            pltpu.VMEM((SUBS,) + chunk, f32),
            pltpu.VMEM((SUBS,) + chunk, f32),
            pltpu.VMEM((SUBS, RING, RING) + chunk, f32),
            pltpu.VMEM((SUBS, RING, RING) + chunk, f32),
            dma((2,)), dma((1,)), dma((RING, SUBS)), dma((RING, SUBS)), dma((3, SUBS)),
            dma((SUBS,)), dma((SUBS,)), dma((SUBS,)), dma((SUBS,)), dma((SUBS,)),
            dma((3, SUBS)), dma((SUBS,)), dma((SUBS,)), dma((SUBS,)),
            dma((SUBS, RING, RING, 4)), dma((SUBS, RING, RING)), dma((SUBS, RING, RING)), dma((SUBS, RING, RING)),
        ],
        compiler_params=pltpu.CompilerParams(collective_id=0, has_side_effects=True, vmem_limit_bytes=48 * 2**20),
        cost_estimate=pl.CostEstimate(flops=2 * num_seqs // RING * w_o.shape[0] * cols_core, bytes_accessed=30 * 2**20, transcendentals=0),
        name="combine",
    )(p, sinks, hidden, b_o, w_o)


def front_kernel(
    logit_scale, x_hbm, len_hbm, cos_hbm, sin_hbm, k_hbm, v_hbm, gain_hbm, w_hbm, bias_hbm, sink_hbm,
    p_ref, k_out, v_out,
    xbuf, lens, cos, sin, gain, bias, sinks, hexp, wbuf, acc, qs, kn, vn, kbuf, vbuf,
    in_sem, w_sem, k_sem, v_sem, ko_sem, vo_sem,
):
    num_seqs, d_model = x_hbm.shape
    kv = w_hbm.shape[1]
    qkv = w_hbm.shape[2]
    tiles = qkv // LANES
    heads = tiles - 2
    slots, depth2, _ = wbuf.shape
    chunks = d_model * kv // depth2
    blocks, _, seqs1 = p_ref.shape[0], p_ref.shape[1], p_ref.shape[2]
    seqs = seqs1 - 1
    ctx2 = k_hbm.shape[1]
    w_rows = w_hbm.reshape(d_model * kv, qkv)

    def w_copy(chunk, slot):
        return pltpu.make_async_copy(
            w_rows.at[pl.ds(pl.multiple_of(chunk * depth2, depth2), depth2), :], wbuf.at[slot], w_sem.at[slot])

    def w_start(chunk, slot):
        w_copy(chunk, slot).start()

    small = [
        pltpu.make_async_copy(src, dst, in_sem.at[i])
        for i, (src, dst) in enumerate((
            (x_hbm, xbuf), (gain_hbm, gain), (len_hbm, lens), (cos_hbm, cos), (sin_hbm, sin), (bias_hbm, bias), (sink_hbm, sinks)))
    ]
    for copy in small:
        copy.start()
    for slot in range(slots - 1):
        w_start(slot, slot)

    def cache_copy(hbm, buf, sem, block, out):
        rows = pl.ds(block * seqs, seqs)
        src, dst = hbm.at[rows], buf.at[rows]
        return pltpu.make_async_copy(dst, src, sem.at[block]) if out else pltpu.make_async_copy(src, dst, sem.at[block])

    small[0].wait()
    small[1].wait()
    row = lax.broadcasted_iota(jnp.int32, (LANES, kv * LANES), 0)
    col = lax.broadcasted_iota(jnp.int32, (LANES, kv * LANES), 1)
    picks = [(col == row * kv + k).astype(jnp.bfloat16) for k in range(kv)]
    square = jnp.zeros((num_seqs, LANES), jnp.float32)
    for t in range(d_model // LANES):
        xt = xbuf[:, t * LANES : (t + 1) * LANES].astype(jnp.float32)
        square += xt * xt
    inv_rms = lax.rsqrt(jnp.sum(square, axis=-1, keepdims=True) / d_model + NORM_EPS)
    per_chunk = depth2 // (kv * LANES)
    for t in range(d_model // LANES):
        xt = xbuf[:, t * LANES : (t + 1) * LANES].astype(jnp.float32)
        ht = (xt * inv_rms * gain[:, t * LANES : (t + 1) * LANES].astype(jnp.float32)).astype(jnp.bfloat16)
        for k in range(kv):
            spread = jnp.dot(ht, picks[k], preferred_element_type=jnp.float32).astype(jnp.bfloat16)
            place = t % per_chunk * kv * LANES
            hexp[t // per_chunk, k * num_seqs : (k + 1) * num_seqs, place : place + kv * LANES] = spread
    acc[...] = jnp.zeros_like(acc)

    @pl.loop(0, chunks)
    def _(chunk):
        slot = lax.rem(chunk, slots)

        @pl.when(chunk + slots - 1 < chunks)
        def _():
            w_start(chunk + slots - 1, lax.rem(chunk + slots - 1, slots))

        @pl.when(chunk == chunks - slots)
        def _():
            for block in range(blocks):
                cache_copy(k_hbm, kbuf, k_sem, block, False).start()
                cache_copy(v_hbm, vbuf, v_sem, block, False).start()

        w_copy(chunk, slot).wait()
        lhs = hexp.at[chunk]
        for t in range(0, tiles, 2):
            cols = slice(t * LANES, (t + 2) * LANES)
            acc[:, cols] += jnp.dot(lhs[...], wbuf[slot, :, cols], preferred_element_type=jnp.float32)

    for copy in small[2:]:
        copy.wait()
    cos_t = jnp.transpose(jnp.concatenate([cos[...], cos[...]], axis=0))
    sin_t = jnp.transpose(jnp.concatenate([-sin[...], sin[...]], axis=0))

    def rotate(t):
        return t * cos_t + pltpu.roll(t, HALF, 1) * sin_t

    def rounded(t):
        return t.astype(jnp.bfloat16).astype(jnp.float32)

    for k in range(kv):
        for t in range(tiles):
            cols = slice(t * LANES, (t + 1) * LANES)
            value = acc[k * num_seqs : (k + 1) * num_seqs, cols] + bias[k : k + 1, cols].astype(jnp.float32)
            if t < heads:
                qs[pl.ds(k * heads + t, num_seqs, stride=kv * heads + 1), :] = rotate(value)
            elif t == heads:
                kn[pl.ds(k, num_seqs, stride=kv), :] = rotate(value)
            else:
                vn[pl.ds(k, num_seqs, stride=kv), :] = value

    q_rows = kv * heads
    base = lax.axis_index("sp") * (ctx2 // kv)
    row = lax.broadcasted_iota(jnp.int32, (q_rows, LANES), 0)
    lane = lax.broadcasted_iota(jnp.int32, (q_rows, LANES), 1)
    assert ctx2 == LANES
    position = jnp.where(lane % kv == row // heads, lane // kv + base, jnp.iinfo(jnp.int32).max)
    sink = jnp.zeros((q_rows, LANES), jnp.float32)
    for i in range(q_rows):
        sink = jnp.where(row == i, sinks[i], sink)
    sink_col = jnp.max(sink, axis=-1, keepdims=True)
    group = 16
    wave = 16
    group_row = lax.broadcasted_iota(jnp.int32, (group, LANES), 0)

    @pl.loop(0, blocks)
    def _(block):
        cache_copy(k_hbm, kbuf, k_sem, block, False).wait()
        cache_copy(v_hbm, vbuf, v_sem, block, False).wait()
        stats = jnp.zeros((q_rows, LANES), jnp.float32)
        updates = []
        for i in range(seqs):
            b = block * seqs + i
            local = lens[b] - base
            here = jnp.logical_and(local >= 0, local < ctx2 // kv)
            place = jnp.where(here, local * kv, 0)
            start = pl.multiple_of(place // group * group, group)
            target = jnp.where(here, place - start, group)
            for buf, new in ((kbuf, kn), (vbuf, vn)):
                updates.append((buf, b, start, target, new[pl.ds(b * kv, kv), :], buf[b, pl.ds(start, group), :]))
        fresh_groups = []
        for _, _, _, target, fresh, old in updates:
            value = old.astype(jnp.float32)
            for k in range(kv):
                value = jnp.where(group_row == target + k, fresh[k : k + 1], value)
            fresh_groups.append(value.astype(jnp.bfloat16))
        for (buf, b, start, _, _, _), value in zip(updates, fresh_groups):
            buf[b, pl.ds(start, group), :] = value
        for first in range(0, seqs, wave):
            members = range(first, first + wave)
            queries = [qs[pl.ds((block * seqs + i) * (q_rows + 1), q_rows), :].astype(jnp.bfloat16) for i in members]
            logits = [
                lax.dot_general(q, kbuf[block * seqs + i], (((1,), (1,)), ((), ())), preferred_element_type=jnp.float32)
                for i, q in zip(members, queries)]
            logits = [jnp.where(position <= lens[block * seqs + i], l * logit_scale, -jnp.inf) for i, l in zip(members, logits)]
            tops = [jnp.maximum(jnp.max(l, axis=-1, keepdims=True), sink_col) for l in logits]
            weights = [jnp.exp(l - top) for l, top in zip(logits, tops)]
            totals = [jnp.sum(w, axis=-1, keepdims=True) for w in weights]
            numers = [
                jnp.dot(w.astype(jnp.bfloat16), vbuf[block * seqs + i], preferred_element_type=jnp.float32)
                for i, w in zip(members, weights)]
            for i, numer, top, total in zip(members, numers, tops, totals):
                for k in range(kv):
                    p_ref[block, k, i] = numer[k * heads : (k + 1) * heads]
                stats = jnp.where(lane == i, top, jnp.where(lane == HALF + i, total, stats))
        for k in range(kv):
            p_ref[block, k, seqs] = stats[k * heads : (k + 1) * heads]
        cache_copy(k_out, kbuf, ko_sem, block, True).start()
        cache_copy(v_out, vbuf, vo_sem, block, True).start()

    for block in range(blocks):
        cache_copy(k_out, kbuf, ko_sem, block, True).wait()
        cache_copy(v_out, vbuf, vo_sem, block, True).wait()


def front(hidden, seq_lens, cos_t, sin_t, k_cache, v_cache, gain, w_qkv, b_qkv, sinks):
    num_seqs, d_model = hidden.shape
    kv, qkv = w_qkv.shape[1:]
    tiles = qkv // LANES
    heads = tiles - 2
    seqs = num_seqs // (RING * SUBS)
    ctx2 = k_cache.shape[1]
    depth2 = 1024
    chunks = d_model * kv // depth2
    slots = 4
    f32, bf16 = jnp.float32, jnp.bfloat16
    dma = pltpu.SemaphoreType.DMA
    hbm = pl.BlockSpec(memory_space=pl.ANY)
    cache = jax.ShapeDtypeStruct(k_cache.shape, bf16)
    return pl.pallas_call(
        functools.partial(front_kernel, LANES ** -0.5),
        out_shape=(jax.ShapeDtypeStruct((RING * SUBS, kv, seqs + 1, heads, LANES), f32), cache, cache),
        in_specs=[hbm] * 10,
        out_specs=(pl.BlockSpec(memory_space=pltpu.VMEM), hbm, hbm),
        scratch_shapes=[
            pltpu.VMEM(hidden.shape, bf16),
            pltpu.SMEM(seq_lens.shape, jnp.int32),
            pltpu.VMEM(cos_t.shape, f32),
            pltpu.VMEM(sin_t.shape, f32),
            pltpu.VMEM(gain.shape, bf16),
            pltpu.VMEM(b_qkv.shape, bf16),
            pltpu.SMEM(sinks.shape, f32),
            pltpu.VMEM((chunks, kv * num_seqs, depth2), bf16),
            pltpu.VMEM((slots, depth2, qkv), bf16),
            pltpu.VMEM((kv * num_seqs, qkv), f32),
            pltpu.VMEM((num_seqs * (kv * heads + 1), LANES), f32),
            pltpu.VMEM((num_seqs * kv, LANES), f32),
            pltpu.VMEM((num_seqs * kv, LANES), f32),
            pltpu.VMEM(k_cache.shape, bf16),
            pltpu.VMEM(v_cache.shape, bf16),
            dma((7,)), dma((slots,)), dma((RING * SUBS,)), dma((RING * SUBS,)), dma((RING * SUBS,)), dma((RING * SUBS,)),
        ],
        compiler_params=pltpu.CompilerParams(vmem_limit_bytes=44 * 2**20),
        cost_estimate=pl.CostEstimate(flops=4 * num_seqs * d_model * kv * qkv, bytes_accessed=50 * 2**20, transcendentals=0),
        name="front",
    )(*(pltpu.with_memory_space_constraint(a, pltpu.HBM) for a in (hidden, seq_lens, cos_t, sin_t, k_cache, v_cache, gain, w_qkv, b_qkv, sinks)))


def solution(mesh):
    cache_spec = P("dp", "sp", "tp", None)

    def block_step(hidden, seq_lens, rope_cos, rope_sin, k_cache, v_cache, norm_gain, w_qkv, b_qkv, sink_logits, w_o, b_o):
        num_seqs, ctx, kv, head_dim = k_cache.shape
        assert head_dim == LANES and mesh.shape["tp"] == RING and mesh.shape["sp"] == RING * CORES
        flat = (num_seqs, ctx * kv, head_dim)
        packed, k_out, v_out = front(
            hidden, seq_lens, rope_cos.T, rope_sin.T, k_cache.reshape(flat), v_cache.reshape(flat), norm_gain[None, :], w_qkv, b_qkv, sink_logits)
        packed = packed.reshape((RING, SUBS) + packed.shape[1:])
        sinks = jnp.broadcast_to(sink_logits[:, None], (sink_logits.shape[0], LANES))
        out_hidden = combine(packed, sinks, hidden, b_o[None, :], w_o)
        return out_hidden, k_out.reshape(k_cache.shape), v_out.reshape(v_cache.shape)

    return jax.shard_map(block_step, mesh=mesh, in_specs=(P("dp", None), P("dp"), P("dp", None), P("dp", None), cache_spec, cache_spec, P(None), P(None, "tp", None), P("tp", None), P("tp"), P("tp", None), P(None)), out_specs=(P("dp", None), cache_spec, cache_spec), check_vma=False)
```

```python
import functools

import jax
import jax.numpy as jnp
from jax import lax
from jax.experimental import pallas as pl
from jax.experimental.pallas import tpu as pltpu
from jax.sharding import PartitionSpec as P

NORM_EPS = 1e-5
MESH = pl.DeviceIdType.MESH
LANES = 128
HALF = LANES // 2
SUBS = 2
CORES = 2
FRONT_MIB = 34
COMBINE_MIB = 26
WAVE = 4
RING = 4


def lane_column(tile, index):
    return tile[:, index : index + 1]


def merge_parts(parts, seqs):
    stats = [part[seqs] for part in parts]
    top = functools.reduce(jnp.maximum, stats)
    scales = [jnp.exp(stat - top) for stat in stats]
    total = sum(pltpu.roll(scale, HALF, 1) * stat for scale, stat in zip(scales, stats))
    return top, total, scales


def weighted_sums(columns, parts, seqs):
    loaded = [[part[i] for part in parts] for i in range(seqs)]
    scaled = [[column * value for column, value in zip(cols, values)] for cols, values in zip(columns, loaded)]
    return [functools.reduce(jnp.add, terms) for terms in scaled]


def merge_into(dst, parts, seqs):
    top, total, scales = merge_parts(parts, seqs)
    columns = [[lane_column(scale, i) for scale in scales] for i in range(seqs)]
    sums = weighted_sums(columns, parts, seqs)
    lane = lax.broadcasted_iota(jnp.int32, top.shape, 1)
    stats = jnp.where(lane < HALF, top, total)
    for i in range(seqs):
        dst[i] = sums[i]
    dst[seqs] = stats


def combine_kernel(
    seqs, logit_scale, q_ref, k_ref, v_ref, lens, sink_ref, x_hbm, bo_hbm, wo_hbm, out_ref,
    p_ref, bo_ref, bias_rows, ra, cb, rl, rm, rd, own_o, other_o, wbuf, xbuf, z, yrl, ym, yrm, yrd, g, gp,
    w_sem, x_sem, a_send, a_recv, b_send, rl_recv, rm_recv, rd_recv, o_send, o_recv,
    d_send, yrl_recv, yrm_recv, yrd_recv, g_send, g_recv, gp_send, gp_recv,
):
    y = lax.axis_index("tp")
    sp = lax.axis_index("sp")
    x = sp // CORES
    c = sp % CORES
    step = 1 - 2 * c
    xn, xp, xo = (x + step + RING) % RING, (x - step + RING) % RING, (x + 2) % RING
    yn, yp, yo = (y + step + RING) % RING, (y - step + RING) % RING, (y + 2) % RING
    partner = {"sp": x * CORES + 1 - c}
    to_xn, to_xp = {"sp": xn * CORES + c}, {"sp": xp * CORES + c}
    to_yn, to_yp = {"tp": yn}, {"tp": yp}

    rows_half = wo_hbm.shape[0] // 2
    cols_core = wo_hbm.shape[1] // CORES
    cols_sub = cols_core // SUBS
    heads = p_ref.shape[4]
    block_rows = z.shape[2]

    w_copies = []
    for k in range(2):
        rows = (c if k == 0 else 1 - c) * rows_half
        copy = pltpu.make_async_copy(
            wo_hbm.at[pl.ds(pl.multiple_of(rows, LANES), rows_half), pl.ds(pl.multiple_of(c * cols_core, LANES), cols_core)],
            wbuf.at[k], w_sem.at[k])
        copy.start()
        w_copies.append(copy)
    row0 = pl.multiple_of((x * RING + y) * block_rows, block_rows)
    x_copy = pltpu.make_async_copy(
        x_hbm.at[pl.ds(row0, block_rows), pl.ds(pl.multiple_of(c * cols_core, LANES), cols_core)], xbuf, x_sem.at[0])
    x_copy.start()
    bo_copy = pltpu.make_async_copy(bo_hbm, bo_ref, x_sem.at[1])
    bo_copy.start()

    barrier = pltpu.get_barrier_semaphore()
    for where in (partner, to_xn, to_xp, to_yn, to_yp):
        pl.semaphore_signal(barrier, inc=1, device_id=where, device_id_type=MESH)
    pl.semaphore_wait(barrier, 5)

    def send(src, dst, send_sem, recv_sem, where):
        copy = pltpu.make_async_remote_copy(
            src_ref=src, dst_ref=dst, send_sem=send_sem, recv_sem=recv_sem, device_id=where, device_id_type=MESH)
        copy.start()

    def sent(shape_of, send_sem):
        pltpu.make_async_remote_copy(
            src_ref=shape_of, dst_ref=shape_of, send_sem=send_sem, recv_sem=send_sem, device_id=partner, device_id_type=MESH).wait_send()

    def arrived(dst, recv_sem):
        pltpu.make_async_remote_copy(
            src_ref=dst, dst_ref=dst, send_sem=recv_sem, recv_sem=recv_sem, device_id=partner, device_id_type=MESH).wait_recv()

    kv = p_ref.shape[2]
    q_rows = kv * heads
    ctx2 = k_ref.shape[1]
    row = lax.broadcasted_iota(jnp.int32, (q_rows, ctx2), 0)
    lane = lax.broadcasted_iota(jnp.int32, (q_rows, ctx2), 1)
    position = jnp.where(lane % kv == row // heads, lane // kv + sp * (ctx2 // kv), jnp.iinfo(jnp.int32).max)
    sinks = jnp.zeros((q_rows, LANES), jnp.float32)
    for i in range(q_rows):
        sinks = jnp.where(row == i, sink_ref[i], sinks)
    sink_col = jnp.max(sinks, axis=-1, keepdims=True)

    def attend(b, s):
        first = (b * SUBS + s) * seqs
        waves = [range(j, j + WAVE) for j in range(0, seqs, WAVE)]
        logits, tops, totals, weights, stats = {}, {}, {}, {}, jnp.zeros((q_rows, LANES), jnp.float32)
        for turn in range(len(waves) + 2):
            if turn < len(waves):
                for i in waves[turn]:
                    q = q_ref[pl.ds((first + i) * (q_rows + 1), q_rows), :].astype(jnp.bfloat16)
                    logits[i] = lax.dot_general(q, k_ref[first + i], (((1,), (1,)), ((), ())), preferred_element_type=jnp.float32)
            if 0 <= turn - 1 < len(waves):
                members = waves[turn - 1]
                for i in members:
                    logits[i] = jnp.where(position <= lens[first + i], logits[i] * logit_scale, -jnp.inf)
                for i in members:
                    tops[i] = jnp.maximum(jnp.max(logits[i], axis=-1, keepdims=True), sink_col)
                for i in members:
                    weights[i] = jnp.exp(logits[i] - tops[i])
                for i in members:
                    totals[i] = jnp.sum(weights[i], axis=-1, keepdims=True)
            if 0 <= turn - 2:
                members = waves[turn - 2]
                numers = [
                    jnp.dot(weights[i].astype(jnp.bfloat16), v_ref[first + i], preferred_element_type=jnp.float32) for i in members]
                for i, numer in zip(members, numers):
                    for k in range(kv):
                        p_ref[b, s, k, i] = numer[k * heads : (k + 1) * heads]
                    stats = jnp.where(lane == i, tops[i], jnp.where(lane == HALF + i, totals[i], stats))
        for k in range(kv):
            p_ref[b, s, k, seqs] = stats[k * heads : (k + 1) * heads]
        send(p_ref.at[b, s, 1 - c], ra.at[b, s], a_send.at[0], a_recv.at[b, s], partner)

    def attend_both(b):
        @pl.loop(0, SUBS)
        def _(s):
            attend(b, s)

    def relay(s):
        arrived(ra.at[xo, s], a_recv.at[xo, s])
        merge_into(cb.at[0, s], (p_ref.at[xo, s, c], ra.at[xo, s]), seqs)
        send(cb.at[0, s], rl.at[s], b_send.at[0], rl_recv.at[s], to_xn)

    def pass_on(s):
        arrived(ra.at[xn, s], a_recv.at[xn, s])
        arrived(rl.at[s], rl_recv.at[s])
        merge_into(cb.at[2, s], (p_ref.at[xn, s, c], ra.at[xn, s], rl.at[s]), seqs)
        send(cb.at[2, s], rm.at[s], b_send.at[0], rm_recv.at[s], to_xn)

    attend_both(xo)
    for s in range(SUBS):
        attend(xn, s)
        relay(s)
    attend_both(xp)
    for s in range(SUBS):
        arrived(ra.at[xp, s], a_recv.at[xp, s])
        merge_into(cb.at[1, s], (p_ref.at[xp, s, c], ra.at[xp, s]), seqs)
        send(cb.at[1, s], rd.at[s], b_send.at[0], rd_recv.at[s], to_xp)
    for s in range(SUBS):
        attend(x, s)
        pass_on(s)
    for s in range(SUBS):
        arrived(ra.at[x, s], a_recv.at[x, s])
        merge_into(cb.at[3, s], (p_ref.at[x, s, c], ra.at[x, s]), seqs)
    sink = jnp.zeros((heads, LANES), jnp.float32)
    head_row = lax.broadcasted_iota(jnp.int32, sink.shape, 0)
    for h in range(heads):
        sink = jnp.where(head_row == h, sink_ref[c * heads + h], sink)
    for s in range(SUBS):
        arrived(rd.at[s], rd_recv.at[s])
        arrived(rm.at[s], rm_recv.at[s])
        parts = (cb.at[3, s], rd.at[s], rm.at[s])
        top, total, scales = merge_parts(parts, seqs)
        inverse = 1.0 / (pltpu.roll(total, HALF, 1) + jnp.exp(sink - top))
        columns = [[lane_column(scale * inverse, i) for scale in scales] for i in range(seqs)]
        outs = [out.astype(jnp.bfloat16).astype(jnp.float32) for out in weighted_sums(columns, parts, seqs)]
        for i in range(seqs):
            own_o[s, pl.ds(i * heads, heads), :] = outs[i]
        send(own_o.at[s], other_o.at[s], o_send.at[0], o_recv.at[s], partner)

    def head_rows(ref):
        columns = []
        for h in range(heads):
            columns.append(jnp.concatenate(
                [ref[s, pl.ds(h, seqs, stride=heads), :] for s in range(SUBS)], axis=0).astype(jnp.bfloat16))
        return jnp.concatenate(columns, axis=1)

    own_rows = head_rows(own_o)
    w_copies[0].wait()
    for q in range(SUBS):
        part = jnp.dot(own_rows, wbuf[0, :, pl.ds(q * cols_sub, cols_sub)], preferred_element_type=jnp.float32)
        for r in range(RING):
            z[q, r] = part[r * block_rows : (r + 1) * block_rows]
    for s in range(SUBS):
        arrived(other_o.at[s], o_recv.at[s])
    other_rows = head_rows(other_o)
    w_copies[1].wait()
    for q in range(SUBS):
        part = jnp.dot(other_rows, wbuf[1, :, pl.ds(q * cols_sub, cols_sub)], preferred_element_type=jnp.float32)
        for r in range(RING):
            z[q, r] += part[r * block_rows : (r + 1) * block_rows]
        send(z.at[q, yo], yrl.at[q], d_send.at[0], yrl_recv.at[q], to_yn)
        send(z.at[q, yp], yrd.at[q], d_send.at[0], yrd_recv.at[q], to_yp)
    for q in range(SUBS):
        arrived(yrl.at[q], yrl_recv.at[q])
        ym[q] = z[q, yn] + yrl[q]
        send(ym.at[q], yrm.at[q], d_send.at[0], yrm_recv.at[q], to_yn)
    chunk = g.shape[3:]
    sent(ra, a_send.at[0])
    sent(cb.at[pl.ds(0, 3)], b_send.at[0])
    sent(own_o, o_send.at[0])
    sent(g.reshape((-1,) + chunk).at[pl.ds(0, 3 * SUBS)], d_send.at[0])
    x_copy.wait()
    bo_copy.wait()
    bias_rows[...] = bo_ref[...].astype(jnp.float32)

    def store(q, xx, yy, core, value):
        rows = pl.ds(pl.multiple_of((xx * RING + yy) * block_rows, block_rows), block_rows)
        cols = pl.ds(pl.multiple_of(core * cols_core + q * cols_sub, LANES), cols_sub)
        out_ref[rows, cols] = value.astype(jnp.bfloat16)

    def slot(q, first, second):
        return (first, second) if q == 0 else (second, first)

    ahead = ((to_xn, to_xp), (to_yn, to_yp))
    first_now, first_n, first_p, first_o = (x, y), (xn, yn), (xp, yp), (xo, yo)

    pushes = []

    def push(q, first, second, where):
        xx, yy = slot(q, first, second)
        pushes.append(q)
        send(g.at[q, xx, yy], g.at[q, xx, yy], g_send.at[0], g_recv.at[q, xx, yy], where)

    def share(q, first, second):
        xx, yy = slot(q, first, second)
        send(g.at[q, xx, yy], gp.at[q, xx, yy], gp_send.at[0], gp_recv.at[q, xx, yy], partner)

    def receive(q, first, second):
        xx, yy = slot(q, first, second)
        arrived(g.at[q, xx, yy], g_recv.at[q, xx, yy])

    def keep(q, first, second):
        xx, yy = slot(q, first, second)
        store(q, xx, yy, c, g[q, xx, yy])

    for q in range(SUBS):
        arrived(yrd.at[q], yrd_recv.at[q])
        arrived(yrm.at[q], yrm_recv.at[q])
        first_row = (c * cols_core + q * cols_sub) // LANES
        bias = jnp.concatenate([bias_rows[pl.ds(first_row + t, 1), :] for t in range(cols_sub // LANES)], axis=1)
        summed = z[q, y] + yrd[q] + yrm[q]
        final = xbuf[:, pl.ds(q * cols_sub, cols_sub)].astype(jnp.float32) + summed + bias
        g[q, x, y] = final.astype(jnp.bfloat16).astype(jnp.float32)
        for axis in (q, 1 - q):
            for kind in range(2):
                push(q, first_now[q], first_now[1 - q], ahead[axis][kind])
        share(q, first_now[q], first_now[1 - q])

    def spread(q, first, forward):
        other = 1 - q
        receive(q, first, first_now[other])
        if forward:
            push(q, first, first_now[other], ahead[q][0])
        for kind in range(2):
            push(q, first, first_now[other], ahead[other][kind])
        share(q, first, first_now[other])
        keep(q, first, first_now[other])

    def settle(q, first, second, forward):
        receive(q, first, second)
        if forward:
            push(q, first, second, ahead[1 - q][0])
        share(q, first, second)
        keep(q, first, second)

    both = range(SUBS)
    for q in both:
        spread(q, first_p[q], True)
    for q in both:
        spread(q, first_n[q], False)
    for q in both:
        keep(q, first_now[q], first_now[1 - q])
    for q in both:
        settle(q, first_now[q], first_p[1 - q], True)
    for q in both:
        settle(q, first_now[q], first_n[1 - q], False)
    for q in both:
        spread(q, first_o[q], False)
    for first in (first_p, first_n):
        for q in both:
            settle(q, first[q], first_p[1 - q], True)
        for q in both:
            settle(q, first[q], first_n[1 - q], False)
    for q in both:
        settle(q, first_now[q], first_o[1 - q], False)
    for q in both:
        settle(q, first_o[q], first_p[1 - q], True)
    for q in both:
        settle(q, first_o[q], first_n[1 - q], False)
    for first in (first_p, first_n, first_o):
        for q in both:
            settle(q, first[q], first_o[1 - q], False)
    orders = [first_now, first_p, first_n, first_o]
    for xi in range(RING):
        for yi in range(RING):
            for q in both:
                xx, yy = slot(q, orders[xi][q], orders[yi][1 - q])
                arrived(gp.at[q, xx, yy], gp_recv.at[q, xx, yy])
                store(q, xx, yy, 1 - c, gp[q, xx, yy])
    sent(g.reshape((-1,) + chunk).at[pl.ds(0, len(pushes))], g_send.at[0])
    sent(gp, gp_send.at[0])


def combine(queries, k_out, v_out, seq_lens, sinks, hidden, b_o, w_o):
    num_seqs, d_model = hidden.shape
    seqs = num_seqs // (RING * SUBS)
    kv = CORES
    heads = sinks.shape[0] // kv
    cols_core = d_model // CORES
    cols_sub = cols_core // SUBS
    block_rows = num_seqs // (RING * RING)
    part = (seqs + 1, heads, LANES)
    f32, bf16 = jnp.float32, jnp.bfloat16
    dma = pltpu.SemaphoreType.DMA
    vmem = pl.BlockSpec(memory_space=pltpu.VMEM)
    hbm = pl.BlockSpec(memory_space=pl.ANY)
    smem = pl.BlockSpec(memory_space=pltpu.SMEM)
    chunk = (block_rows, cols_sub)
    return pl.pallas_call(
        functools.partial(combine_kernel, seqs, LANES ** -0.5),
        out_shape=jax.ShapeDtypeStruct((num_seqs, d_model), bf16),
        in_specs=[vmem, vmem, vmem, smem, smem, hbm, hbm, hbm],
        out_specs=vmem,
        scratch_shapes=[
            pltpu.VMEM((RING, SUBS, kv) + part, f32),
            pltpu.VMEM(b_o.shape, bf16),
            pltpu.VMEM(b_o.shape, f32),
            pltpu.VMEM((RING, SUBS) + part, f32),
            pltpu.VMEM((RING, SUBS) + part, f32),
            pltpu.VMEM((SUBS,) + part, f32),
            pltpu.VMEM((SUBS,) + part, f32),
            pltpu.VMEM((SUBS,) + part, f32),
            pltpu.VMEM((SUBS, seqs * heads, LANES), f32),
            pltpu.VMEM((SUBS, seqs * heads, LANES), f32),
            pltpu.VMEM((2, w_o.shape[0] // 2, cols_core), bf16),
            pltpu.VMEM((block_rows, cols_core), bf16),
            pltpu.VMEM((SUBS, RING) + chunk, f32),
            pltpu.VMEM((SUBS,) + chunk, f32),
            pltpu.VMEM((SUBS,) + chunk, f32),
            pltpu.VMEM((SUBS,) + chunk, f32),
            pltpu.VMEM((SUBS,) + chunk, f32),
            pltpu.VMEM((SUBS, RING, RING) + chunk, f32),
            pltpu.VMEM((SUBS, RING, RING) + chunk, f32),
            dma((2,)), dma((2,)), dma((1,)), dma((RING, SUBS)), dma((1,)),
            dma((SUBS,)), dma((SUBS,)), dma((SUBS,)), dma((1,)), dma((SUBS,)),
            dma((1,)), dma((SUBS,)), dma((SUBS,)), dma((SUBS,)),
            dma((1,)), dma((SUBS, RING, RING)), dma((1,)), dma((SUBS, RING, RING)),
        ],
        compiler_params=pltpu.CompilerParams(collective_id=0, has_side_effects=True, vmem_limit_bytes=COMBINE_MIB * 2**20),
        cost_estimate=pl.CostEstimate(flops=2 * num_seqs // RING * w_o.shape[0] * cols_core, bytes_accessed=30 * 2**20, transcendentals=0),
        name="combine",
    )(queries, k_out, v_out, seq_lens, sinks, *(pltpu.with_memory_space_constraint(a, pltpu.HBM) for a in (hidden, b_o, w_o)))


def front_kernel(
    x_hbm, len_hbm, cos_hbm, sin_hbm, k_hbm, v_hbm, gain_hbm, w_hbm, bias_hbm,
    qs, kbuf, vbuf, k_out, v_out,
    xbuf, lens, cos, sin, gain, bias, hexp, wbuf, acc, kn, vn,
    in_sem, w_sem, k_sem, v_sem, ko_sem, vo_sem,
):
    num_seqs, d_model = x_hbm.shape
    kv = w_hbm.shape[1]
    qkv = w_hbm.shape[2]
    tiles = qkv // LANES
    heads = tiles - 2
    slots, depth2, _ = wbuf.shape
    chunks = d_model * kv // depth2
    blocks = k_sem.shape[0]
    seqs = num_seqs // blocks
    ctx2 = k_hbm.shape[1]
    w_rows = w_hbm.reshape(d_model * kv, qkv)

    def w_copy(chunk, slot):
        return pltpu.make_async_copy(
            w_rows.at[pl.ds(pl.multiple_of(chunk * depth2, depth2), depth2), :], wbuf.at[slot], w_sem.at[slot])

    def w_start(chunk, slot):
        w_copy(chunk, slot).start()

    small = [
        pltpu.make_async_copy(src, dst, in_sem.at[i])
        for i, (src, dst) in enumerate((
            (x_hbm, xbuf), (gain_hbm, gain), (len_hbm, lens), (cos_hbm, cos), (sin_hbm, sin), (bias_hbm, bias)))
    ]
    for copy in small:
        copy.start()
    for slot in range(slots - 1):
        w_start(slot, slot)

    def cache_copy(hbm, buf, sem, block):
        rows = pl.ds(block * seqs, seqs)
        return pltpu.make_async_copy(hbm.at[rows], buf.at[rows], sem.at[block])

    def cache_write(hbm, buf, sem, block):
        rows = pl.ds(block * seqs, seqs)
        return pltpu.make_async_copy(buf.at[rows], hbm.at[rows], sem.at[block])

    small[0].wait()
    small[1].wait()
    row = lax.broadcasted_iota(jnp.int32, (LANES, kv * LANES), 0)
    col = lax.broadcasted_iota(jnp.int32, (LANES, kv * LANES), 1)
    pick = (col == row * kv).astype(jnp.bfloat16)
    gains = gain[...].astype(jnp.float32)
    square = jnp.zeros((num_seqs, LANES), jnp.float32)
    for t in range(d_model // LANES):
        xt = xbuf[:, t * LANES : (t + 1) * LANES].astype(jnp.float32)
        square += xt * xt
    inv_rms = lax.rsqrt(jnp.sum(square, axis=-1, keepdims=True) / d_model + NORM_EPS)
    per_chunk = depth2 // (kv * LANES)
    for t in range(d_model // LANES):
        xt = xbuf[:, t * LANES : (t + 1) * LANES].astype(jnp.float32)
        ht = (xt * inv_rms * gains[t : t + 1]).astype(jnp.bfloat16)
        spread = jnp.dot(ht, pick, preferred_element_type=jnp.float32).astype(jnp.bfloat16)
        for k in range(kv):
            for j in range(kv):
                piece = spread[:, j * LANES : (j + 1) * LANES]
                place = t % per_chunk * kv * LANES + j * LANES
                hexp[t // per_chunk, k * num_seqs : (k + 1) * num_seqs, place : place + LANES] = pltpu.roll(piece, k, 1) if k else piece
    acc[...] = jnp.zeros_like(acc)

    @pl.loop(0, chunks)
    def _(chunk):
        slot = lax.rem(chunk, slots)

        @pl.when(chunk + slots - 1 < chunks)
        def _():
            w_start(chunk + slots - 1, lax.rem(chunk + slots - 1, slots))

        @pl.when(chunk == chunks - slots)
        def _():
            for block in range(blocks):
                cache_copy(k_hbm, kbuf, k_sem, block).start()
                cache_copy(v_hbm, vbuf, v_sem, block).start()

        w_copy(chunk, slot).wait()
        lhs = hexp.at[chunk]
        for t in range(0, tiles, 2):
            cols = slice(t * LANES, (t + 2) * LANES)
            acc[:, cols] += jnp.dot(lhs[...], wbuf[slot, :, cols], preferred_element_type=jnp.float32)

    for copy in small[2:]:
        copy.wait()
    cos_t = jnp.transpose(jnp.concatenate([cos[...], cos[...]], axis=0))
    sin_t = jnp.transpose(jnp.concatenate([-sin[...], sin[...]], axis=0))

    def rotate(t):
        return t * cos_t + pltpu.roll(t, HALF, 1) * sin_t

    def rounded(t):
        return t.astype(jnp.bfloat16).astype(jnp.float32)

    for k in range(kv):
        for t in range(tiles):
            cols = slice(t * LANES, (t + 1) * LANES)
            value = acc[k * num_seqs : (k + 1) * num_seqs, cols] + bias[k : k + 1, cols].astype(jnp.float32)
            if t < heads:
                qs[pl.ds(k * heads + t, num_seqs, stride=kv * heads + 1), :] = rotate(value)
            elif t == heads:
                kn[pl.ds(k, num_seqs, stride=kv), :] = rotate(value)
            else:
                vn[pl.ds(k, num_seqs, stride=kv), :] = value

    base = lax.axis_index("sp") * (ctx2 // kv)
    group = 16
    group_row = lax.broadcasted_iota(jnp.int32, (group, LANES), 0)

    @pl.loop(0, blocks)
    def _(block):
        cache_copy(k_hbm, kbuf, k_sem, block).wait()
        cache_copy(v_hbm, vbuf, v_sem, block).wait()
        found = []
        for i in range(seqs):
            b = block * seqs + i
            local = lens[b] - base
            here = jnp.logical_and(local >= 0, local < ctx2 // kv)
            place = jnp.where(here, local * kv, 0)
            start = pl.multiple_of(place // group * group, group)
            target = jnp.where(here, place - start, group)
            for buf, new in ((kbuf, kn), (vbuf, vn)):
                found.append((buf, b, start, target, new[pl.ds(b * kv, kv), :], buf[b, pl.ds(start, group), :]))
        values = []
        for _, _, _, target, fresh, old in found:
            value = old.astype(jnp.float32)
            for k in range(kv):
                value = jnp.where(group_row == target + k, fresh[k : k + 1], value)
            values.append(value.astype(jnp.bfloat16))
        for (buf, b, start, _, _, _), value in zip(found, values):
            buf[b, pl.ds(start, group), :] = value
        cache_write(k_out, kbuf, ko_sem, block).start()
        cache_write(v_out, vbuf, vo_sem, block).start()

    @pl.loop(0, blocks)
    def _(block):
        cache_write(k_out, kbuf, ko_sem, block).wait()
        cache_write(v_out, vbuf, vo_sem, block).wait()


def front(hidden, seq_lens, cos_t, sin_t, k_cache, v_cache, gain, w_qkv, b_qkv):
    num_seqs, d_model = hidden.shape
    kv, qkv = w_qkv.shape[1:]
    heads = qkv // LANES - 2
    depth2, slots = 1024, 4
    chunks = d_model * kv // depth2
    blocks = RING * SUBS
    f32, bf16 = jnp.float32, jnp.bfloat16
    dma = pltpu.SemaphoreType.DMA
    hbm = pl.BlockSpec(memory_space=pl.ANY)
    vmem = pl.BlockSpec(memory_space=pltpu.VMEM)
    operands = (hidden, seq_lens, cos_t, sin_t, k_cache, v_cache, gain, w_qkv, b_qkv)
    return pl.pallas_call(
        front_kernel,
        out_shape=(
            jax.ShapeDtypeStruct((num_seqs * (kv * heads + 1), LANES), f32),
            pltpu.VMEM(k_cache.shape, bf16), pltpu.VMEM(v_cache.shape, bf16),
            jax.ShapeDtypeStruct(k_cache.shape, bf16), jax.ShapeDtypeStruct(v_cache.shape, bf16)),
        in_specs=[hbm] * len(operands),
        out_specs=(vmem, vmem, vmem, hbm, hbm),
        scratch_shapes=[
            pltpu.VMEM(hidden.shape, bf16),
            pltpu.SMEM(seq_lens.shape, jnp.int32),
            pltpu.VMEM(cos_t.shape, f32),
            pltpu.VMEM(sin_t.shape, f32),
            pltpu.VMEM(gain.shape, bf16),
            pltpu.VMEM(b_qkv.shape, bf16),
            pltpu.VMEM((chunks, kv * num_seqs, depth2), bf16),
            pltpu.VMEM((slots, depth2, qkv), bf16),
            pltpu.VMEM((kv * num_seqs, qkv), f32),
            pltpu.VMEM((num_seqs * kv, LANES), f32),
            pltpu.VMEM((num_seqs * kv, LANES), f32),
            dma((6,)), dma((slots,)), dma((blocks,)), dma((blocks,)), dma((blocks,)), dma((blocks,)),
        ],
        compiler_params=pltpu.CompilerParams(vmem_limit_bytes=FRONT_MIB * 2**20),
        cost_estimate=pl.CostEstimate(flops=4 * num_seqs * d_model * kv * qkv, bytes_accessed=40 * 2**20, transcendentals=0),
        name="front",
    )(*(pltpu.with_memory_space_constraint(a, pltpu.HBM) for a in operands))


def solution(mesh):
    cache_spec = P("dp", "sp", "tp", None)

    def block_step(hidden, seq_lens, rope_cos, rope_sin, k_cache, v_cache, norm_gain, w_qkv, b_qkv, sink_logits, w_o, b_o):
        num_seqs, ctx, kv, head_dim = k_cache.shape
        assert head_dim == LANES and mesh.shape["tp"] == RING and mesh.shape["sp"] == RING * CORES
        flat = (num_seqs, ctx * kv, head_dim)
        queries, k_near, v_near, k_out, v_out = front(
            hidden, seq_lens, rope_cos.T, rope_sin.T, k_cache.reshape(flat), v_cache.reshape(flat), norm_gain.reshape(-1, LANES), w_qkv, b_qkv)
        out_hidden = combine(queries, k_near, v_near, seq_lens, sink_logits, hidden, b_o.reshape(-1, LANES), w_o)
        return out_hidden, k_out.reshape(k_cache.shape), v_out.reshape(v_cache.shape)

    return jax.shard_map(block_step, mesh=mesh, in_specs=(P("dp", None), P("dp"), P("dp", None), P("dp", None), cache_spec, cache_spec, P(None), P(None, "tp", None), P("tp", None), P("tp"), P("tp", None), P(None)), out_specs=(P("dp", None), cache_spec, cache_spec), check_vma=False)
```

```python
import functools

import jax
import jax.numpy as jnp
from jax import lax
from jax.experimental import pallas as pl
from jax.experimental.pallas import tpu as pltpu
from jax.sharding import PartitionSpec as P

NORM_EPS = 1e-5
MESH = pl.DeviceIdType.MESH
LANES = 128
HALF = LANES // 2
SUBS = 2
CORES = 2
PROJECT_MIB = 28
UPDATE_MIB = 4
COMBINE_MIB = 26
WAVE = 4
RING = 4


def lane_column(tile, index):
    return tile[:, index : index + 1]


def merge_parts(parts, seqs):
    stats = [part[seqs] for part in parts]
    top = functools.reduce(jnp.maximum, stats)
    scales = [jnp.exp(stat - top) for stat in stats]
    total = sum(pltpu.roll(scale, HALF, 1) * stat for scale, stat in zip(scales, stats))
    return top, total, scales


def weighted_sums(columns, parts, seqs):
    loaded = [[part[i] for part in parts] for i in range(seqs)]
    scaled = [[column * value for column, value in zip(cols, values)] for cols, values in zip(columns, loaded)]
    return [functools.reduce(jnp.add, terms) for terms in scaled]


def merge_into(dst, parts, seqs):
    top, total, scales = merge_parts(parts, seqs)
    columns = [[lane_column(scale, i) for scale in scales] for i in range(seqs)]
    sums = weighted_sums(columns, parts, seqs)
    lane = lax.broadcasted_iota(jnp.int32, top.shape, 1)
    stats = jnp.where(lane < HALF, top, total)
    for i in range(seqs):
        dst[i] = sums[i]
    dst[seqs] = stats


def combine_kernel(
    seqs, logit_scale, q_ref, k_ref, v_ref, lens, sink_ref, x_hbm, bo_hbm, wo_hbm, out_ref,
    p_ref, bo_ref, bias_rows, ra, cb, rl, rm, rd, own_o, other_o, wbuf, xbuf, z, yrl, ym, yrm, yrd, g, gp,
    w_sem, x_sem, a_send, a_recv, b_send, rl_recv, rm_recv, rd_recv, o_send, o_recv,
    d_send, yrl_recv, yrm_recv, yrd_recv, g_send, g_recv, gp_send, gp_recv,
):
    y = lax.axis_index("tp")
    sp = lax.axis_index("sp")
    x = sp // CORES
    c = sp % CORES
    step = 1 - 2 * c
    xn, xp, xo = (x + step + RING) % RING, (x - step + RING) % RING, (x + 2) % RING
    yn, yp, yo = (y + step + RING) % RING, (y - step + RING) % RING, (y + 2) % RING
    partner = {"sp": x * CORES + 1 - c}
    to_xn, to_xp = {"sp": xn * CORES + c}, {"sp": xp * CORES + c}
    to_yn, to_yp = {"tp": yn}, {"tp": yp}

    rows_half = wo_hbm.shape[0] // 2
    cols_core = wo_hbm.shape[1] // CORES
    cols_sub = cols_core // SUBS
    heads = p_ref.shape[4]
    block_rows = z.shape[2]

    w_copies = []
    for k in range(2):
        rows = (c if k == 0 else 1 - c) * rows_half
        copy = pltpu.make_async_copy(
            wo_hbm.at[pl.ds(pl.multiple_of(rows, LANES), rows_half), pl.ds(pl.multiple_of(c * cols_core, LANES), cols_core)],
            wbuf.at[k], w_sem.at[k])
        copy.start()
        w_copies.append(copy)
    row0 = pl.multiple_of((x * RING + y) * block_rows, block_rows)
    x_copy = pltpu.make_async_copy(
        x_hbm.at[pl.ds(row0, block_rows), pl.ds(pl.multiple_of(c * cols_core, LANES), cols_core)], xbuf, x_sem.at[0])
    x_copy.start()
    bo_copy = pltpu.make_async_copy(bo_hbm, bo_ref, x_sem.at[1])
    bo_copy.start()

    barrier = pltpu.get_barrier_semaphore()
    for where in (partner, to_xn, to_xp, to_yn, to_yp):
        pl.semaphore_signal(barrier, inc=1, device_id=where, device_id_type=MESH)
    pl.semaphore_wait(barrier, 5)

    def send(src, dst, send_sem, recv_sem, where):
        copy = pltpu.make_async_remote_copy(
            src_ref=src, dst_ref=dst, send_sem=send_sem, recv_sem=recv_sem, device_id=where, device_id_type=MESH)
        copy.start()

    def sent(shape_of, send_sem):
        pltpu.make_async_remote_copy(
            src_ref=shape_of, dst_ref=shape_of, send_sem=send_sem, recv_sem=send_sem, device_id=partner, device_id_type=MESH).wait_send()

    def arrived(dst, recv_sem):
        pltpu.make_async_remote_copy(
            src_ref=dst, dst_ref=dst, send_sem=recv_sem, recv_sem=recv_sem, device_id=partner, device_id_type=MESH).wait_recv()

    kv = p_ref.shape[2]
    q_rows = kv * heads
    ctx2 = k_ref.shape[1]
    q_stride = q_ref.shape[1] // (heads + 2)
    row = lax.broadcasted_iota(jnp.int32, (q_rows, ctx2), 0)
    lane = lax.broadcasted_iota(jnp.int32, (q_rows, ctx2), 1)
    position = jnp.where(lane % kv == row // heads, lane // kv + sp * (ctx2 // kv), jnp.iinfo(jnp.int32).max)
    sinks = jnp.zeros((q_rows, LANES), jnp.float32)
    for i in range(q_rows):
        sinks = jnp.where(row == i, sink_ref[i], sinks)
    sink_col = jnp.max(sinks, axis=-1, keepdims=True)

    def attend(b, s):
        first = (b * SUBS + s) * seqs
        waves = [range(j, j + WAVE) for j in range(0, seqs, WAVE)]
        logits, tops, totals, weights, stats = {}, {}, {}, {}, jnp.zeros((q_rows, LANES), jnp.float32)
        for turn in range(len(waves) + 2):
            if turn < len(waves):
                for i in waves[turn]:
                    q = jnp.concatenate([q_ref[k, pl.ds(first + i, heads, stride=q_stride), :] for k in range(kv)], axis=0).astype(jnp.bfloat16)
                    logits[i] = lax.dot_general(q, k_ref[first + i], (((1,), (1,)), ((), ())), preferred_element_type=jnp.float32)
            if 0 <= turn - 1 < len(waves):
                members = waves[turn - 1]
                for i in members:
                    logits[i] = jnp.where(position <= lens[first + i], logits[i] * logit_scale, -jnp.inf)
                for i in members:
                    tops[i] = jnp.maximum(jnp.max(logits[i], axis=-1, keepdims=True), sink_col)
                for i in members:
                    weights[i] = jnp.exp(logits[i] - tops[i])
                for i in members:
                    totals[i] = jnp.sum(weights[i], axis=-1, keepdims=True)
            if 0 <= turn - 2:
                members = waves[turn - 2]
                numers = [
                    jnp.dot(weights[i].astype(jnp.bfloat16), v_ref[first + i], preferred_element_type=jnp.float32) for i in members]
                for i, numer in zip(members, numers):
                    for k in range(kv):
                        p_ref[b, s, k, i] = numer[k * heads : (k + 1) * heads]
                    stats = jnp.where(lane == i, tops[i], jnp.where(lane == HALF + i, totals[i], stats))
        for k in range(kv):
            p_ref[b, s, k, seqs] = stats[k * heads : (k + 1) * heads]
        send(p_ref.at[b, s, 1 - c], ra.at[b, s], a_send.at[0], a_recv.at[b, s], partner)

    def attend_both(b):
        @pl.loop(0, SUBS)
        def _(s):
            attend(b, s)

    def relay(s):
        arrived(ra.at[xo, s], a_recv.at[xo, s])
        merge_into(cb.at[0, s], (p_ref.at[xo, s, c], ra.at[xo, s]), seqs)
        send(cb.at[0, s], rl.at[s], b_send.at[0], rl_recv.at[s], to_xn)

    def pass_on(s):
        arrived(ra.at[xn, s], a_recv.at[xn, s])
        arrived(rl.at[s], rl_recv.at[s])
        merge_into(cb.at[2, s], (p_ref.at[xn, s, c], ra.at[xn, s], rl.at[s]), seqs)
        send(cb.at[2, s], rm.at[s], b_send.at[0], rm_recv.at[s], to_xn)

    attend_both(xo)
    for s in range(SUBS):
        attend(xn, s)
        relay(s)
    attend_both(xp)
    for s in range(SUBS):
        arrived(ra.at[xp, s], a_recv.at[xp, s])
        merge_into(cb.at[1, s], (p_ref.at[xp, s, c], ra.at[xp, s]), seqs)
        send(cb.at[1, s], rd.at[s], b_send.at[0], rd_recv.at[s], to_xp)
    for s in range(SUBS):
        attend(x, s)
        pass_on(s)
    for s in range(SUBS):
        arrived(ra.at[x, s], a_recv.at[x, s])
        merge_into(cb.at[3, s], (p_ref.at[x, s, c], ra.at[x, s]), seqs)
    sink = jnp.zeros((heads, LANES), jnp.float32)
    head_row = lax.broadcasted_iota(jnp.int32, sink.shape, 0)
    for h in range(heads):
        sink = jnp.where(head_row == h, sink_ref[c * heads + h], sink)
    for s in range(SUBS):
        arrived(rd.at[s], rd_recv.at[s])
        arrived(rm.at[s], rm_recv.at[s])
        parts = (cb.at[3, s], rd.at[s], rm.at[s])
        top, total, scales = merge_parts(parts, seqs)
        inverse = 1.0 / (pltpu.roll(total, HALF, 1) + jnp.exp(sink - top))
        columns = [[lane_column(scale * inverse, i) for scale in scales] for i in range(seqs)]
        outs = [out.astype(jnp.bfloat16).astype(jnp.float32) for out in weighted_sums(columns, parts, seqs)]
        for i in range(seqs):
            own_o[s, pl.ds(i * heads, heads), :] = outs[i]
        send(own_o.at[s], other_o.at[s], o_send.at[0], o_recv.at[s], partner)

    def head_rows(ref):
        columns = []
        for h in range(heads):
            columns.append(jnp.concatenate(
                [ref[s, pl.ds(h, seqs, stride=heads), :] for s in range(SUBS)], axis=0).astype(jnp.bfloat16))
        return jnp.concatenate(columns, axis=1)

    own_rows = head_rows(own_o)
    w_copies[0].wait()
    for q in range(SUBS):
        part = jnp.dot(own_rows, wbuf[0, :, pl.ds(q * cols_sub, cols_sub)], preferred_element_type=jnp.float32)
        for r in range(RING):
            z[q, r] = part[r * block_rows : (r + 1) * block_rows]
    for s in range(SUBS):
        arrived(other_o.at[s], o_recv.at[s])
    other_rows = head_rows(other_o)
    w_copies[1].wait()
    for q in range(SUBS):
        part = jnp.dot(other_rows, wbuf[1, :, pl.ds(q * cols_sub, cols_sub)], preferred_element_type=jnp.float32)
        for r in range(RING):
            z[q, r] += part[r * block_rows : (r + 1) * block_rows]
        send(z.at[q, yo], yrl.at[q], d_send.at[0], yrl_recv.at[q], to_yn)
        send(z.at[q, yp], yrd.at[q], d_send.at[0], yrd_recv.at[q], to_yp)
    for q in range(SUBS):
        arrived(yrl.at[q], yrl_recv.at[q])
        ym[q] = z[q, yn] + yrl[q]
        send(ym.at[q], yrm.at[q], d_send.at[0], yrm_recv.at[q], to_yn)
    chunk = g.shape[3:]
    sent(ra, a_send.at[0])
    sent(cb.at[pl.ds(0, 3)], b_send.at[0])
    sent(own_o, o_send.at[0])
    sent(g.reshape((-1,) + chunk).at[pl.ds(0, 3 * SUBS)], d_send.at[0])
    x_copy.wait()
    bo_copy.wait()
    bias_rows[...] = bo_ref[...].astype(jnp.float32)

    def store(q, xx, yy, core, value):
        rows = pl.ds(pl.multiple_of((xx * RING + yy) * block_rows, block_rows), block_rows)
        cols = pl.ds(pl.multiple_of(core * cols_core + q * cols_sub, LANES), cols_sub)
        out_ref[rows, cols] = value.astype(jnp.bfloat16)

    def slot(q, first, second):
        return (first, second) if q == 0 else (second, first)

    ahead = ((to_xn, to_xp), (to_yn, to_yp))
    first_now, first_n, first_p, first_o = (x, y), (xn, yn), (xp, yp), (xo, yo)

    pushes = []

    def push(q, first, second, where):
        xx, yy = slot(q, first, second)
        pushes.append(q)
        send(g.at[q, xx, yy], g.at[q, xx, yy], g_send.at[0], g_recv.at[q, xx, yy], where)

    def share(q, first, second):
        xx, yy = slot(q, first, second)
        send(g.at[q, xx, yy], gp.at[q, xx, yy], gp_send.at[0], gp_recv.at[q, xx, yy], partner)

    def receive(q, first, second):
        xx, yy = slot(q, first, second)
        arrived(g.at[q, xx, yy], g_recv.at[q, xx, yy])

    def keep(q, first, second):
        xx, yy = slot(q, first, second)
        store(q, xx, yy, c, g[q, xx, yy])

    for q in range(SUBS):
        arrived(yrd.at[q], yrd_recv.at[q])
        arrived(yrm.at[q], yrm_recv.at[q])
        first_row = (c * cols_core + q * cols_sub) // LANES
        bias = jnp.concatenate([bias_rows[pl.ds(first_row + t, 1), :] for t in range(cols_sub // LANES)], axis=1)
        summed = z[q, y] + yrd[q] + yrm[q]
        final = xbuf[:, pl.ds(q * cols_sub, cols_sub)].astype(jnp.float32) + summed + bias
        g[q, x, y] = final.astype(jnp.bfloat16).astype(jnp.float32)
        for axis in (q, 1 - q):
            for kind in range(2):
                push(q, first_now[q], first_now[1 - q], ahead[axis][kind])
        share(q, first_now[q], first_now[1 - q])

    def spread(q, first, forward):
        other = 1 - q
        receive(q, first, first_now[other])
        if forward:
            push(q, first, first_now[other], ahead[q][0])
        for kind in range(2):
            push(q, first, first_now[other], ahead[other][kind])
        share(q, first, first_now[other])
        keep(q, first, first_now[other])

    def settle(q, first, second, forward):
        receive(q, first, second)
        if forward:
            push(q, first, second, ahead[1 - q][0])
        share(q, first, second)
        keep(q, first, second)

    both = range(SUBS)
    for q in both:
        spread(q, first_p[q], True)
    for q in both:
        spread(q, first_n[q], False)
    for q in both:
        keep(q, first_now[q], first_now[1 - q])
    for q in both:
        settle(q, first_now[q], first_p[1 - q], True)
    for q in both:
        settle(q, first_now[q], first_n[1 - q], False)
    for q in both:
        spread(q, first_o[q], False)
    for first in (first_p, first_n):
        for q in both:
            settle(q, first[q], first_p[1 - q], True)
        for q in both:
            settle(q, first[q], first_n[1 - q], False)
    for q in both:
        settle(q, first_now[q], first_o[1 - q], False)
    for q in both:
        settle(q, first_o[q], first_p[1 - q], True)
    for q in both:
        settle(q, first_o[q], first_n[1 - q], False)
    for first in (first_p, first_n, first_o):
        for q in both:
            settle(q, first[q], first_o[1 - q], False)
    orders = [first_now, first_p, first_n, first_o]
    for xi in range(RING):
        for yi in range(RING):
            for q in both:
                xx, yy = slot(q, orders[xi][q], orders[yi][1 - q])
                arrived(gp.at[q, xx, yy], gp_recv.at[q, xx, yy])
                store(q, xx, yy, 1 - c, gp[q, xx, yy])
    sent(g.reshape((-1,) + chunk).at[pl.ds(0, len(pushes))], g_send.at[0])
    sent(gp, gp_send.at[0])


def combine(queries, k_out, v_out, seq_lens, sinks, hidden, b_o, w_o):
    num_seqs, d_model = hidden.shape
    seqs = num_seqs // (RING * SUBS)
    kv = CORES
    heads = sinks.shape[0] // kv
    cols_core = d_model // CORES
    cols_sub = cols_core // SUBS
    block_rows = num_seqs // (RING * RING)
    part = (seqs + 1, heads, LANES)
    f32, bf16 = jnp.float32, jnp.bfloat16
    dma = pltpu.SemaphoreType.DMA
    vmem = pl.BlockSpec(memory_space=pltpu.VMEM)
    hbm = pl.BlockSpec(memory_space=pl.ANY)
    smem = pl.BlockSpec(memory_space=pltpu.SMEM)
    chunk = (block_rows, cols_sub)
    return pl.pallas_call(
        functools.partial(combine_kernel, seqs, LANES ** -0.5),
        out_shape=jax.ShapeDtypeStruct((num_seqs, d_model), bf16),
        in_specs=[vmem, vmem, vmem, smem, smem, hbm, hbm, hbm],
        out_specs=vmem,
        scratch_shapes=[
            pltpu.VMEM((RING, SUBS, kv) + part, f32),
            pltpu.VMEM(b_o.shape, bf16),
            pltpu.VMEM(b_o.shape, f32),
            pltpu.VMEM((RING, SUBS) + part, f32),
            pltpu.VMEM((RING, SUBS) + part, f32),
            pltpu.VMEM((SUBS,) + part, f32),
            pltpu.VMEM((SUBS,) + part, f32),
            pltpu.VMEM((SUBS,) + part, f32),
            pltpu.VMEM((SUBS, seqs * heads, LANES), f32),
            pltpu.VMEM((SUBS, seqs * heads, LANES), f32),
            pltpu.VMEM((2, w_o.shape[0] // 2, cols_core), bf16),
            pltpu.VMEM((block_rows, cols_core), bf16),
            pltpu.VMEM((SUBS, RING) + chunk, f32),
            pltpu.VMEM((SUBS,) + chunk, f32),
            pltpu.VMEM((SUBS,) + chunk, f32),
            pltpu.VMEM((SUBS,) + chunk, f32),
            pltpu.VMEM((SUBS,) + chunk, f32),
            pltpu.VMEM((SUBS, RING, RING) + chunk, f32),
            pltpu.VMEM((SUBS, RING, RING) + chunk, f32),
            dma((2,)), dma((2,)), dma((1,)), dma((RING, SUBS)), dma((1,)),
            dma((SUBS,)), dma((SUBS,)), dma((SUBS,)), dma((1,)), dma((SUBS,)),
            dma((1,)), dma((SUBS,)), dma((SUBS,)), dma((SUBS,)),
            dma((1,)), dma((SUBS, RING, RING)), dma((1,)), dma((SUBS, RING, RING)),
        ],
        compiler_params=pltpu.CompilerParams(collective_id=0, has_side_effects=True, vmem_limit_bytes=COMBINE_MIB * 2**20),
        cost_estimate=pl.CostEstimate(flops=2 * num_seqs // RING * w_o.shape[0] * cols_core, bytes_accessed=30 * 2**20, transcendentals=0),
        name="combine",
    )(queries, k_out, v_out, seq_lens, sinks, *(pltpu.with_memory_space_constraint(a, pltpu.HBM) for a in (hidden, b_o, w_o)))


def project_kernel(
    x_hbm, cos_hbm, sin_hbm, k_hbm, v_hbm, gain_hbm, w_hbm, bias_hbm,
    heads_ref, kbuf, vbuf,
    xbuf, cos, sin, gain, bias, hexp, wbuf, acc,
    in_sem, w_sem, cache_sem, send_sem, recv_sem,
):
    num_seqs, d_model = x_hbm.shape
    kv = w_hbm.shape[1]
    qkv = w_hbm.shape[2]
    tiles = qkv // LANES // CORES
    slots, depth2, cols = wbuf.shape
    chunks = d_model * kv // depth2
    stride = heads_ref.shape[1] // (CORES * tiles)
    c = lax.axis_index("sp") % CORES
    partner = {"sp": lax.axis_index("sp") + 1 - 2 * c}
    w_rows = w_hbm.reshape(d_model * kv, qkv)
    first_col = pl.multiple_of(c * cols, LANES)

    def w_copy(chunk, slot):
        return pltpu.make_async_copy(
            w_rows.at[pl.ds(pl.multiple_of(chunk * depth2, depth2), depth2), pl.ds(first_col, cols)], wbuf.at[slot], w_sem.at[slot])

    small = [
        pltpu.make_async_copy(src, dst, in_sem.at[i])
        for i, (src, dst) in enumerate((
            (x_hbm, xbuf), (gain_hbm, gain), (cos_hbm, cos), (sin_hbm, sin), (bias_hbm, bias)))
    ]
    for copy in small:
        copy.start()
    for slot in range(slots):
        w_copy(slot, slot).start()
    barrier = pltpu.get_barrier_semaphore()
    pl.semaphore_signal(barrier, inc=1, device_id=partner, device_id_type=MESH)

    small[0].wait()
    small[1].wait()
    row = lax.broadcasted_iota(jnp.int32, (LANES, kv * LANES), 0)
    col = lax.broadcasted_iota(jnp.int32, (LANES, kv * LANES), 1)
    pick = (col == row * kv).astype(jnp.bfloat16)
    gains = gain[...].astype(jnp.float32)
    square = jnp.zeros((num_seqs, LANES), jnp.float32)
    for t in range(d_model // LANES):
        xt = xbuf[:, t * LANES : (t + 1) * LANES].astype(jnp.float32)
        square += xt * xt
    inv_rms = lax.rsqrt(jnp.sum(square, axis=-1, keepdims=True) / d_model + NORM_EPS)
    per_chunk = depth2 // (kv * LANES)
    for t in range(d_model // LANES):
        xt = xbuf[:, t * LANES : (t + 1) * LANES].astype(jnp.float32)
        ht = (xt * inv_rms * gains[t : t + 1]).astype(jnp.bfloat16)
        spread = jnp.dot(ht, pick, preferred_element_type=jnp.float32).astype(jnp.bfloat16)
        for k in range(kv):
            for j in range(kv):
                piece = spread[:, j * LANES : (j + 1) * LANES]
                place = t % per_chunk * kv * LANES + j * LANES
                hexp[t // per_chunk, k * num_seqs : (k + 1) * num_seqs, place : place + LANES] = pltpu.roll(piece, k, 1) if k else piece
    acc[...] = jnp.zeros_like(acc)
    cache_copies = [pltpu.make_async_copy(src, dst, cache_sem.at[i]) for i, (src, dst) in enumerate(((k_hbm, kbuf), (v_hbm, vbuf)))]

    @pl.loop(0, chunks)
    def _(chunk):
        slot = lax.rem(chunk, slots)
        w_copy(chunk, slot).wait()
        lhs = hexp.at[chunk]
        for t in range(0, tiles, 2):
            part = slice(t * LANES, min(t + 2, tiles) * LANES)
            acc[:, part] += jnp.dot(lhs[...], wbuf[slot, :, part], preferred_element_type=jnp.float32)

        @pl.when(chunk + slots < chunks)
        def _():
            w_copy(chunk + slots, slot).start()

        @pl.when(chunk + slots == chunks - 1)
        def _():
            for copy in cache_copies:
                copy.start()

    for copy in small[2:]:
        copy.wait()
    cos_t = jnp.transpose(jnp.concatenate([cos[...], cos[...]], axis=0))
    sin_t = jnp.transpose(jnp.concatenate([-sin[...], sin[...]], axis=0))
    pl.semaphore_wait(barrier, 1)

    def mine(k):
        rows = tiles * stride
        return heads_ref.at[k, pl.ds(pl.multiple_of(c * rows, 8), rows)]

    for k in range(kv):
        for j in range(tiles):
            tile = c * tiles + j
            value = acc[k * num_seqs : (k + 1) * num_seqs, j * LANES : (j + 1) * LANES]
            value += bias[k : k + 1, pl.ds(pl.multiple_of(tile * LANES, LANES), LANES)].astype(jnp.float32)
            turned = value * cos_t + pltpu.roll(value, HALF, 1) * sin_t
            value = jnp.where(jnp.full(value.shape, tile, jnp.int32) == CORES * tiles - 1, value, turned)
            heads_ref[k, pl.ds(pl.multiple_of(tile * stride, 8), num_seqs), :] = value.astype(jnp.bfloat16).astype(jnp.float32)
        pltpu.make_async_remote_copy(
            src_ref=mine(k), dst_ref=mine(k), send_sem=send_sem.at[k], recv_sem=recv_sem.at[k],
            device_id=partner, device_id_type=MESH).start()
    for copy in cache_copies:
        copy.wait()
    for k in range(kv):
        copy = pltpu.make_async_remote_copy(
            src_ref=mine(k), dst_ref=mine(k), send_sem=send_sem.at[k], recv_sem=recv_sem.at[k],
            device_id=partner, device_id_type=MESH)
        copy.wait_send()
        copy.wait_recv()


def project(hidden, cos_t, sin_t, k_cache, v_cache, gain, w_qkv, b_qkv):
    num_seqs, d_model = hidden.shape
    kv, qkv = w_qkv.shape[1:]
    tiles = qkv // LANES
    depth2, slots = 1024, 6
    chunks = d_model * kv // depth2
    f32, bf16 = jnp.float32, jnp.bfloat16
    dma = pltpu.SemaphoreType.DMA
    hbm = pl.BlockSpec(memory_space=pl.ANY)
    vmem = pl.BlockSpec(memory_space=pltpu.VMEM)
    operands = (hidden, cos_t, sin_t, k_cache, v_cache, gain, w_qkv, b_qkv)
    return pl.pallas_call(
        project_kernel,
        out_shape=(pltpu.VMEM((kv, tiles * (num_seqs + 8), LANES), f32), pltpu.VMEM(k_cache.shape, bf16), pltpu.VMEM(v_cache.shape, bf16)),
        in_specs=[hbm] * len(operands),
        out_specs=(vmem, vmem, vmem),
        scratch_shapes=[
            pltpu.VMEM(hidden.shape, bf16),
            pltpu.VMEM(cos_t.shape, f32),
            pltpu.VMEM(sin_t.shape, f32),
            pltpu.VMEM(gain.shape, bf16),
            pltpu.VMEM(b_qkv.shape, bf16),
            pltpu.VMEM((chunks, kv * num_seqs, depth2), bf16),
            pltpu.VMEM((slots, depth2, qkv // CORES), bf16),
            pltpu.VMEM((kv * num_seqs, qkv // CORES), f32),
            dma((5,)), dma((slots,)), dma((2,)), dma((kv,)), dma((kv,)),
        ],
        compiler_params=pltpu.CompilerParams(collective_id=1, has_side_effects=True, vmem_limit_bytes=PROJECT_MIB * 2**20),
        cost_estimate=pl.CostEstimate(flops=2 * num_seqs * d_model * kv * qkv, bytes_accessed=24 * 2**20, transcendentals=0),
        name="project",
    )(*(pltpu.with_memory_space_constraint(a, pltpu.HBM) for a in operands))


def update_kernel(lens, heads_ref, k_in, v_in, kbuf, vbuf, k_out, v_out, ko_sem, vo_sem):
    kv = heads_ref.shape[0]
    num_seqs, ctx2 = kbuf.shape[:2]
    blocks = ko_sem.shape[0]
    seqs = num_seqs // blocks
    stride = num_seqs + 8
    tiles = heads_ref.shape[1] // stride
    base = lax.axis_index("sp") * (ctx2 // kv)
    group = 16
    group_row = lax.broadcasted_iota(jnp.int32, (group, LANES), 0)

    def cache_write(hbm, buf, sem, block):
        rows = pl.ds(block * seqs, seqs)
        return pltpu.make_async_copy(buf.at[rows], hbm.at[rows], sem.at[block])

    @pl.loop(0, blocks)
    def _(block):
        found = []
        for i in range(seqs):
            b = block * seqs + i
            local = lens[b] - base
            here = jnp.logical_and(local >= 0, local < ctx2 // kv)
            place = jnp.where(here, local * kv, 0)
            start = pl.multiple_of(place // group * group, group)
            target = jnp.where(here, place - start, group)
            for n, buf in enumerate((kbuf, vbuf)):
                fresh = [heads_ref[k, pl.ds((tiles - 2 + n) * stride + b, 1), :] for k in range(kv)]
                found.append((buf, b, start, target, fresh, buf[b, pl.ds(start, group), :]))
        values = []
        for _, _, _, target, fresh, old in found:
            value = old.astype(jnp.float32)
            for k in range(kv):
                value = jnp.where(group_row == target + k, fresh[k], value)
            values.append(value.astype(jnp.bfloat16))
        for (buf, b, start, _, _, _), value in zip(found, values):
            buf[b, pl.ds(start, group), :] = value
        cache_write(k_out, kbuf, ko_sem, block).start()
        cache_write(v_out, vbuf, vo_sem, block).start()

    @pl.loop(0, blocks)
    def _(block):
        cache_write(k_out, kbuf, ko_sem, block).wait()
        cache_write(v_out, vbuf, vo_sem, block).wait()


def update(seq_lens, heads_out, k_near, v_near):
    blocks = RING * SUBS
    hbm = pl.BlockSpec(memory_space=pl.ANY)
    vmem = pl.BlockSpec(memory_space=pltpu.VMEM)
    near = pltpu.VMEM(k_near.shape, k_near.dtype)
    far = jax.ShapeDtypeStruct(k_near.shape, k_near.dtype)
    dma = pltpu.SemaphoreType.DMA
    return pl.pallas_call(
        update_kernel,
        out_shape=(near, near, far, far),
        in_specs=[pl.BlockSpec(memory_space=pltpu.SMEM), vmem, vmem, vmem],
        out_specs=(vmem, vmem, hbm, hbm),
        scratch_shapes=[dma((blocks,)), dma((blocks,))],
        input_output_aliases={2: 0, 3: 1},
        compiler_params=pltpu.CompilerParams(vmem_limit_bytes=UPDATE_MIB * 2**20),
        cost_estimate=pl.CostEstimate(flops=10**6, bytes_accessed=10 * 2**20, transcendentals=0),
        name="update",
    )(seq_lens, heads_out, k_near, v_near)


def solution(mesh):
    cache_spec = P("dp", "sp", "tp", None)

    def block_step(hidden, seq_lens, rope_cos, rope_sin, k_cache, v_cache, norm_gain, w_qkv, b_qkv, sink_logits, w_o, b_o):
        num_seqs, ctx, kv, head_dim = k_cache.shape
        assert head_dim == LANES and mesh.shape["tp"] == RING and mesh.shape["sp"] == RING * CORES
        flat = (num_seqs, ctx * kv, head_dim)
        heads_out, k_near, v_near = project(
            hidden, rope_cos.T, rope_sin.T, k_cache.reshape(flat), v_cache.reshape(flat), norm_gain.reshape(-1, LANES), w_qkv, b_qkv)
        k_near, v_near, k_out, v_out = update(seq_lens, heads_out, k_near, v_near)
        out_hidden = combine(heads_out, k_near, v_near, seq_lens, sink_logits, hidden, b_o.reshape(-1, LANES), w_o)
        return out_hidden, k_out.reshape(k_cache.shape), v_out.reshape(v_cache.shape)

    return jax.shard_map(block_step, mesh=mesh, in_specs=(P("dp", None), P("dp"), P("dp", None), P("dp", None), cache_spec, cache_spec, P(None), P(None, "tp", None), P("tp", None), P("tp"), P("tp", None), P(None)), out_specs=(P("dp", None), cache_spec, cache_spec), check_vma=False)
```

```python
import functools

import jax
import jax.numpy as jnp
from jax import lax
from jax.experimental import pallas as pl
from jax.experimental.pallas import tpu as pltpu
from jax.sharding import PartitionSpec as P

NORM_EPS = 1e-5
MESH = pl.DeviceIdType.MESH
LANES = 128
HALF = LANES // 2
SUBS = 2
CORES = 2
PROJECT_MIB = 30
UPDATE_MIB = 4
COMBINE_MIB = 26
WAVE = 4
RING = 4


def lane_column(tile, index):
    return tile[:, index : index + 1]


def merge_parts(parts, seqs):
    stats = [part[seqs] for part in parts]
    top = functools.reduce(jnp.maximum, stats)
    scales = [jnp.exp(stat - top) for stat in stats]
    total = sum(pltpu.roll(scale, HALF, 1) * stat for scale, stat in zip(scales, stats))
    return top, total, scales


def weighted_sums(columns, parts, seqs):
    loaded = [[part[i] for part in parts] for i in range(seqs)]
    scaled = [[column * value for column, value in zip(cols, values)] for cols, values in zip(columns, loaded)]
    return [functools.reduce(jnp.add, terms) for terms in scaled]


def merge_into(dst, parts, seqs):
    top, total, scales = merge_parts(parts, seqs)
    columns = [[lane_column(scale, i) for scale in scales] for i in range(seqs)]
    sums = weighted_sums(columns, parts, seqs)
    lane = lax.broadcasted_iota(jnp.int32, top.shape, 1)
    stats = jnp.where(lane < HALF, top, total)
    for i in range(seqs):
        dst[i] = sums[i]
    dst[seqs] = stats


def combine_kernel(
    seqs, logit_scale, q_ref, k_ref, v_ref, lens, sink_ref, x_hbm, bo_hbm, wo_hbm, out_ref,
    p_ref, bo_ref, bias_rows, ra, cb, rl, rm, rd, own_o, other_o, wbuf, xbuf, z, yrl, ym, yrm, yrd, g, gp,
    w_sem, x_sem, a_send, a_recv, b_send, rl_recv, rm_recv, rd_recv, o_send, o_recv,
    d_send, yrl_recv, yrm_recv, yrd_recv, g_send, g_recv, gp_send, gp_recv,
):
    y = lax.axis_index("tp")
    sp = lax.axis_index("sp")
    x = sp // CORES
    c = sp % CORES
    step = 1 - 2 * c
    xn, xp, xo = (x + step + RING) % RING, (x - step + RING) % RING, (x + 2) % RING
    yn, yp, yo = (y + step + RING) % RING, (y - step + RING) % RING, (y + 2) % RING
    partner = {"sp": x * CORES + 1 - c}
    to_xn, to_xp = {"sp": xn * CORES + c}, {"sp": xp * CORES + c}
    to_yn, to_yp = {"tp": yn}, {"tp": yp}

    rows_half = wo_hbm.shape[0] // 2
    cols_core = wo_hbm.shape[1] // CORES
    cols_sub = cols_core // SUBS
    heads = p_ref.shape[4]
    block_rows = z.shape[2]

    w_copies = []
    for k in range(2):
        rows = (c if k == 0 else 1 - c) * rows_half
        copy = pltpu.make_async_copy(
            wo_hbm.at[pl.ds(pl.multiple_of(rows, LANES), rows_half), pl.ds(pl.multiple_of(c * cols_core, LANES), cols_core)],
            wbuf.at[k], w_sem.at[k])
        copy.start()
        w_copies.append(copy)
    row0 = pl.multiple_of((x * RING + y) * block_rows, block_rows)
    x_copy = pltpu.make_async_copy(
        x_hbm.at[pl.ds(row0, block_rows), pl.ds(pl.multiple_of(c * cols_core, LANES), cols_core)], xbuf, x_sem.at[0])
    x_copy.start()
    bo_copy = pltpu.make_async_copy(bo_hbm, bo_ref, x_sem.at[1])
    bo_copy.start()

    barrier = pltpu.get_barrier_semaphore()
    for where in (partner, to_xn, to_xp, to_yn, to_yp):
        pl.semaphore_signal(barrier, inc=1, device_id=where, device_id_type=MESH)
    pl.semaphore_wait(barrier, 5)

    def send(src, dst, send_sem, recv_sem, where):
        copy = pltpu.make_async_remote_copy(
            src_ref=src, dst_ref=dst, send_sem=send_sem, recv_sem=recv_sem, device_id=where, device_id_type=MESH)
        copy.start()

    def sent(shape_of, send_sem):
        pltpu.make_async_remote_copy(
            src_ref=shape_of, dst_ref=shape_of, send_sem=send_sem, recv_sem=send_sem, device_id=partner, device_id_type=MESH).wait_send()

    def arrived(dst, recv_sem):
        pltpu.make_async_remote_copy(
            src_ref=dst, dst_ref=dst, send_sem=recv_sem, recv_sem=recv_sem, device_id=partner, device_id_type=MESH).wait_recv()

    kv = p_ref.shape[2]
    q_rows = kv * heads
    ctx2 = k_ref.shape[1]
    q_stride = q_ref.shape[1] // (heads + 2)
    row = lax.broadcasted_iota(jnp.int32, (q_rows, ctx2), 0)
    lane = lax.broadcasted_iota(jnp.int32, (q_rows, ctx2), 1)
    position = jnp.where(lane % kv == row // heads, lane // kv + sp * (ctx2 // kv), jnp.iinfo(jnp.int32).max)
    sinks = jnp.zeros((q_rows, LANES), jnp.float32)
    for i in range(q_rows):
        sinks = jnp.where(row == i, sink_ref[i], sinks)
    sink_col = jnp.max(sinks, axis=-1, keepdims=True)

    def attend(b, s):
        first = (b * SUBS + s) * seqs
        waves = [range(j, j + WAVE) for j in range(0, seqs, WAVE)]
        logits, tops, totals, weights, stats = {}, {}, {}, {}, jnp.zeros((q_rows, LANES), jnp.float32)
        for turn in range(len(waves) + 2):
            if turn < len(waves):
                for i in waves[turn]:
                    q = jnp.concatenate([q_ref[k, pl.ds(first + i, heads, stride=q_stride), :] for k in range(kv)], axis=0).astype(jnp.bfloat16)
                    logits[i] = lax.dot_general(q, k_ref[first + i], (((1,), (1,)), ((), ())), preferred_element_type=jnp.float32)
            if 0 <= turn - 1 < len(waves):
                members = waves[turn - 1]
                for i in members:
                    logits[i] = jnp.where(position <= lens[first + i], logits[i] * logit_scale, -jnp.inf)
                for i in members:
                    tops[i] = jnp.maximum(jnp.max(logits[i], axis=-1, keepdims=True), sink_col)
                for i in members:
                    weights[i] = jnp.exp(logits[i] - tops[i])
                for i in members:
                    totals[i] = jnp.sum(weights[i], axis=-1, keepdims=True)
            if 0 <= turn - 2:
                members = waves[turn - 2]
                numers = [
                    jnp.dot(weights[i].astype(jnp.bfloat16), v_ref[first + i], preferred_element_type=jnp.float32) for i in members]
                for i, numer in zip(members, numers):
                    for k in range(kv):
                        p_ref[b, s, k, i] = numer[k * heads : (k + 1) * heads]
                    stats = jnp.where(lane == i, tops[i], jnp.where(lane == HALF + i, totals[i], stats))
        for k in range(kv):
            p_ref[b, s, k, seqs] = stats[k * heads : (k + 1) * heads]
        send(p_ref.at[b, s, 1 - c], ra.at[b, s], a_send.at[0], a_recv.at[b, s], partner)

    def attend_both(b):
        @pl.loop(0, SUBS)
        def _(s):
            attend(b, s)

    def relay(s):
        arrived(ra.at[xo, s], a_recv.at[xo, s])
        merge_into(cb.at[0, s], (p_ref.at[xo, s, c], ra.at[xo, s]), seqs)
        send(cb.at[0, s], rl.at[s], b_send.at[0], rl_recv.at[s], to_xn)

    def pass_on(s):
        arrived(ra.at[xn, s], a_recv.at[xn, s])
        arrived(rl.at[s], rl_recv.at[s])
        merge_into(cb.at[2, s], (p_ref.at[xn, s, c], ra.at[xn, s], rl.at[s]), seqs)
        send(cb.at[2, s], rm.at[s], b_send.at[0], rm_recv.at[s], to_xn)

    attend_both(xo)
    attend(xn, 0)
    for s in range(SUBS):
        relay(s)
    for s in range(1, SUBS):
        attend(xn, s)
    attend_both(xp)
    for s in range(SUBS):
        arrived(ra.at[xp, s], a_recv.at[xp, s])
        merge_into(cb.at[1, s], (p_ref.at[xp, s, c], ra.at[xp, s]), seqs)
        send(cb.at[1, s], rd.at[s], b_send.at[0], rd_recv.at[s], to_xp)
    for s in range(SUBS):
        pass_on(s)
    attend_both(x)
    for s in range(SUBS):
        arrived(ra.at[x, s], a_recv.at[x, s])
        merge_into(cb.at[3, s], (p_ref.at[x, s, c], ra.at[x, s]), seqs)
    sink = jnp.zeros((heads, LANES), jnp.float32)
    head_row = lax.broadcasted_iota(jnp.int32, sink.shape, 0)
    for h in range(heads):
        sink = jnp.where(head_row == h, sink_ref[c * heads + h], sink)
    for s in range(SUBS):
        arrived(rd.at[s], rd_recv.at[s])
        arrived(rm.at[s], rm_recv.at[s])
        parts = (cb.at[3, s], rd.at[s], rm.at[s])
        top, total, scales = merge_parts(parts, seqs)
        inverse = 1.0 / (pltpu.roll(total, HALF, 1) + jnp.exp(sink - top))
        columns = [[lane_column(scale * inverse, i) for scale in scales] for i in range(seqs)]
        outs = [out.astype(jnp.bfloat16).astype(jnp.float32) for out in weighted_sums(columns, parts, seqs)]
        for i in range(seqs):
            own_o[s, pl.ds(i * heads, heads), :] = outs[i]
        send(own_o.at[s], other_o.at[s], o_send.at[0], o_recv.at[s], partner)

    def head_rows(ref):
        columns = []
        for h in range(heads):
            columns.append(jnp.concatenate(
                [ref[s, pl.ds(h, seqs, stride=heads), :] for s in range(SUBS)], axis=0).astype(jnp.bfloat16))
        return jnp.concatenate(columns, axis=1)

    own_rows = head_rows(own_o)
    w_copies[0].wait()
    for q in range(SUBS):
        part = jnp.dot(own_rows, wbuf[0, :, pl.ds(q * cols_sub, cols_sub)], preferred_element_type=jnp.float32)
        for r in range(RING):
            z[q, r] = part[r * block_rows : (r + 1) * block_rows]
    for s in range(SUBS):
        arrived(other_o.at[s], o_recv.at[s])
    other_rows = head_rows(other_o)
    w_copies[1].wait()
    for q in range(SUBS):
        part = jnp.dot(other_rows, wbuf[1, :, pl.ds(q * cols_sub, cols_sub)], preferred_element_type=jnp.float32)
        for r in range(RING):
            z[q, r] += part[r * block_rows : (r + 1) * block_rows]
        send(z.at[q, yo], yrl.at[q], d_send.at[0], yrl_recv.at[q], to_yn)
        send(z.at[q, yp], yrd.at[q], d_send.at[0], yrd_recv.at[q], to_yp)
    for q in range(SUBS):
        arrived(yrl.at[q], yrl_recv.at[q])
        ym[q] = z[q, yn] + yrl[q]
        send(ym.at[q], yrm.at[q], d_send.at[0], yrm_recv.at[q], to_yn)
    chunk = g.shape[3:]
    sent(ra, a_send.at[0])
    sent(cb.at[pl.ds(0, 3)], b_send.at[0])
    sent(own_o, o_send.at[0])
    sent(g.reshape((-1,) + chunk).at[pl.ds(0, 3 * SUBS)], d_send.at[0])
    x_copy.wait()
    bo_copy.wait()
    bias_rows[...] = bo_ref[...].astype(jnp.float32)

    def store(q, xx, yy, core, value):
        rows = pl.ds(pl.multiple_of((xx * RING + yy) * block_rows, block_rows), block_rows)
        cols = pl.ds(pl.multiple_of(core * cols_core + q * cols_sub, LANES), cols_sub)
        out_ref[rows, cols] = value.astype(jnp.bfloat16)

    def slot(q, first, second):
        return (first, second) if q == 0 else (second, first)

    ahead = ((to_xn, to_xp), (to_yn, to_yp))
    first_now, first_n, first_p, first_o = (x, y), (xn, yn), (xp, yp), (xo, yo)

    pushes = []

    def push(q, first, second, where):
        xx, yy = slot(q, first, second)
        pushes.append(q)
        send(g.at[q, xx, yy], g.at[q, xx, yy], g_send.at[0], g_recv.at[q, xx, yy], where)

    def share(q, first, second):
        xx, yy = slot(q, first, second)
        send(g.at[q, xx, yy], gp.at[q, xx, yy], gp_send.at[0], gp_recv.at[q, xx, yy], partner)

    def receive(q, first, second):
        xx, yy = slot(q, first, second)
        arrived(g.at[q, xx, yy], g_recv.at[q, xx, yy])

    def keep(q, first, second):
        xx, yy = slot(q, first, second)
        store(q, xx, yy, c, g[q, xx, yy])

    for q in range(SUBS):
        arrived(yrd.at[q], yrd_recv.at[q])
        arrived(yrm.at[q], yrm_recv.at[q])
        first_row = (c * cols_core + q * cols_sub) // LANES
        bias = jnp.concatenate([bias_rows[pl.ds(first_row + t, 1), :] for t in range(cols_sub // LANES)], axis=1)
        summed = z[q, y] + yrd[q] + yrm[q]
        final = xbuf[:, pl.ds(q * cols_sub, cols_sub)].astype(jnp.float32) + summed + bias
        g[q, x, y] = final.astype(jnp.bfloat16).astype(jnp.float32)
        for axis in (q, 1 - q):
            for kind in range(2):
                push(q, first_now[q], first_now[1 - q], ahead[axis][kind])
        share(q, first_now[q], first_now[1 - q])

    def spread(q, first, forward):
        other = 1 - q
        receive(q, first, first_now[other])
        if forward:
            push(q, first, first_now[other], ahead[q][0])
        for kind in range(2):
            push(q, first, first_now[other], ahead[other][kind])
        share(q, first, first_now[other])
        keep(q, first, first_now[other])

    def settle(q, first, second, forward):
        receive(q, first, second)
        if forward:
            push(q, first, second, ahead[1 - q][0])
        share(q, first, second)
        keep(q, first, second)

    both = range(SUBS)
    for q in both:
        spread(q, first_p[q], True)
    for q in both:
        spread(q, first_n[q], False)
    for q in both:
        keep(q, first_now[q], first_now[1 - q])
    for q in both:
        settle(q, first_now[q], first_p[1 - q], True)
    for q in both:
        settle(q, first_now[q], first_n[1 - q], False)
    for q in both:
        spread(q, first_o[q], False)
    for first in (first_p, first_n):
        for q in both:
            settle(q, first[q], first_p[1 - q], True)
        for q in both:
            settle(q, first[q], first_n[1 - q], False)
    for q in both:
        settle(q, first_now[q], first_o[1 - q], False)
    for q in both:
        settle(q, first_o[q], first_p[1 - q], True)
    for q in both:
        settle(q, first_o[q], first_n[1 - q], False)
    for first in (first_p, first_n, first_o):
        for q in both:
            settle(q, first[q], first_o[1 - q], False)
    orders = [first_now, first_p, first_n, first_o]
    for xi in range(RING):
        for yi in range(RING):
            for q in both:
                xx, yy = slot(q, orders[xi][q], orders[yi][1 - q])
                arrived(gp.at[q, xx, yy], gp_recv.at[q, xx, yy])
                store(q, xx, yy, 1 - c, gp[q, xx, yy])
    sent(g.reshape((-1,) + chunk).at[pl.ds(0, len(pushes))], g_send.at[0])
    sent(gp, gp_send.at[0])


def combine(queries, k_out, v_out, seq_lens, sinks, hidden, b_o, w_o):
    num_seqs, d_model = hidden.shape
    seqs = num_seqs // (RING * SUBS)
    kv = CORES
    heads = sinks.shape[0] // kv
    cols_core = d_model // CORES
    cols_sub = cols_core // SUBS
    block_rows = num_seqs // (RING * RING)
    part = (seqs + 1, heads, LANES)
    f32, bf16 = jnp.float32, jnp.bfloat16
    dma = pltpu.SemaphoreType.DMA
    vmem = pl.BlockSpec(memory_space=pltpu.VMEM)
    hbm = pl.BlockSpec(memory_space=pl.ANY)
    smem = pl.BlockSpec(memory_space=pltpu.SMEM)
    chunk = (block_rows, cols_sub)
    return pl.pallas_call(
        functools.partial(combine_kernel, seqs, LANES ** -0.5),
        out_shape=jax.ShapeDtypeStruct((num_seqs, d_model), bf16),
        in_specs=[vmem, vmem, vmem, smem, smem, hbm, hbm, hbm],
        out_specs=vmem,
        scratch_shapes=[
            pltpu.VMEM((RING, SUBS, kv) + part, f32),
            pltpu.VMEM(b_o.shape, bf16),
            pltpu.VMEM(b_o.shape, f32),
            pltpu.VMEM((RING, SUBS) + part, f32),
            pltpu.VMEM((RING, SUBS) + part, f32),
            pltpu.VMEM((SUBS,) + part, f32),
            pltpu.VMEM((SUBS,) + part, f32),
            pltpu.VMEM((SUBS,) + part, f32),
            pltpu.VMEM((SUBS, seqs * heads, LANES), f32),
            pltpu.VMEM((SUBS, seqs * heads, LANES), f32),
            pltpu.VMEM((2, w_o.shape[0] // 2, cols_core), bf16),
            pltpu.VMEM((block_rows, cols_core), bf16),
            pltpu.VMEM((SUBS, RING) + chunk, f32),
            pltpu.VMEM((SUBS,) + chunk, f32),
            pltpu.VMEM((SUBS,) + chunk, f32),
            pltpu.VMEM((SUBS,) + chunk, f32),
            pltpu.VMEM((SUBS,) + chunk, f32),
            pltpu.VMEM((SUBS, RING, RING) + chunk, f32),
            pltpu.VMEM((SUBS, RING, RING) + chunk, f32),
            dma((2,)), dma((2,)), dma((1,)), dma((RING, SUBS)), dma((1,)),
            dma((SUBS,)), dma((SUBS,)), dma((SUBS,)), dma((1,)), dma((SUBS,)),
            dma((1,)), dma((SUBS,)), dma((SUBS,)), dma((SUBS,)),
            dma((1,)), dma((SUBS, RING, RING)), dma((1,)), dma((SUBS, RING, RING)),
        ],
        compiler_params=pltpu.CompilerParams(collective_id=0, has_side_effects=True, vmem_limit_bytes=COMBINE_MIB * 2**20),
        cost_estimate=pl.CostEstimate(flops=2 * num_seqs // RING * w_o.shape[0] * cols_core, bytes_accessed=30 * 2**20, transcendentals=0),
        name="combine",
    )(queries, k_out, v_out, seq_lens, sinks, *(pltpu.with_memory_space_constraint(a, pltpu.HBM) for a in (hidden, b_o, w_o)))


def project_kernel(
    x_hbm, cos_hbm, sin_hbm, k_hbm, v_hbm, gain_hbm, w_hbm, bias_hbm,
    heads_ref, kbuf, vbuf,
    xbuf, cos, sin, gain, bias, hexp, wbuf, acc,
    in_sem, w_sem, cache_sem, send_sem, recv_sem,
):
    num_seqs, d_model = x_hbm.shape
    kv = w_hbm.shape[1]
    qkv = w_hbm.shape[2]
    tiles = qkv // LANES // CORES
    chunks, depth2, cols = wbuf.shape
    stride = heads_ref.shape[1] // (CORES * tiles)
    c = lax.axis_index("sp") % CORES
    partner = {"sp": lax.axis_index("sp") + 1 - 2 * c}
    w_rows = w_hbm.reshape(d_model * kv, qkv)
    first_col = pl.multiple_of(c * cols, LANES)

    def w_copy(chunk):
        return pltpu.make_async_copy(
            w_rows.at[pl.ds(chunk * depth2, depth2), pl.ds(first_col, cols)], wbuf.at[chunk], w_sem.at[chunk])

    small = [
        pltpu.make_async_copy(src, dst, in_sem.at[i])
        for i, (src, dst) in enumerate((
            (x_hbm, xbuf), (gain_hbm, gain), (cos_hbm, cos), (sin_hbm, sin), (bias_hbm, bias)))
    ]
    for copy in small:
        copy.start()
    for chunk in range(chunks):
        w_copy(chunk).start()
    barrier = pltpu.get_barrier_semaphore()
    pl.semaphore_signal(barrier, inc=1, device_id=partner, device_id_type=MESH)

    small[0].wait()
    small[1].wait()
    row = lax.broadcasted_iota(jnp.int32, (LANES, kv * LANES), 0)
    col = lax.broadcasted_iota(jnp.int32, (LANES, kv * LANES), 1)
    pick = (col == row * kv).astype(jnp.bfloat16)
    gains = gain[...].astype(jnp.float32)
    square = jnp.zeros((num_seqs, LANES), jnp.float32)
    for t in range(d_model // LANES):
        xt = xbuf[:, t * LANES : (t + 1) * LANES].astype(jnp.float32)
        square += xt * xt
    inv_rms = lax.rsqrt(jnp.sum(square, axis=-1, keepdims=True) / d_model + NORM_EPS)
    for t in range(d_model // LANES):
        xt = xbuf[:, t * LANES : (t + 1) * LANES].astype(jnp.float32)
        ht = (xt * inv_rms * gains[t : t + 1]).astype(jnp.bfloat16)
        spread = jnp.dot(ht, pick, preferred_element_type=jnp.float32).astype(jnp.bfloat16)
        for k in range(kv):
            for j in range(kv):
                piece = spread[:, j * LANES : (j + 1) * LANES]
                hexp[t * kv + j, k * num_seqs : (k + 1) * num_seqs] = pltpu.roll(piece, k, 1) if k else piece
    cache_copies = [pltpu.make_async_copy(src, dst, cache_sem.at[i]) for i, (src, dst) in enumerate(((k_hbm, kbuf), (v_hbm, vbuf)))]

    for copy in cache_copies:
        copy.start()
    pieces = depth2 // LANES
    for chunk in range(chunks):
        w_copy(chunk).wait()
        lhs = jnp.concatenate([hexp[chunk * pieces + i] for i in range(pieces)], axis=1)
        for t in range(0, tiles, 2):
            part = slice(t * LANES, min(t + 2, tiles) * LANES)
            product = jnp.dot(lhs, wbuf[chunk, :, part], preferred_element_type=jnp.float32)
            acc[:, part] = acc[:, part] + product if chunk else product

    for copy in small[2:]:
        copy.wait()
    cos_t = jnp.transpose(jnp.concatenate([cos[...], cos[...]], axis=0))
    sin_t = jnp.transpose(jnp.concatenate([-sin[...], sin[...]], axis=0))
    pl.semaphore_wait(barrier, 1)

    def mine(k):
        rows = tiles * stride
        return heads_ref.at[k, pl.ds(pl.multiple_of(c * rows, 8), rows)]

    for k in range(kv):
        for j in range(tiles):
            tile = c * tiles + j
            value = acc[k * num_seqs : (k + 1) * num_seqs, j * LANES : (j + 1) * LANES]
            value += bias[k : k + 1, pl.ds(pl.multiple_of(tile * LANES, LANES), LANES)].astype(jnp.float32)
            turned = value * cos_t + pltpu.roll(value, HALF, 1) * sin_t
            value = jnp.where(jnp.full(value.shape, tile, jnp.int32) == CORES * tiles - 1, value, turned)
            heads_ref[k, pl.ds(pl.multiple_of(tile * stride, 8), num_seqs), :] = value.astype(jnp.bfloat16).astype(jnp.float32)
        pltpu.make_async_remote_copy(
            src_ref=mine(k), dst_ref=mine(k), send_sem=send_sem.at[k], recv_sem=recv_sem.at[k],
            device_id=partner, device_id_type=MESH).start()
    for copy in cache_copies:
        copy.wait()
    for k in range(kv):
        copy = pltpu.make_async_remote_copy(
            src_ref=mine(k), dst_ref=mine(k), send_sem=send_sem.at[k], recv_sem=recv_sem.at[k],
            device_id=partner, device_id_type=MESH)
        copy.wait_send()
        copy.wait_recv()


def project(hidden, cos_t, sin_t, k_cache, v_cache, gain, w_qkv, b_qkv):
    num_seqs, d_model = hidden.shape
    kv, qkv = w_qkv.shape[1:]
    tiles = qkv // LANES
    chunks = 4
    depth2 = d_model * kv // chunks
    f32, bf16 = jnp.float32, jnp.bfloat16
    dma = pltpu.SemaphoreType.DMA
    hbm = pl.BlockSpec(memory_space=pl.ANY)
    vmem = pl.BlockSpec(memory_space=pltpu.VMEM)
    operands = (hidden, cos_t, sin_t, k_cache, v_cache, gain, w_qkv, b_qkv)
    return pl.pallas_call(
        project_kernel,
        out_shape=(pltpu.VMEM((kv, tiles * (num_seqs + 8), LANES), f32), pltpu.VMEM(k_cache.shape, bf16), pltpu.VMEM(v_cache.shape, bf16)),
        in_specs=[hbm] * len(operands),
        out_specs=(vmem, vmem, vmem),
        scratch_shapes=[
            pltpu.VMEM(hidden.shape, bf16),
            pltpu.VMEM(cos_t.shape, f32),
            pltpu.VMEM(sin_t.shape, f32),
            pltpu.VMEM(gain.shape, bf16),
            pltpu.VMEM(b_qkv.shape, bf16),
            pltpu.VMEM((d_model * kv // LANES, kv * num_seqs, LANES), bf16),
            pltpu.VMEM((chunks, depth2, qkv // CORES), bf16),
            pltpu.VMEM((kv * num_seqs, qkv // CORES), f32),
            dma((5,)), dma((chunks,)), dma((2,)), dma((kv,)), dma((kv,)),
        ],
        compiler_params=pltpu.CompilerParams(collective_id=1, has_side_effects=True, vmem_limit_bytes=PROJECT_MIB * 2**20),
        cost_estimate=pl.CostEstimate(flops=2 * num_seqs * d_model * kv * qkv, bytes_accessed=24 * 2**20, transcendentals=0),
        name="project",
    )(*(pltpu.with_memory_space_constraint(a, pltpu.HBM) for a in operands))


def update_kernel(lens, heads_ref, k_in, v_in, kbuf, vbuf, k_out, v_out, ko_sem, vo_sem):
    kv = heads_ref.shape[0]
    num_seqs, ctx2 = kbuf.shape[:2]
    blocks = ko_sem.shape[0]
    seqs = num_seqs // blocks
    stride = num_seqs + 8
    tiles = heads_ref.shape[1] // stride
    base = lax.axis_index("sp") * (ctx2 // kv)
    group = 16
    group_row = lax.broadcasted_iota(jnp.int32, (group, LANES), 0)

    def cache_write(hbm, buf, sem, block):
        rows = pl.ds(block * seqs, seqs)
        return pltpu.make_async_copy(buf.at[rows], hbm.at[rows], sem.at[block])

    @pl.loop(0, blocks)
    def _(block):
        found = []
        for i in range(seqs):
            b = block * seqs + i
            local = lens[b] - base
            here = jnp.logical_and(local >= 0, local < ctx2 // kv)
            place = jnp.where(here, local * kv, 0)
            start = pl.multiple_of(place // group * group, group)
            target = jnp.where(here, place - start, group)
            for n, buf in enumerate((kbuf, vbuf)):
                fresh = [heads_ref[k, pl.ds((tiles - 2 + n) * stride + b, 1), :] for k in range(kv)]
                found.append((buf, b, start, target, fresh, buf[b, pl.ds(start, group), :]))
        values = []
        for _, _, _, target, fresh, old in found:
            value = old.astype(jnp.float32)
            for k in range(kv):
                value = jnp.where(group_row == target + k, fresh[k], value)
            values.append(value.astype(jnp.bfloat16))
        for (buf, b, start, _, _, _), value in zip(found, values):
            buf[b, pl.ds(start, group), :] = value
        cache_write(k_out, kbuf, ko_sem, block).start()
        cache_write(v_out, vbuf, vo_sem, block).start()

    @pl.loop(0, blocks)
    def _(block):
        cache_write(k_out, kbuf, ko_sem, block).wait()
        cache_write(v_out, vbuf, vo_sem, block).wait()


def update(seq_lens, heads_out, k_near, v_near):
    blocks = RING * SUBS
    hbm = pl.BlockSpec(memory_space=pl.ANY)
    vmem = pl.BlockSpec(memory_space=pltpu.VMEM)
    near = pltpu.VMEM(k_near.shape, k_near.dtype)
    far = jax.ShapeDtypeStruct(k_near.shape, k_near.dtype)
    dma = pltpu.SemaphoreType.DMA
    return pl.pallas_call(
        update_kernel,
        out_shape=(near, near, far, far),
        in_specs=[pl.BlockSpec(memory_space=pltpu.SMEM), vmem, vmem, vmem],
        out_specs=(vmem, vmem, hbm, hbm),
        scratch_shapes=[dma((blocks,)), dma((blocks,))],
        input_output_aliases={2: 0, 3: 1},
        compiler_params=pltpu.CompilerParams(vmem_limit_bytes=UPDATE_MIB * 2**20),
        cost_estimate=pl.CostEstimate(flops=10**6, bytes_accessed=10 * 2**20, transcendentals=0),
        name="update",
    )(seq_lens, heads_out, k_near, v_near)


def solution(mesh):
    cache_spec = P("dp", "sp", "tp", None)

    def block_step(hidden, seq_lens, rope_cos, rope_sin, k_cache, v_cache, norm_gain, w_qkv, b_qkv, sink_logits, w_o, b_o):
        num_seqs, ctx, kv, head_dim = k_cache.shape
        assert head_dim == LANES and mesh.shape["tp"] == RING and mesh.shape["sp"] == RING * CORES
        flat = (num_seqs, ctx * kv, head_dim)
        heads_out, k_near, v_near = project(
            hidden, rope_cos.T, rope_sin.T, k_cache.reshape(flat), v_cache.reshape(flat), norm_gain.reshape(-1, LANES), w_qkv, b_qkv)
        k_near, v_near, k_out, v_out = update(seq_lens, heads_out, k_near, v_near)
        out_hidden = combine(heads_out, k_near, v_near, seq_lens, sink_logits, hidden, b_o.reshape(-1, LANES), w_o)
        return out_hidden, k_out.reshape(k_cache.shape), v_out.reshape(v_cache.shape)

    return jax.shard_map(block_step, mesh=mesh, in_specs=(P("dp", None), P("dp"), P("dp", None), P("dp", None), cache_spec, cache_spec, P(None), P(None, "tp", None), P("tp", None), P("tp"), P("tp", None), P(None)), out_specs=(P("dp", None), cache_spec, cache_spec), check_vma=False)
```

```python
import functools

import jax
import jax.numpy as jnp
from jax import lax
from jax.experimental import pallas as pl
from jax.experimental.pallas import tpu as pltpu
from jax.sharding import PartitionSpec as P

NORM_EPS = 1e-5
MESH = pl.DeviceIdType.MESH
LANES = 128
HALF = LANES // 2
SUBS = 2
CORES = 2
PROJECT_MIB = 30
UPDATE_MIB = 4
COMBINE_MIB = 26
WAVE = 4
RING = 4


def lane_column(tile, index):
    return tile[:, index : index + 1]


def merge_parts(parts, seqs):
    stats = [part[seqs] for part in parts]
    top = functools.reduce(jnp.maximum, stats)
    scales = [jnp.exp(stat - top) for stat in stats]
    total = sum(pltpu.roll(scale, HALF, 1) * stat for scale, stat in zip(scales, stats))
    return top, total, scales


def weighted_sums(columns, parts, seqs):
    loaded = [[part[i] for part in parts] for i in range(seqs)]
    scaled = [[column * value for column, value in zip(cols, values)] for cols, values in zip(columns, loaded)]
    return [functools.reduce(jnp.add, terms) for terms in scaled]


def merge_into(dst, parts, seqs):
    top, total, scales = merge_parts(parts, seqs)
    columns = [[lane_column(scale, i) for scale in scales] for i in range(seqs)]
    sums = weighted_sums(columns, parts, seqs)
    lane = lax.broadcasted_iota(jnp.int32, top.shape, 1)
    stats = jnp.where(lane < HALF, top, total)
    for i in range(seqs):
        dst[i] = sums[i]
    dst[seqs] = stats


def combine_kernel(
    seqs, logit_scale, q_ref, k_ref, v_ref, lens, sink_ref, x_hbm, bo_hbm, wo_hbm, out_ref,
    p_ref, bo_ref, bias_rows, ra, cb, rl, rm, rd, own_o, other_o, wbuf, xbuf, z, yrl, ym, yrm, yrd, g, gp,
    w_sem, x_sem, a_send, a_recv, b_send, rl_recv, rm_recv, rd_recv, o_send, o_recv,
    d_send, yrl_recv, yrm_recv, yrd_recv, g_send, g_recv, gp_send, gp_recv,
):
    y = lax.axis_index("tp")
    sp = lax.axis_index("sp")
    x = sp // CORES
    c = sp % CORES
    step = 1 - 2 * c
    xn, xp, xo = (x + step + RING) % RING, (x - step + RING) % RING, (x + 2) % RING
    yn, yp, yo = (y + step + RING) % RING, (y - step + RING) % RING, (y + 2) % RING
    partner = {"sp": x * CORES + 1 - c}
    to_xn, to_xp = {"sp": xn * CORES + c}, {"sp": xp * CORES + c}
    to_yn, to_yp = {"tp": yn}, {"tp": yp}

    rows_half = wo_hbm.shape[0] // 2
    cols_core = wo_hbm.shape[1] // CORES
    cols_sub = cols_core // SUBS
    heads = p_ref.shape[4]
    block_rows = z.shape[2]

    w_copies = []
    for k in range(2):
        rows = (c if k == 0 else 1 - c) * rows_half
        copy = pltpu.make_async_copy(
            wo_hbm.at[pl.ds(pl.multiple_of(rows, LANES), rows_half), pl.ds(pl.multiple_of(c * cols_core, LANES), cols_core)],
            wbuf.at[k], w_sem.at[k])
        copy.start()
        w_copies.append(copy)
    row0 = pl.multiple_of((x * RING + y) * block_rows, block_rows)
    x_copy = pltpu.make_async_copy(
        x_hbm.at[pl.ds(row0, block_rows), pl.ds(pl.multiple_of(c * cols_core, LANES), cols_core)], xbuf, x_sem.at[0])
    x_copy.start()
    bo_copy = pltpu.make_async_copy(bo_hbm, bo_ref, x_sem.at[1])
    bo_copy.start()

    barrier = pltpu.get_barrier_semaphore()
    for where in (partner, to_xn, to_xp, to_yn, to_yp):
        pl.semaphore_signal(barrier, inc=1, device_id=where, device_id_type=MESH)
    pl.semaphore_wait(barrier, 5)

    def send(src, dst, send_sem, recv_sem, where):
        copy = pltpu.make_async_remote_copy(
            src_ref=src, dst_ref=dst, send_sem=send_sem, recv_sem=recv_sem, device_id=where, device_id_type=MESH)
        copy.start()

    def sent(shape_of, send_sem):
        pltpu.make_async_remote_copy(
            src_ref=shape_of, dst_ref=shape_of, send_sem=send_sem, recv_sem=send_sem, device_id=partner, device_id_type=MESH).wait_send()

    def arrived(dst, recv_sem):
        pltpu.make_async_remote_copy(
            src_ref=dst, dst_ref=dst, send_sem=recv_sem, recv_sem=recv_sem, device_id=partner, device_id_type=MESH).wait_recv()

    kv = p_ref.shape[2]
    q_rows = kv * heads
    ctx2 = k_ref.shape[1]
    q_stride = q_ref.shape[1] // (heads + 2)
    row = lax.broadcasted_iota(jnp.int32, (q_rows, ctx2), 0)
    lane = lax.broadcasted_iota(jnp.int32, (q_rows, ctx2), 1)
    position = jnp.where(lane % kv == row // heads, lane // kv + sp * (ctx2 // kv), jnp.iinfo(jnp.int32).max)
    sinks = jnp.zeros((q_rows, LANES), jnp.float32)
    for i in range(q_rows):
        sinks = jnp.where(row == i, sink_ref[i], sinks)
    sink_col = jnp.max(sinks, axis=-1, keepdims=True)

    def attend(b, s):
        first = (b * SUBS + s) * seqs
        waves = [range(j, j + WAVE) for j in range(0, seqs, WAVE)]
        logits, tops, totals, weights, stats = {}, {}, {}, {}, jnp.zeros((q_rows, LANES), jnp.float32)
        for turn in range(len(waves) + 2):
            if turn < len(waves):
                for i in waves[turn]:
                    q = jnp.concatenate([q_ref[k, pl.ds(first + i, heads, stride=q_stride), :] for k in range(kv)], axis=0).astype(jnp.bfloat16)
                    logits[i] = lax.dot_general(q, k_ref[first + i], (((1,), (1,)), ((), ())), preferred_element_type=jnp.float32)
            if 0 <= turn - 1 < len(waves):
                members = waves[turn - 1]
                for i in members:
                    logits[i] = jnp.where(position <= lens[first + i], logits[i] * logit_scale, -jnp.inf)
                for i in members:
                    tops[i] = jnp.maximum(jnp.max(logits[i], axis=-1, keepdims=True), sink_col)
                for i in members:
                    weights[i] = jnp.exp(logits[i] - tops[i])
                for i in members:
                    totals[i] = jnp.sum(weights[i], axis=-1, keepdims=True)
            if 0 <= turn - 2:
                members = waves[turn - 2]
                numers = [
                    jnp.dot(weights[i].astype(jnp.bfloat16), v_ref[first + i], preferred_element_type=jnp.float32) for i in members]
                for i, numer in zip(members, numers):
                    for k in range(kv):
                        p_ref[b, s, k, i] = numer[k * heads : (k + 1) * heads]
                    stats = jnp.where(lane == i, tops[i], jnp.where(lane == HALF + i, totals[i], stats))
        for k in range(kv):
            p_ref[b, s, k, seqs] = stats[k * heads : (k + 1) * heads]
        send(p_ref.at[b, s, 1 - c], ra.at[b, s], a_send.at[0], a_recv.at[b, s], partner)

    def attend_both(b):
        @pl.loop(0, SUBS)
        def _(s):
            attend(b, s)

    def relay(s):
        arrived(ra.at[xo, s], a_recv.at[xo, s])
        merge_into(cb.at[0, s], (p_ref.at[xo, s, c], ra.at[xo, s]), seqs)
        send(cb.at[0, s], rl.at[s], b_send.at[0], rl_recv.at[s], to_xn)

    def pass_on(s):
        arrived(ra.at[xn, s], a_recv.at[xn, s])
        arrived(rl.at[s], rl_recv.at[s])
        merge_into(cb.at[2, s], (p_ref.at[xn, s, c], ra.at[xn, s], rl.at[s]), seqs)
        send(cb.at[2, s], rm.at[s], b_send.at[0], rm_recv.at[s], to_xn)

    attend_both(xo)
    attend(xn, 0)
    for s in range(SUBS):
        relay(s)
    for s in range(1, SUBS):
        attend(xn, s)
    attend_both(xp)
    for s in range(SUBS):
        arrived(ra.at[xp, s], a_recv.at[xp, s])
        merge_into(cb.at[1, s], (p_ref.at[xp, s, c], ra.at[xp, s]), seqs)
        send(cb.at[1, s], rd.at[s], b_send.at[0], rd_recv.at[s], to_xp)
    for s in range(SUBS):
        pass_on(s)
    attend_both(x)
    for s in range(SUBS):
        arrived(ra.at[x, s], a_recv.at[x, s])
        merge_into(cb.at[3, s], (p_ref.at[x, s, c], ra.at[x, s]), seqs)
    sink = jnp.zeros((heads, LANES), jnp.float32)
    head_row = lax.broadcasted_iota(jnp.int32, sink.shape, 0)
    for h in range(heads):
        sink = jnp.where(head_row == h, sink_ref[c * heads + h], sink)
    for s in range(SUBS):
        arrived(rd.at[s], rd_recv.at[s])
        arrived(rm.at[s], rm_recv.at[s])
        parts = (cb.at[3, s], rd.at[s], rm.at[s])
        top, total, scales = merge_parts(parts, seqs)
        inverse = 1.0 / (pltpu.roll(total, HALF, 1) + jnp.exp(sink - top))
        columns = [[lane_column(scale * inverse, i) for scale in scales] for i in range(seqs)]
        outs = [out.astype(jnp.bfloat16).astype(jnp.float32) for out in weighted_sums(columns, parts, seqs)]
        for i in range(seqs):
            own_o[s, pl.ds(i * heads, heads), :] = outs[i]
        send(own_o.at[s], other_o.at[s], o_send.at[0], o_recv.at[s], partner)

    def head_rows(ref):
        columns = []
        for h in range(heads):
            columns.append(jnp.concatenate(
                [ref[s, pl.ds(h, seqs, stride=heads), :] for s in range(SUBS)], axis=0).astype(jnp.bfloat16))
        return jnp.concatenate(columns, axis=1)

    own_rows = head_rows(own_o)
    w_copies[0].wait()
    for q in range(SUBS):
        part = jnp.dot(own_rows, wbuf[0, :, pl.ds(q * cols_sub, cols_sub)], preferred_element_type=jnp.float32)
        for r in range(RING):
            z[q, r] = part[r * block_rows : (r + 1) * block_rows]
    for s in range(SUBS):
        arrived(other_o.at[s], o_recv.at[s])
    other_rows = head_rows(other_o)
    w_copies[1].wait()
    for q in range(SUBS):
        part = jnp.dot(other_rows, wbuf[1, :, pl.ds(q * cols_sub, cols_sub)], preferred_element_type=jnp.float32)
        for r in range(RING):
            z[q, r] += part[r * block_rows : (r + 1) * block_rows]
        send(z.at[q, yo], yrl.at[q], d_send.at[0], yrl_recv.at[q], to_yn)
        send(z.at[q, yp], yrd.at[q], d_send.at[0], yrd_recv.at[q], to_yp)
    for q in range(SUBS):
        arrived(yrl.at[q], yrl_recv.at[q])
        ym[q] = z[q, yn] + yrl[q]
        send(ym.at[q], yrm.at[q], d_send.at[0], yrm_recv.at[q], to_yn)
    chunk = g.shape[3:]
    sent(ra, a_send.at[0])
    sent(cb.at[pl.ds(0, 3)], b_send.at[0])
    sent(own_o, o_send.at[0])
    sent(g.reshape((-1,) + chunk).at[pl.ds(0, 3 * SUBS)], d_send.at[0])
    x_copy.wait()
    bo_copy.wait()
    bias_rows[...] = bo_ref[...].astype(jnp.float32)

    def store(q, xx, yy, core, value):
        rows = pl.ds(pl.multiple_of((xx * RING + yy) * block_rows, block_rows), block_rows)
        cols = pl.ds(pl.multiple_of(core * cols_core + q * cols_sub, LANES), cols_sub)
        out_ref[rows, cols] = value.astype(jnp.bfloat16)

    def slot(q, first, second):
        return (first, second) if q == 0 else (second, first)

    ahead = ((to_xn, to_xp), (to_yn, to_yp))
    first_now, first_n, first_p, first_o = (x, y), (xn, yn), (xp, yp), (xo, yo)

    pushes = []

    def push(q, first, second, where):
        xx, yy = slot(q, first, second)
        pushes.append(q)
        send(g.at[q, xx, yy], g.at[q, xx, yy], g_send.at[0], g_recv.at[q, xx, yy], where)

    def share(q, first, second, group):
        xx, yy = slot(q, first, second)
        send(g.at[q, xx, yy], gp.at[q, xx, yy], gp_send.at[0], gp_recv.at[group], partner)

    def receive(q, first, second):
        xx, yy = slot(q, first, second)
        arrived(g.at[q, xx, yy], g_recv.at[q, xx, yy])

    def keep(q, first, second):
        xx, yy = slot(q, first, second)
        store(q, xx, yy, c, g[q, xx, yy])

    for q in range(SUBS):
        arrived(yrd.at[q], yrd_recv.at[q])
        arrived(yrm.at[q], yrm_recv.at[q])
        first_row = (c * cols_core + q * cols_sub) // LANES
        bias = jnp.concatenate([bias_rows[pl.ds(first_row + t, 1), :] for t in range(cols_sub // LANES)], axis=1)
        summed = z[q, y] + yrd[q] + yrm[q]
        final = xbuf[:, pl.ds(q * cols_sub, cols_sub)].astype(jnp.float32) + summed + bias
        g[q, x, y] = final.astype(jnp.bfloat16).astype(jnp.float32)
        for axis in (q, 1 - q):
            for kind in range(2):
                push(q, first_now[q], first_now[1 - q], ahead[axis][kind])
        share(q, first_now[q], first_now[1 - q], 0)

    def spread(q, first, forward):
        other = 1 - q
        receive(q, first, first_now[other])
        if forward:
            push(q, first, first_now[other], ahead[q][0])
        for kind in range(2):
            push(q, first, first_now[other], ahead[other][kind])
        share(q, first, first_now[other], 0)

    def settle(q, first, second, where, group):
        receive(q, first, second)
        for target in where:
            push(q, first, second, target)
        share(q, first, second, group)

    both = range(SUBS)
    along = [ahead[1 - q][0] for q in both]
    diagonal = dict(to_xn, **to_yn)
    steps = [
        (lambda q: spread(q, first_p[q], True), first_p, first_now),
        (lambda q: spread(q, first_n[q], False), first_n, first_now),
        (lambda q: settle(q, first_now[q], first_p[1 - q], (along[q],), 0), first_now, first_p),
        (lambda q: settle(q, first_now[q], first_n[1 - q], (), 0), first_now, first_n),
        (lambda q: settle(q, first_p[q], first_p[1 - q], (diagonal, along[q]), 0), first_p, first_p),
        (lambda q: spread(q, first_o[q], False), first_o, first_now),
        (lambda q: settle(q, first_n[q], first_p[1 - q], (along[q],), 0), first_n, first_p),
        (lambda q: settle(q, first_p[q], first_n[1 - q], (), 0), first_p, first_n),
        (lambda q: settle(q, first_n[q], first_n[1 - q], (), 0), first_n, first_n),
        (lambda q: settle(q, first_now[q], first_o[1 - q], (), 0), first_now, first_o),
        (lambda q: settle(q, first_o[q], first_p[1 - q], (), 1), first_o, first_p),
        (lambda q: settle(q, first_o[q], first_n[1 - q], (), 1), first_o, first_n),
        (lambda q: settle(q, first_p[q], first_o[1 - q], (), 1), first_p, first_o),
        (lambda q: settle(q, first_n[q], first_o[1 - q], (), 1), first_n, first_o),
        (lambda q: settle(q, first_o[q], first_o[1 - q], (), 2), first_o, first_o),
    ]
    for q in both:
        keep(q, first_now[q], first_now[1 - q])
    for step_fn, first, second in steps:
        for q in both:
            step_fn(q)
        for q in both:
            keep(q, first[q], second[1 - q])
    blocks = [(first_now, first_now, 0)] + [(first, second, 0) for _, first, second in steps[:10]]
    blocks += [(first, second, 1) for _, first, second in steps[10:14]] + [(first_o, first_o, 2)]
    for group in range(3):
        members = [(first, second) for first, second, which in blocks if which == group]
        arrived(gp.reshape((-1,) + chunk).at[pl.ds(0, SUBS * len(members))], gp_recv.at[group])
        for first, second in members:
            for q in both:
                xx, yy = slot(q, first[q], second[1 - q])
                store(q, xx, yy, 1 - c, gp[q, xx, yy])
    sent(g.reshape((-1,) + chunk).at[pl.ds(0, len(pushes))], g_send.at[0])
    sent(gp, gp_send.at[0])


def combine(queries, k_out, v_out, seq_lens, sinks, hidden, b_o, w_o):
    num_seqs, d_model = hidden.shape
    seqs = num_seqs // (RING * SUBS)
    kv = CORES
    heads = sinks.shape[0] // kv
    cols_core = d_model // CORES
    cols_sub = cols_core // SUBS
    block_rows = num_seqs // (RING * RING)
    part = (seqs + 1, heads, LANES)
    f32, bf16 = jnp.float32, jnp.bfloat16
    dma = pltpu.SemaphoreType.DMA
    vmem = pl.BlockSpec(memory_space=pltpu.VMEM)
    hbm = pl.BlockSpec(memory_space=pl.ANY)
    smem = pl.BlockSpec(memory_space=pltpu.SMEM)
    chunk = (block_rows, cols_sub)
    return pl.pallas_call(
        functools.partial(combine_kernel, seqs, LANES ** -0.5),
        out_shape=jax.ShapeDtypeStruct((num_seqs, d_model), bf16),
        in_specs=[vmem, vmem, vmem, smem, smem, hbm, hbm, hbm],
        out_specs=vmem,
        scratch_shapes=[
            pltpu.VMEM((RING, SUBS, kv) + part, f32),
            pltpu.VMEM(b_o.shape, bf16),
            pltpu.VMEM(b_o.shape, f32),
            pltpu.VMEM((RING, SUBS) + part, f32),
            pltpu.VMEM((RING, SUBS) + part, f32),
            pltpu.VMEM((SUBS,) + part, f32),
            pltpu.VMEM((SUBS,) + part, f32),
            pltpu.VMEM((SUBS,) + part, f32),
            pltpu.VMEM((SUBS, seqs * heads, LANES), f32),
            pltpu.VMEM((SUBS, seqs * heads, LANES), f32),
            pltpu.VMEM((2, w_o.shape[0] // 2, cols_core), bf16),
            pltpu.VMEM((block_rows, cols_core), bf16),
            pltpu.VMEM((SUBS, RING) + chunk, f32),
            pltpu.VMEM((SUBS,) + chunk, f32),
            pltpu.VMEM((SUBS,) + chunk, f32),
            pltpu.VMEM((SUBS,) + chunk, f32),
            pltpu.VMEM((SUBS,) + chunk, f32),
            pltpu.VMEM((SUBS, RING, RING) + chunk, f32),
            pltpu.VMEM((SUBS, RING, RING) + chunk, f32),
            dma((2,)), dma((2,)), dma((1,)), dma((RING, SUBS)), dma((1,)),
            dma((SUBS,)), dma((SUBS,)), dma((SUBS,)), dma((1,)), dma((SUBS,)),
            dma((1,)), dma((SUBS,)), dma((SUBS,)), dma((SUBS,)),
            dma((1,)), dma((SUBS, RING, RING)), dma((1,)), dma((3,)),
        ],
        compiler_params=pltpu.CompilerParams(collective_id=0, has_side_effects=True, vmem_limit_bytes=COMBINE_MIB * 2**20),
        cost_estimate=pl.CostEstimate(flops=2 * num_seqs // RING * w_o.shape[0] * cols_core, bytes_accessed=30 * 2**20, transcendentals=0),
        name="combine",
    )(queries, k_out, v_out, seq_lens, sinks, *(pltpu.with_memory_space_constraint(a, pltpu.HBM) for a in (hidden, b_o, w_o)))


def project_kernel(
    x_hbm, cos_hbm, sin_hbm, k_hbm, v_hbm, gain_hbm, w_hbm, bias_hbm,
    heads_ref, kbuf, vbuf,
    xbuf, cos, sin, gain, bias, hexp, wbuf, acc,
    in_sem, w_sem, cache_sem, send_sem, recv_sem,
):
    num_seqs, d_model = x_hbm.shape
    kv = w_hbm.shape[1]
    qkv = w_hbm.shape[2]
    tiles = qkv // LANES // CORES
    chunks, depth2, cols = wbuf.shape
    stride = heads_ref.shape[1] // (CORES * tiles)
    c = lax.axis_index("sp") % CORES
    partner = {"sp": lax.axis_index("sp") + 1 - 2 * c}
    w_rows = w_hbm.reshape(d_model * kv, qkv)
    first_col = pl.multiple_of(c * cols, LANES)

    def w_copy(chunk):
        return pltpu.make_async_copy(
            w_rows.at[pl.ds(chunk * depth2, depth2), pl.ds(first_col, cols)], wbuf.at[chunk], w_sem.at[chunk])

    small = [
        pltpu.make_async_copy(src, dst, in_sem.at[i])
        for i, (src, dst) in enumerate((
            (x_hbm, xbuf), (gain_hbm, gain), (cos_hbm, cos), (sin_hbm, sin), (bias_hbm, bias)))
    ]
    for copy in small:
        copy.start()
    for chunk in range(chunks):
        w_copy(chunk).start()
    barrier = pltpu.get_barrier_semaphore()
    pl.semaphore_signal(barrier, inc=1, device_id=partner, device_id_type=MESH)

    small[0].wait()
    small[1].wait()
    row = lax.broadcasted_iota(jnp.int32, (LANES, kv * LANES), 0)
    col = lax.broadcasted_iota(jnp.int32, (LANES, kv * LANES), 1)
    pick = (col == row * kv).astype(jnp.bfloat16)
    gains = gain[...].astype(jnp.float32)
    square = jnp.zeros((num_seqs, LANES), jnp.float32)
    for t in range(d_model // LANES):
        xt = xbuf[:, t * LANES : (t + 1) * LANES].astype(jnp.float32)
        square += xt * xt
    inv_rms = lax.rsqrt(jnp.sum(square, axis=-1, keepdims=True) / d_model + NORM_EPS)
    for t in range(d_model // LANES):
        xt = xbuf[:, t * LANES : (t + 1) * LANES].astype(jnp.float32)
        ht = (xt * inv_rms * gains[t : t + 1]).astype(jnp.bfloat16)
        spread = jnp.dot(ht, pick, preferred_element_type=jnp.float32).astype(jnp.bfloat16)
        for k in range(kv):
            for j in range(kv):
                piece = spread[:, j * LANES : (j + 1) * LANES]
                hexp[t * kv + j, k * num_seqs : (k + 1) * num_seqs] = pltpu.roll(piece, k, 1) if k else piece
    cache_copies = [pltpu.make_async_copy(src, dst, cache_sem.at[i]) for i, (src, dst) in enumerate(((k_hbm, kbuf), (v_hbm, vbuf)))]

    for copy in cache_copies:
        copy.start()
    pieces = depth2 // LANES
    for chunk in range(chunks):
        w_copy(chunk).wait()
        lhs = jnp.concatenate([hexp[chunk * pieces + i] for i in range(pieces)], axis=1)
        for t in range(0, tiles, 2):
            part = slice(t * LANES, min(t + 2, tiles) * LANES)
            product = jnp.dot(lhs, wbuf[chunk, :, part], preferred_element_type=jnp.float32)
            acc[:, part] = acc[:, part] + product if chunk else product

    for copy in small[2:]:
        copy.wait()
    cos_t = jnp.transpose(jnp.concatenate([cos[...], cos[...]], axis=0))
    sin_t = jnp.transpose(jnp.concatenate([-sin[...], sin[...]], axis=0))
    pl.semaphore_wait(barrier, 1)

    def mine(k):
        rows = tiles * stride
        return heads_ref.at[k, pl.ds(pl.multiple_of(c * rows, 8), rows)]

    for k in range(kv):
        for j in range(tiles):
            tile = c * tiles + j
            value = acc[k * num_seqs : (k + 1) * num_seqs, j * LANES : (j + 1) * LANES]
            value += bias[k : k + 1, pl.ds(pl.multiple_of(tile * LANES, LANES), LANES)].astype(jnp.float32)
            turned = value * cos_t + pltpu.roll(value, HALF, 1) * sin_t
            value = jnp.where(jnp.full(value.shape, tile, jnp.int32) == CORES * tiles - 1, value, turned)
            heads_ref[k, pl.ds(pl.multiple_of(tile * stride, 8), num_seqs), :] = value.astype(jnp.bfloat16).astype(jnp.float32)
        pltpu.make_async_remote_copy(
            src_ref=mine(k), dst_ref=mine(k), send_sem=send_sem.at[k], recv_sem=recv_sem.at[k],
            device_id=partner, device_id_type=MESH).start()
    for copy in cache_copies:
        copy.wait()
    for k in range(kv):
        copy = pltpu.make_async_remote_copy(
            src_ref=mine(k), dst_ref=mine(k), send_sem=send_sem.at[k], recv_sem=recv_sem.at[k],
            device_id=partner, device_id_type=MESH)
        copy.wait_send()
        copy.wait_recv()


def project(hidden, cos_t, sin_t, k_cache, v_cache, gain, w_qkv, b_qkv):
    num_seqs, d_model = hidden.shape
    kv, qkv = w_qkv.shape[1:]
    tiles = qkv // LANES
    chunks = 4
    depth2 = d_model * kv // chunks
    f32, bf16 = jnp.float32, jnp.bfloat16
    dma = pltpu.SemaphoreType.DMA
    hbm = pl.BlockSpec(memory_space=pl.ANY)
    vmem = pl.BlockSpec(memory_space=pltpu.VMEM)
    operands = (hidden, cos_t, sin_t, k_cache, v_cache, gain, w_qkv, b_qkv)
    return pl.pallas_call(
        project_kernel,
        out_shape=(pltpu.VMEM((kv, tiles * (num_seqs + 8), LANES), f32), pltpu.VMEM(k_cache.shape, bf16), pltpu.VMEM(v_cache.shape, bf16)),
        in_specs=[hbm] * len(operands),
        out_specs=(vmem, vmem, vmem),
        scratch_shapes=[
            pltpu.VMEM(hidden.shape, bf16),
            pltpu.VMEM(cos_t.shape, f32),
            pltpu.VMEM(sin_t.shape, f32),
            pltpu.VMEM(gain.shape, bf16),
            pltpu.VMEM(b_qkv.shape, bf16),
            pltpu.VMEM((d_model * kv // LANES, kv * num_seqs, LANES), bf16),
            pltpu.VMEM((chunks, depth2, qkv // CORES), bf16),
            pltpu.VMEM((kv * num_seqs, qkv // CORES), f32),
            dma((5,)), dma((chunks,)), dma((2,)), dma((kv,)), dma((kv,)),
        ],
        compiler_params=pltpu.CompilerParams(collective_id=1, has_side_effects=True, vmem_limit_bytes=PROJECT_MIB * 2**20),
        cost_estimate=pl.CostEstimate(flops=2 * num_seqs * d_model * kv * qkv, bytes_accessed=24 * 2**20, transcendentals=0),
        name="project",
    )(*(pltpu.with_memory_space_constraint(a, pltpu.HBM) for a in operands))


def update_kernel(lens, heads_ref, k_in, v_in, kbuf, vbuf, k_out, v_out, ko_sem, vo_sem):
    kv = heads_ref.shape[0]
    num_seqs, ctx2 = kbuf.shape[:2]
    blocks = ko_sem.shape[0]
    seqs = num_seqs // blocks
    stride = num_seqs + 8
    tiles = heads_ref.shape[1] // stride
    base = lax.axis_index("sp") * (ctx2 // kv)
    group = 16
    group_row = lax.broadcasted_iota(jnp.int32, (group, LANES), 0)

    def cache_write(hbm, buf, sem, block):
        rows = pl.ds(block * seqs, seqs)
        return pltpu.make_async_copy(buf.at[rows], hbm.at[rows], sem.at[block])

    @pl.loop(0, blocks)
    def _(block):
        found = []
        for i in range(seqs):
            b = block * seqs + i
            local = lens[b] - base
            here = jnp.logical_and(local >= 0, local < ctx2 // kv)
            place = jnp.where(here, local * kv, 0)
            start = pl.multiple_of(place // group * group, group)
            target = jnp.where(here, place - start, group)
            for n, buf in enumerate((kbuf, vbuf)):
                fresh = [heads_ref[k, pl.ds((tiles - 2 + n) * stride + b, 1), :] for k in range(kv)]
                found.append((buf, b, start, target, fresh, buf[b, pl.ds(start, group), :]))
        values = []
        for _, _, _, target, fresh, old in found:
            value = old.astype(jnp.float32)
            for k in range(kv):
                value = jnp.where(group_row == target + k, fresh[k], value)
            values.append(value.astype(jnp.bfloat16))
        for (buf, b, start, _, _, _), value in zip(found, values):
            buf[b, pl.ds(start, group), :] = value
        cache_write(k_out, kbuf, ko_sem, block).start()
        cache_write(v_out, vbuf, vo_sem, block).start()

    @pl.loop(0, blocks)
    def _(block):
        cache_write(k_out, kbuf, ko_sem, block).wait()
        cache_write(v_out, vbuf, vo_sem, block).wait()


def update(seq_lens, heads_out, k_near, v_near):
    blocks = RING * SUBS
    hbm = pl.BlockSpec(memory_space=pl.ANY)
    vmem = pl.BlockSpec(memory_space=pltpu.VMEM)
    near = pltpu.VMEM(k_near.shape, k_near.dtype)
    far = jax.ShapeDtypeStruct(k_near.shape, k_near.dtype)
    dma = pltpu.SemaphoreType.DMA
    return pl.pallas_call(
        update_kernel,
        out_shape=(near, near, far, far),
        in_specs=[pl.BlockSpec(memory_space=pltpu.SMEM), vmem, vmem, vmem],
        out_specs=(vmem, vmem, hbm, hbm),
        scratch_shapes=[dma((blocks,)), dma((blocks,))],
        input_output_aliases={2: 0, 3: 1},
        compiler_params=pltpu.CompilerParams(vmem_limit_bytes=UPDATE_MIB * 2**20),
        cost_estimate=pl.CostEstimate(flops=10**6, bytes_accessed=10 * 2**20, transcendentals=0),
        name="update",
    )(seq_lens, heads_out, k_near, v_near)


def solution(mesh):
    cache_spec = P("dp", "sp", "tp", None)

    def block_step(hidden, seq_lens, rope_cos, rope_sin, k_cache, v_cache, norm_gain, w_qkv, b_qkv, sink_logits, w_o, b_o):
        num_seqs, ctx, kv, head_dim = k_cache.shape
        assert head_dim == LANES and mesh.shape["tp"] == RING and mesh.shape["sp"] == RING * CORES
        flat = (num_seqs, ctx * kv, head_dim)
        heads_out, k_near, v_near = project(
            hidden, rope_cos.T, rope_sin.T, k_cache.reshape(flat), v_cache.reshape(flat), norm_gain.reshape(-1, LANES), w_qkv, b_qkv)
        k_near, v_near, k_out, v_out = update(seq_lens, heads_out, k_near, v_near)
        out_hidden = combine(heads_out, k_near, v_near, seq_lens, sink_logits, hidden, b_o.reshape(-1, LANES), w_o)
        return out_hidden, k_out.reshape(k_cache.shape), v_out.reshape(v_cache.shape)

    return jax.shard_map(block_step, mesh=mesh, in_specs=(P("dp", None), P("dp"), P("dp", None), P("dp", None), cache_spec, cache_spec, P(None), P(None, "tp", None), P("tp", None), P("tp"), P("tp", None), P(None)), out_specs=(P("dp", None), cache_spec, cache_spec), check_vma=False)
```

```python
import functools

import jax
import jax.numpy as jnp
from jax import lax
from jax.experimental import pallas as pl
from jax.experimental.pallas import tpu as pltpu
from jax.sharding import PartitionSpec as P

NORM_EPS = 1e-5
MESH = pl.DeviceIdType.MESH
LANES = 128
HALF = LANES // 2
SUBS = 2
CORES = 2
PROJECT_MIB = 30
UPDATE_MIB = 4
COMBINE_MIB = 26
WAVE = 4
RING = 4


def lane_column(tile, index):
    return tile[:, index : index + 1]


def merge_parts(parts, seqs):
    stats = [part[seqs] for part in parts]
    top = functools.reduce(jnp.maximum, stats)
    scales = [jnp.exp(stat - top) for stat in stats]
    total = sum(pltpu.roll(scale, HALF, 1) * stat for scale, stat in zip(scales, stats))
    return top, total, scales


def weighted_sums(columns, parts, seqs):
    loaded = [[part[i] for part in parts] for i in range(seqs)]
    scaled = [[column * value for column, value in zip(cols, values)] for cols, values in zip(columns, loaded)]
    return [functools.reduce(jnp.add, terms) for terms in scaled]


def merge_into(dst, parts, seqs):
    top, total, scales = merge_parts(parts, seqs)
    columns = [[lane_column(scale, i) for scale in scales] for i in range(seqs)]
    sums = weighted_sums(columns, parts, seqs)
    lane = lax.broadcasted_iota(jnp.int32, top.shape, 1)
    stats = jnp.where(lane < HALF, top, total)
    for i in range(seqs):
        dst[i] = sums[i]
    dst[seqs] = stats


def attention_setup(kv, heads, ctx2, sink_ref):
    row = lax.broadcasted_iota(jnp.int32, (kv * heads, ctx2), 0)
    lane = lax.broadcasted_iota(jnp.int32, (kv * heads, ctx2), 1)
    base = lax.axis_index("sp") * (ctx2 // kv)
    position = jnp.where(lane % kv == row // heads, lane // kv + base, jnp.iinfo(jnp.int32).max)
    sinks = jnp.zeros((kv * heads, ctx2), jnp.float32)
    for i in range(kv * heads):
        sinks = jnp.where(row == i, sink_ref[i], sinks)
    return position, jnp.max(sinks, axis=-1, keepdims=True)


def attend_block(first, seqs, logit_scale, q_ref, k_ref, v_ref, lens, position, sink_col, dst):
    kv, _, heads, _ = dst.shape
    q_rows = kv * heads
    q_stride = q_ref.shape[1] // (heads + 2)
    lane = lax.broadcasted_iota(jnp.int32, (q_rows, LANES), 1)
    waves = [range(j, j + WAVE) for j in range(0, seqs, WAVE)]
    logits, tops, totals, weights, stats = {}, {}, {}, {}, jnp.zeros((q_rows, LANES), jnp.float32)
    for turn in range(len(waves) + 2):
        if turn < len(waves):
            for i in waves[turn]:
                q = jnp.concatenate([q_ref[k, pl.ds(first + i, heads, stride=q_stride), :] for k in range(kv)], axis=0).astype(jnp.bfloat16)
                logits[i] = lax.dot_general(q, k_ref[first + i], (((1,), (1,)), ((), ())), preferred_element_type=jnp.float32)
        if 0 <= turn - 1 < len(waves):
            members = waves[turn - 1]
            for i in members:
                logits[i] = jnp.where(position <= lens[first + i], logits[i] * logit_scale, -jnp.inf)
            for i in members:
                tops[i] = jnp.maximum(jnp.max(logits[i], axis=-1, keepdims=True), sink_col)
            for i in members:
                weights[i] = jnp.exp(logits[i] - tops[i])
            for i in members:
                totals[i] = jnp.sum(weights[i], axis=-1, keepdims=True)
        if 0 <= turn - 2:
            members = waves[turn - 2]
            numers = [
                jnp.dot(weights[i].astype(jnp.bfloat16), v_ref[first + i], preferred_element_type=jnp.float32) for i in members]
            for i, numer in zip(members, numers):
                for k in range(kv):
                    dst[k, i] = numer[k * heads : (k + 1) * heads]
                stats = jnp.where(lane == i, tops[i], jnp.where(lane == HALF + i, totals[i], stats))
    for k in range(kv):
        dst[k, seqs] = stats[k * heads : (k + 1) * heads]


def combine_kernel(
    seqs, logit_scale, early_ref, q_ref, k_ref, v_ref, lens, sink_ref, x_hbm, bo_hbm, wo_hbm, out_ref,
    p_ref, bo_ref, bias_rows, ra, cb, rl, rm, rd, own_o, other_o, wbuf, xbuf, z, yrl, ym, yrm, yrd, g, gp,
    w_sem, x_sem, a_send, a_recv, b_send, rl_recv, rm_recv, rd_recv, o_send, o_recv,
    d_send, yrl_recv, yrm_recv, yrd_recv, g_send, g_recv, gp_send, gp_recv,
):
    y = lax.axis_index("tp")
    sp = lax.axis_index("sp")
    x = sp // CORES
    c = sp % CORES
    step = 1 - 2 * c
    xn, xp, xo = (x + step + RING) % RING, (x - step + RING) % RING, (x + 2) % RING
    yn, yp, yo = (y + step + RING) % RING, (y - step + RING) % RING, (y + 2) % RING
    partner = {"sp": x * CORES + 1 - c}
    to_xn, to_xp = {"sp": xn * CORES + c}, {"sp": xp * CORES + c}
    to_yn, to_yp = {"tp": yn}, {"tp": yp}

    rows_half = wo_hbm.shape[0] // 2
    cols_core = wo_hbm.shape[1] // CORES
    cols_sub = cols_core // SUBS
    heads = p_ref.shape[4]
    block_rows = z.shape[2]

    w_copies = []
    for k in range(2):
        rows = (c if k == 0 else 1 - c) * rows_half
        copy = pltpu.make_async_copy(
            wo_hbm.at[pl.ds(pl.multiple_of(rows, LANES), rows_half), pl.ds(pl.multiple_of(c * cols_core, LANES), cols_core)],
            wbuf.at[k], w_sem.at[k])
        copy.start()
        w_copies.append(copy)
    row0 = pl.multiple_of((x * RING + y) * block_rows, block_rows)
    x_copy = pltpu.make_async_copy(
        x_hbm.at[pl.ds(row0, block_rows), pl.ds(pl.multiple_of(c * cols_core, LANES), cols_core)], xbuf, x_sem.at[0])
    x_copy.start()
    bo_copy = pltpu.make_async_copy(bo_hbm, bo_ref, x_sem.at[1])
    bo_copy.start()

    barrier = pltpu.get_barrier_semaphore()
    for where in (partner, to_xn, to_xp, to_yn, to_yp):
        pl.semaphore_signal(barrier, inc=1, device_id=where, device_id_type=MESH)
    pl.semaphore_wait(barrier, 5)

    def send(src, dst, send_sem, recv_sem, where):
        copy = pltpu.make_async_remote_copy(
            src_ref=src, dst_ref=dst, send_sem=send_sem, recv_sem=recv_sem, device_id=where, device_id_type=MESH)
        copy.start()

    def sent(shape_of, send_sem):
        pltpu.make_async_remote_copy(
            src_ref=shape_of, dst_ref=shape_of, send_sem=send_sem, recv_sem=send_sem, device_id=partner, device_id_type=MESH).wait_send()

    def arrived(dst, recv_sem):
        pltpu.make_async_remote_copy(
            src_ref=dst, dst_ref=dst, send_sem=recv_sem, recv_sem=recv_sem, device_id=partner, device_id_type=MESH).wait_recv()

    kv = p_ref.shape[2]
    ctx2 = k_ref.shape[1]
    position, sink_col = attention_setup(kv, heads, ctx2, sink_ref)

    def attend(b, s):
        attend_block((b * SUBS + s) * seqs, seqs, logit_scale, q_ref, k_ref, v_ref, lens, position, sink_col, p_ref.at[b, s])
        join(b, s)

    def join(b, s):
        send(p_ref.at[b, s, 1 - c], ra.at[b, s], a_send.at[0], a_recv.at[b, s], partner)

    def attend_both(b):
        @pl.loop(0, SUBS)
        def _(s):
            attend(b, s)

    def relay(s):
        arrived(ra.at[xo, s], a_recv.at[xo, s])
        merge_into(cb.at[0, s], (early_ref.at[s, c], ra.at[xo, s]), seqs)
        send(cb.at[0, s], rl.at[s], b_send.at[0], rl_recv.at[s], to_xn)

    def pass_on(s):
        arrived(ra.at[xn, s], a_recv.at[xn, s])
        arrived(rl.at[s], rl_recv.at[s])
        merge_into(cb.at[2, s], (p_ref.at[xn, s, c], ra.at[xn, s], rl.at[s]), seqs)
        send(cb.at[2, s], rm.at[s], b_send.at[0], rm_recv.at[s], to_xn)

    for s in range(SUBS):
        send(early_ref.at[s, 1 - c], ra.at[xo, s], a_send.at[0], a_recv.at[xo, s], partner)
    attend(xn, 0)
    for s in range(SUBS):
        relay(s)
    for s in range(1, SUBS):
        attend(xn, s)
    attend_both(xp)
    for s in range(SUBS):
        arrived(ra.at[xp, s], a_recv.at[xp, s])
        merge_into(cb.at[1, s], (p_ref.at[xp, s, c], ra.at[xp, s]), seqs)
        send(cb.at[1, s], rd.at[s], b_send.at[0], rd_recv.at[s], to_xp)
    for s in range(SUBS):
        pass_on(s)
    attend_both(x)
    for s in range(SUBS):
        arrived(ra.at[x, s], a_recv.at[x, s])
        merge_into(cb.at[3, s], (p_ref.at[x, s, c], ra.at[x, s]), seqs)
    sink = jnp.zeros((heads, LANES), jnp.float32)
    head_row = lax.broadcasted_iota(jnp.int32, sink.shape, 0)
    for h in range(heads):
        sink = jnp.where(head_row == h, sink_ref[c * heads + h], sink)
    for s in range(SUBS):
        arrived(rd.at[s], rd_recv.at[s])
        arrived(rm.at[s], rm_recv.at[s])
        parts = (cb.at[3, s], rd.at[s], rm.at[s])
        top, total, scales = merge_parts(parts, seqs)
        inverse = 1.0 / (pltpu.roll(total, HALF, 1) + jnp.exp(sink - top))
        columns = [[lane_column(scale * inverse, i) for scale in scales] for i in range(seqs)]
        outs = [out.astype(jnp.bfloat16).astype(jnp.float32) for out in weighted_sums(columns, parts, seqs)]
        for i in range(seqs):
            own_o[s, pl.ds(i * heads, heads), :] = outs[i]
        send(own_o.at[s], other_o.at[s], o_send.at[0], o_recv.at[s], partner)

    def head_rows(ref):
        columns = []
        for h in range(heads):
            columns.append(jnp.concatenate(
                [ref[s, pl.ds(h, seqs, stride=heads), :] for s in range(SUBS)], axis=0).astype(jnp.bfloat16))
        return jnp.concatenate(columns, axis=1)

    own_rows = head_rows(own_o)
    w_copies[0].wait()
    for q in range(SUBS):
        part = jnp.dot(own_rows, wbuf[0, :, pl.ds(q * cols_sub, cols_sub)], preferred_element_type=jnp.float32)
        for r in range(RING):
            z[q, r] = part[r * block_rows : (r + 1) * block_rows]
    for s in range(SUBS):
        arrived(other_o.at[s], o_recv.at[s])
    other_rows = head_rows(other_o)
    w_copies[1].wait()
    for q in range(SUBS):
        part = jnp.dot(other_rows, wbuf[1, :, pl.ds(q * cols_sub, cols_sub)], preferred_element_type=jnp.float32)
        for r in range(RING):
            z[q, r] += part[r * block_rows : (r + 1) * block_rows]
        send(z.at[q, yo], yrl.at[q], d_send.at[0], yrl_recv.at[q], to_yn)
        send(z.at[q, yp], yrd.at[q], d_send.at[0], yrd_recv.at[q], to_yp)
    for q in range(SUBS):
        arrived(yrl.at[q], yrl_recv.at[q])
        ym[q] = z[q, yn] + yrl[q]
        send(ym.at[q], yrm.at[q], d_send.at[0], yrm_recv.at[q], to_yn)
    chunk = g.shape[3:]
    sent(ra, a_send.at[0])
    sent(cb.at[pl.ds(0, 3)], b_send.at[0])
    sent(own_o, o_send.at[0])
    sent(g.reshape((-1,) + chunk).at[pl.ds(0, 3 * SUBS)], d_send.at[0])
    x_copy.wait()
    bo_copy.wait()
    bias_rows[...] = bo_ref[...].astype(jnp.float32)

    def store(q, xx, yy, core, value):
        rows = pl.ds(pl.multiple_of((xx * RING + yy) * block_rows, block_rows), block_rows)
        cols = pl.ds(pl.multiple_of(core * cols_core + q * cols_sub, LANES), cols_sub)
        out_ref[rows, cols] = value.astype(jnp.bfloat16)

    def slot(q, first, second):
        return (first, second) if q == 0 else (second, first)

    ahead = ((to_xn, to_xp), (to_yn, to_yp))
    first_now, first_n, first_p, first_o = (x, y), (xn, yn), (xp, yp), (xo, yo)

    pushes = []

    def push(q, first, second, where):
        xx, yy = slot(q, first, second)
        pushes.append(q)
        send(g.at[q, xx, yy], g.at[q, xx, yy], g_send.at[0], g_recv.at[q, xx, yy], where)

    def share(q, first, second, group):
        xx, yy = slot(q, first, second)
        send(g.at[q, xx, yy], gp.at[q, xx, yy], gp_send.at[0], gp_recv.at[group], partner)

    def receive(q, first, second):
        xx, yy = slot(q, first, second)
        arrived(g.at[q, xx, yy], g_recv.at[q, xx, yy])

    def keep(q, first, second):
        xx, yy = slot(q, first, second)
        store(q, xx, yy, c, g[q, xx, yy])

    for q in range(SUBS):
        arrived(yrd.at[q], yrd_recv.at[q])
        arrived(yrm.at[q], yrm_recv.at[q])
        first_row = (c * cols_core + q * cols_sub) // LANES
        bias = jnp.concatenate([bias_rows[pl.ds(first_row + t, 1), :] for t in range(cols_sub // LANES)], axis=1)
        summed = z[q, y] + yrd[q] + yrm[q]
        final = xbuf[:, pl.ds(q * cols_sub, cols_sub)].astype(jnp.float32) + summed + bias
        g[q, x, y] = final.astype(jnp.bfloat16).astype(jnp.float32)
        for axis in (q, 1 - q):
            for kind in range(2):
                push(q, first_now[q], first_now[1 - q], ahead[axis][kind])
        share(q, first_now[q], first_now[1 - q], 0)

    def spread(q, first, forward):
        other = 1 - q
        receive(q, first, first_now[other])
        if forward:
            push(q, first, first_now[other], ahead[q][0])
        for kind in range(2):
            push(q, first, first_now[other], ahead[other][kind])
        share(q, first, first_now[other], 0)

    def settle(q, first, second, where, group):
        receive(q, first, second)
        for target in where:
            push(q, first, second, target)
        share(q, first, second, group)

    both = range(SUBS)
    along = [ahead[1 - q][0] for q in both]
    diagonal = dict(to_xn, **to_yn)
    steps = [
        (lambda q: spread(q, first_p[q], True), first_p, first_now),
        (lambda q: spread(q, first_n[q], False), first_n, first_now),
        (lambda q: settle(q, first_now[q], first_p[1 - q], (along[q],), 0), first_now, first_p),
        (lambda q: settle(q, first_now[q], first_n[1 - q], (), 0), first_now, first_n),
        (lambda q: settle(q, first_p[q], first_p[1 - q], (diagonal, along[q]), 0), first_p, first_p),
        (lambda q: spread(q, first_o[q], False), first_o, first_now),
        (lambda q: settle(q, first_n[q], first_p[1 - q], (along[q],), 0), first_n, first_p),
        (lambda q: settle(q, first_p[q], first_n[1 - q], (), 0), first_p, first_n),
        (lambda q: settle(q, first_n[q], first_n[1 - q], (), 0), first_n, first_n),
        (lambda q: settle(q, first_now[q], first_o[1 - q], (), 0), first_now, first_o),
        (lambda q: settle(q, first_o[q], first_p[1 - q], (), 1), first_o, first_p),
        (lambda q: settle(q, first_o[q], first_n[1 - q], (), 1), first_o, first_n),
        (lambda q: settle(q, first_p[q], first_o[1 - q], (), 1), first_p, first_o),
        (lambda q: settle(q, first_n[q], first_o[1 - q], (), 1), first_n, first_o),
        (lambda q: settle(q, first_o[q], first_o[1 - q], (), 2), first_o, first_o),
    ]
    for q in both:
        keep(q, first_now[q], first_now[1 - q])
    for step_fn, first, second in steps:
        for q in both:
            step_fn(q)
        for q in both:
            keep(q, first[q], second[1 - q])
    blocks = [(first_now, first_now, 0)] + [(first, second, 0) for _, first, second in steps[:10]]
    blocks += [(first, second, 1) for _, first, second in steps[10:14]] + [(first_o, first_o, 2)]
    for group in range(3):
        members = [(first, second) for first, second, which in blocks if which == group]
        arrived(gp.reshape((-1,) + chunk).at[pl.ds(0, SUBS * len(members))], gp_recv.at[group])
        for first, second in members:
            for q in both:
                xx, yy = slot(q, first[q], second[1 - q])
                store(q, xx, yy, 1 - c, gp[q, xx, yy])
    sent(g.reshape((-1,) + chunk).at[pl.ds(0, len(pushes))], g_send.at[0])
    sent(gp, gp_send.at[0])


def combine(early, queries, k_out, v_out, seq_lens, sinks, hidden, b_o, w_o):
    num_seqs, d_model = hidden.shape
    seqs = num_seqs // (RING * SUBS)
    kv = CORES
    heads = sinks.shape[0] // kv
    cols_core = d_model // CORES
    cols_sub = cols_core // SUBS
    block_rows = num_seqs // (RING * RING)
    part = (seqs + 1, heads, LANES)
    f32, bf16 = jnp.float32, jnp.bfloat16
    dma = pltpu.SemaphoreType.DMA
    vmem = pl.BlockSpec(memory_space=pltpu.VMEM)
    hbm = pl.BlockSpec(memory_space=pl.ANY)
    smem = pl.BlockSpec(memory_space=pltpu.SMEM)
    chunk = (block_rows, cols_sub)
    return pl.pallas_call(
        functools.partial(combine_kernel, seqs, LANES ** -0.5),
        out_shape=jax.ShapeDtypeStruct((num_seqs, d_model), bf16),
        in_specs=[vmem, vmem, vmem, vmem, smem, smem, hbm, hbm, hbm],
        out_specs=vmem,
        scratch_shapes=[
            pltpu.VMEM((RING, SUBS, kv) + part, f32),
            pltpu.VMEM(b_o.shape, bf16),
            pltpu.VMEM(b_o.shape, f32),
            pltpu.VMEM((RING, SUBS) + part, f32),
            pltpu.VMEM((RING, SUBS) + part, f32),
            pltpu.VMEM((SUBS,) + part, f32),
            pltpu.VMEM((SUBS,) + part, f32),
            pltpu.VMEM((SUBS,) + part, f32),
            pltpu.VMEM((SUBS, seqs * heads, LANES), f32),
            pltpu.VMEM((SUBS, seqs * heads, LANES), f32),
            pltpu.VMEM((2, w_o.shape[0] // 2, cols_core), bf16),
            pltpu.VMEM((block_rows, cols_core), bf16),
            pltpu.VMEM((SUBS, RING) + chunk, f32),
            pltpu.VMEM((SUBS,) + chunk, f32),
            pltpu.VMEM((SUBS,) + chunk, f32),
            pltpu.VMEM((SUBS,) + chunk, f32),
            pltpu.VMEM((SUBS,) + chunk, f32),
            pltpu.VMEM((SUBS, RING, RING) + chunk, f32),
            pltpu.VMEM((SUBS, RING, RING) + chunk, f32),
            dma((2,)), dma((2,)), dma((1,)), dma((RING, SUBS)), dma((1,)),
            dma((SUBS,)), dma((SUBS,)), dma((SUBS,)), dma((1,)), dma((SUBS,)),
            dma((1,)), dma((SUBS,)), dma((SUBS,)), dma((SUBS,)),
            dma((1,)), dma((SUBS, RING, RING)), dma((1,)), dma((3,)),
        ],
        compiler_params=pltpu.CompilerParams(collective_id=0, has_side_effects=True, vmem_limit_bytes=COMBINE_MIB * 2**20),
        cost_estimate=pl.CostEstimate(flops=2 * num_seqs // RING * w_o.shape[0] * cols_core, bytes_accessed=30 * 2**20, transcendentals=0),
        name="combine",
    )(early, queries, k_out, v_out, seq_lens, sinks, *(pltpu.with_memory_space_constraint(a, pltpu.HBM) for a in (hidden, b_o, w_o)))


def project_kernel(
    x_hbm, cos_hbm, sin_hbm, k_hbm, v_hbm, gain_hbm, w_hbm, bias_hbm,
    heads_ref, kbuf, vbuf,
    xbuf, cos, sin, gain, bias, hexp, wbuf, acc,
    in_sem, w_sem, cache_sem, send_sem, recv_sem,
):
    num_seqs, d_model = x_hbm.shape
    kv = w_hbm.shape[1]
    qkv = w_hbm.shape[2]
    tiles = qkv // LANES // CORES
    chunks, depth2, cols = wbuf.shape
    stride = heads_ref.shape[1] // (CORES * tiles)
    c = lax.axis_index("sp") % CORES
    partner = {"sp": lax.axis_index("sp") + 1 - 2 * c}
    w_rows = w_hbm.reshape(d_model * kv, qkv)
    first_col = pl.multiple_of(c * cols, LANES)

    def w_copy(chunk):
        return pltpu.make_async_copy(
            w_rows.at[pl.ds(chunk * depth2, depth2), pl.ds(first_col, cols)], wbuf.at[chunk], w_sem.at[chunk])

    small = [
        pltpu.make_async_copy(src, dst, in_sem.at[i])
        for i, (src, dst) in enumerate((
            (x_hbm, xbuf), (gain_hbm, gain), (cos_hbm, cos), (sin_hbm, sin), (bias_hbm, bias)))
    ]
    for copy in small:
        copy.start()
    for chunk in range(chunks):
        w_copy(chunk).start()
    barrier = pltpu.get_barrier_semaphore()
    pl.semaphore_signal(barrier, inc=1, device_id=partner, device_id_type=MESH)

    small[0].wait()
    small[1].wait()
    row = lax.broadcasted_iota(jnp.int32, (LANES, kv * LANES), 0)
    col = lax.broadcasted_iota(jnp.int32, (LANES, kv * LANES), 1)
    pick = (col == row * kv).astype(jnp.bfloat16)
    gains = gain[...].astype(jnp.float32)
    square = jnp.zeros((num_seqs, LANES), jnp.float32)
    for t in range(d_model // LANES):
        xt = xbuf[:, t * LANES : (t + 1) * LANES].astype(jnp.float32)
        square += xt * xt
    inv_rms = lax.rsqrt(jnp.sum(square, axis=-1, keepdims=True) / d_model + NORM_EPS)
    def spread_chunk(chunk):
        for t in range(chunk * pieces // kv, (chunk + 1) * pieces // kv):
            xt = xbuf[:, t * LANES : (t + 1) * LANES].astype(jnp.float32)
            ht = (xt * inv_rms * gains[t : t + 1]).astype(jnp.bfloat16)
            spread = jnp.dot(ht, pick, preferred_element_type=jnp.float32).astype(jnp.bfloat16)
            for k in range(kv):
                for j in range(kv):
                    piece = spread[:, j * LANES : (j + 1) * LANES]
                    hexp[t * kv + j, k * num_seqs : (k + 1) * num_seqs] = pltpu.roll(piece, k, 1) if k else piece

    pieces = depth2 // LANES
    for chunk in range(chunks):
        spread_chunk(chunk)
    cache_copies = [pltpu.make_async_copy(src, dst, cache_sem.at[i]) for i, (src, dst) in enumerate(((k_hbm, kbuf), (v_hbm, vbuf)))]

    for copy in cache_copies:
        copy.start()
    for chunk in range(chunks):
        w_copy(chunk).wait()
        lhs = jnp.concatenate([hexp[chunk * pieces + i] for i in range(pieces)], axis=1)
        for t in range(0, tiles, 2):
            part = slice(t * LANES, min(t + 2, tiles) * LANES)
            product = jnp.dot(lhs, wbuf[chunk, :, part], preferred_element_type=jnp.float32)
            acc[:, part] = acc[:, part] + product if chunk else product

    for copy in small[2:]:
        copy.wait()
    cos_t = jnp.transpose(jnp.concatenate([cos[...], cos[...]], axis=0))
    sin_t = jnp.transpose(jnp.concatenate([-sin[...], sin[...]], axis=0))
    pl.semaphore_wait(barrier, 1)

    def mine(k):
        rows = tiles * stride
        return heads_ref.at[k, pl.ds(pl.multiple_of(c * rows, 8), rows)]

    for k in range(kv):
        for j in range(tiles):
            tile = c * tiles + j
            value = acc[k * num_seqs : (k + 1) * num_seqs, j * LANES : (j + 1) * LANES]
            value += bias[k : k + 1, pl.ds(pl.multiple_of(tile * LANES, LANES), LANES)].astype(jnp.float32)
            turned = value * cos_t + pltpu.roll(value, HALF, 1) * sin_t
            value = jnp.where(jnp.full(value.shape, tile, jnp.int32) == CORES * tiles - 1, value, turned)
            heads_ref[k, pl.ds(pl.multiple_of(tile * stride, 8), num_seqs), :] = value.astype(jnp.bfloat16).astype(jnp.float32)
        pltpu.make_async_remote_copy(
            src_ref=mine(k), dst_ref=mine(k), send_sem=send_sem.at[k], recv_sem=recv_sem.at[k],
            device_id=partner, device_id_type=MESH).start()
    for copy in cache_copies:
        copy.wait()
    for k in range(kv):
        copy = pltpu.make_async_remote_copy(
            src_ref=mine(k), dst_ref=mine(k), send_sem=send_sem.at[k], recv_sem=recv_sem.at[k],
            device_id=partner, device_id_type=MESH)
        copy.wait_send()
        copy.wait_recv()


def project(hidden, cos_t, sin_t, k_cache, v_cache, gain, w_qkv, b_qkv):
    num_seqs, d_model = hidden.shape
    kv, qkv = w_qkv.shape[1:]
    tiles = qkv // LANES
    chunks = 4
    depth2 = d_model * kv // chunks
    f32, bf16 = jnp.float32, jnp.bfloat16
    dma = pltpu.SemaphoreType.DMA
    hbm = pl.BlockSpec(memory_space=pl.ANY)
    vmem = pl.BlockSpec(memory_space=pltpu.VMEM)
    operands = (hidden, cos_t, sin_t, k_cache, v_cache, gain, w_qkv, b_qkv)
    return pl.pallas_call(
        project_kernel,
        out_shape=(pltpu.VMEM((kv, tiles * (num_seqs + 8), LANES), f32), pltpu.VMEM(k_cache.shape, bf16), pltpu.VMEM(v_cache.shape, bf16)),
        in_specs=[hbm] * len(operands),
        out_specs=(vmem, vmem, vmem),
        scratch_shapes=[
            pltpu.VMEM(hidden.shape, bf16),
            pltpu.VMEM(cos_t.shape, f32),
            pltpu.VMEM(sin_t.shape, f32),
            pltpu.VMEM(gain.shape, bf16),
            pltpu.VMEM(b_qkv.shape, bf16),
            pltpu.VMEM((d_model * kv // LANES, kv * num_seqs, LANES), bf16),
            pltpu.VMEM((chunks, depth2, qkv // CORES), bf16),
            pltpu.VMEM((kv * num_seqs, qkv // CORES), f32),
            dma((5,)), dma((chunks,)), dma((2,)), dma((kv,)), dma((kv,)),
        ],
        compiler_params=pltpu.CompilerParams(collective_id=1, has_side_effects=True, vmem_limit_bytes=PROJECT_MIB * 2**20),
        cost_estimate=pl.CostEstimate(flops=2 * num_seqs * d_model * kv * qkv, bytes_accessed=24 * 2**20, transcendentals=0),
        name="project",
    )(*(pltpu.with_memory_space_constraint(a, pltpu.HBM) for a in operands))


def update_kernel(logit_scale, lens, sink_ref, heads_ref, k_in, v_in, kbuf, vbuf, k_out, v_out, early_ref, ko_sem, vo_sem):
    kv = heads_ref.shape[0]
    num_seqs, ctx2 = kbuf.shape[:2]
    blocks = ko_sem.shape[0]
    seqs = num_seqs // blocks
    stride = num_seqs + 8
    tiles = heads_ref.shape[1] // stride
    base = lax.axis_index("sp") * (ctx2 // kv)
    group = 16
    group_row = lax.broadcasted_iota(jnp.int32, (group, LANES), 0)

    def cache_write(hbm, buf, sem, block):
        rows = pl.ds(block * seqs, seqs)
        return pltpu.make_async_copy(buf.at[rows], hbm.at[rows], sem.at[block])

    @pl.loop(0, blocks)
    def _(block):
        found = []
        for i in range(seqs):
            b = block * seqs + i
            local = lens[b] - base
            here = jnp.logical_and(local >= 0, local < ctx2 // kv)
            place = jnp.where(here, local * kv, 0)
            start = pl.multiple_of(place // group * group, group)
            target = jnp.where(here, place - start, group)
            for n, buf in enumerate((kbuf, vbuf)):
                fresh = [heads_ref[k, pl.ds((tiles - 2 + n) * stride + b, 1), :] for k in range(kv)]
                found.append((buf, b, start, target, fresh, buf[b, pl.ds(start, group), :]))
        values = []
        for _, _, _, target, fresh, old in found:
            value = old.astype(jnp.float32)
            for k in range(kv):
                value = jnp.where(group_row == target + k, fresh[k], value)
            values.append(value.astype(jnp.bfloat16))
        for (buf, b, start, _, _, _), value in zip(found, values):
            buf[b, pl.ds(start, group), :] = value
        cache_write(k_out, kbuf, ko_sem, block).start()
        cache_write(v_out, vbuf, vo_sem, block).start()

    position, sink_col = attention_setup(kv, tiles - 2, ctx2, sink_ref)
    opposite = (lax.axis_index("sp") // CORES + RING // 2) % RING

    @pl.loop(0, SUBS)
    def _(s):
        attend_block((opposite * SUBS + s) * seqs, seqs, logit_scale, heads_ref, kbuf, vbuf, lens, position, sink_col, early_ref.at[s])

    @pl.loop(0, blocks)
    def _(block):
        cache_write(k_out, kbuf, ko_sem, block).wait()
        cache_write(v_out, vbuf, vo_sem, block).wait()


def update(seq_lens, sinks, heads_out, k_near, v_near):
    blocks = RING * SUBS
    hbm = pl.BlockSpec(memory_space=pl.ANY)
    vmem = pl.BlockSpec(memory_space=pltpu.VMEM)
    smem = pl.BlockSpec(memory_space=pltpu.SMEM)
    kv = heads_out.shape[0]
    heads = sinks.shape[0] // kv
    seqs = k_near.shape[0] // blocks
    near = pltpu.VMEM(k_near.shape, k_near.dtype)
    far = jax.ShapeDtypeStruct(k_near.shape, k_near.dtype)
    dma = pltpu.SemaphoreType.DMA
    return pl.pallas_call(
        functools.partial(update_kernel, LANES ** -0.5),
        out_shape=(near, near, far, far, pltpu.VMEM((SUBS, kv, seqs + 1, heads, LANES), jnp.float32)),
        in_specs=[smem, smem, vmem, vmem, vmem],
        out_specs=(vmem, vmem, hbm, hbm, vmem),
        scratch_shapes=[dma((blocks,)), dma((blocks,))],
        input_output_aliases={3: 0, 4: 1},
        compiler_params=pltpu.CompilerParams(vmem_limit_bytes=UPDATE_MIB * 2**20),
        cost_estimate=pl.CostEstimate(flops=10**6, bytes_accessed=10 * 2**20, transcendentals=0),
        name="update",
    )(seq_lens, sinks, heads_out, k_near, v_near)


def solution(mesh):
    cache_spec = P("dp", "sp", "tp", None)

    def block_step(hidden, seq_lens, rope_cos, rope_sin, k_cache, v_cache, norm_gain, w_qkv, b_qkv, sink_logits, w_o, b_o):
        num_seqs, ctx, kv, head_dim = k_cache.shape
        assert head_dim == LANES and mesh.shape["tp"] == RING and mesh.shape["sp"] == RING * CORES
        flat = (num_seqs, ctx * kv, head_dim)
        heads_out, k_near, v_near = project(
            hidden, rope_cos.T, rope_sin.T, k_cache.reshape(flat), v_cache.reshape(flat), norm_gain.reshape(-1, LANES), w_qkv, b_qkv)
        k_near, v_near, k_out, v_out, early = update(seq_lens, sink_logits, heads_out, k_near, v_near)
        out_hidden = combine(early, heads_out, k_near, v_near, seq_lens, sink_logits, hidden, b_o.reshape(-1, LANES), w_o)
        return out_hidden, k_out.reshape(k_cache.shape), v_out.reshape(v_cache.shape)

    return jax.shard_map(block_step, mesh=mesh, in_specs=(P("dp", None), P("dp"), P("dp", None), P("dp", None), cache_spec, cache_spec, P(None), P(None, "tp", None), P("tp", None), P("tp"), P("tp", None), P(None)), out_specs=(P("dp", None), cache_spec, cache_spec), check_vma=False)
```

```python
import functools

import jax
import jax.numpy as jnp
from jax import lax
from jax.experimental import pallas as pl
from jax.experimental.pallas import tpu as pltpu
from jax.sharding import PartitionSpec as P

NORM_EPS = 1e-5
MESH = pl.DeviceIdType.MESH
LANES = 128
HALF = LANES // 2
SUBS = 2
CORES = 2
PROJECT_MIB = 30
UPDATE_MIB = 4
COMBINE_MIB = 26
WAVE = 4
RING = 4


def lane_column(tile, index):
    return tile[:, index : index + 1]


def merge_parts(parts, seqs):
    stats = [part[seqs] for part in parts]
    top = functools.reduce(jnp.maximum, stats)
    scales = [jnp.exp(stat - top) for stat in stats]
    total = sum(pltpu.roll(scale, HALF, 1) * stat for scale, stat in zip(scales, stats))
    return top, total, scales


def weighted_sums(columns, parts, seqs):
    loaded = [[part[i] for part in parts] for i in range(seqs)]
    scaled = [[column * value for column, value in zip(cols, values)] for cols, values in zip(columns, loaded)]
    return [functools.reduce(jnp.add, terms) for terms in scaled]


def merge_into(dst, parts, seqs):
    top, total, scales = merge_parts(parts, seqs)
    columns = [[lane_column(scale, i) for scale in scales] for i in range(seqs)]
    sums = weighted_sums(columns, parts, seqs)
    lane = lax.broadcasted_iota(jnp.int32, top.shape, 1)
    stats = jnp.where(lane < HALF, top, total)
    for i in range(seqs):
        dst[i] = sums[i]
    dst[seqs] = stats


def attention_setup(kv, heads, ctx2, sink_ref):
    row = lax.broadcasted_iota(jnp.int32, (kv * heads, ctx2), 0)
    lane = lax.broadcasted_iota(jnp.int32, (kv * heads, ctx2), 1)
    base = lax.axis_index("sp") * (ctx2 // kv)
    position = jnp.where(lane % kv == row // heads, lane // kv + base, jnp.iinfo(jnp.int32).max)
    sinks = jnp.zeros((kv * heads, ctx2), jnp.float32)
    for i in range(kv * heads):
        sinks = jnp.where(row == i, sink_ref[i], sinks)
    return position, jnp.max(sinks, axis=-1, keepdims=True)


def attend_block(first, seqs, logit_scale, q_ref, k_ref, v_ref, lens, position, sink_col, dst):
    kv, _, heads, _ = dst.shape
    q_rows = kv * heads
    q_stride = q_ref.shape[1] // (heads + 2)
    lane = lax.broadcasted_iota(jnp.int32, (q_rows, LANES), 1)
    waves = [range(j, j + WAVE) for j in range(0, seqs, WAVE)]
    logits, tops, totals, weights, stats = {}, {}, {}, {}, jnp.zeros((q_rows, LANES), jnp.float32)
    for turn in range(len(waves) + 2):
        if turn < len(waves):
            for i in waves[turn]:
                q = jnp.concatenate([q_ref[k, pl.ds(first + i, heads, stride=q_stride), :] for k in range(kv)], axis=0).astype(jnp.bfloat16)
                logits[i] = lax.dot_general(q, k_ref[first + i], (((1,), (1,)), ((), ())), preferred_element_type=jnp.float32)
        if 0 <= turn - 1 < len(waves):
            members = waves[turn - 1]
            for i in members:
                logits[i] = jnp.where(position <= lens[first + i], logits[i] * logit_scale, -jnp.inf)
            for i in members:
                tops[i] = jnp.maximum(jnp.max(logits[i], axis=-1, keepdims=True), sink_col)
            for i in members:
                weights[i] = jnp.exp(logits[i] - tops[i])
            for i in members:
                totals[i] = jnp.sum(weights[i], axis=-1, keepdims=True)
        if 0 <= turn - 2:
            members = waves[turn - 2]
            numers = [
                jnp.dot(weights[i].astype(jnp.bfloat16), v_ref[first + i], preferred_element_type=jnp.float32) for i in members]
            for i, numer in zip(members, numers):
                for k in range(kv):
                    dst[k, i] = numer[k * heads : (k + 1) * heads]
                stats = jnp.where(lane == i, tops[i], jnp.where(lane == HALF + i, totals[i], stats))
    for k in range(kv):
        dst[k, seqs] = stats[k * heads : (k + 1) * heads]


def combine_kernel(
    seqs, logit_scale, early_ref, q_ref, k_ref, v_ref, lens, sink_ref, x_hbm, bo_hbm, wo_hbm, out_ref,
    p_ref, bo_ref, bias_rows, ra, cb, rl, rm, rd, own_o, other_o, wbuf, xbuf, z, yrl, ym, yrm, yrd, g, gp,
    w_sem, x_sem, a_send, a_recv, b_send, rl_recv, rm_recv, rd_recv, o_send, o_recv,
    d_send, yrl_recv, yrm_recv, yrd_recv, g_send, g_recv, gp_send, gp_recv,
):
    y = lax.axis_index("tp")
    sp = lax.axis_index("sp")
    x = sp // CORES
    c = sp % CORES
    step = 1 - 2 * c
    xn, xp, xo = (x + step + RING) % RING, (x - step + RING) % RING, (x + 2) % RING
    yn, yp, yo = (y + step + RING) % RING, (y - step + RING) % RING, (y + 2) % RING
    partner = {"sp": x * CORES + 1 - c}
    to_xn, to_xp = {"sp": xn * CORES + c}, {"sp": xp * CORES + c}
    to_yn, to_yp = {"tp": yn}, {"tp": yp}

    rows_half = wo_hbm.shape[0] // 2
    cols_core = wo_hbm.shape[1] // CORES
    cols_sub = cols_core // SUBS
    heads = p_ref.shape[4]
    block_rows = z.shape[2]

    w_copies = []
    for k in range(2):
        rows = (c if k == 0 else 1 - c) * rows_half
        copy = pltpu.make_async_copy(
            wo_hbm.at[pl.ds(pl.multiple_of(rows, LANES), rows_half), pl.ds(pl.multiple_of(c * cols_core, LANES), cols_core)],
            wbuf.at[k], w_sem.at[k])
        copy.start()
        w_copies.append(copy)
    row0 = pl.multiple_of((x * RING + y) * block_rows, block_rows)
    x_copy = pltpu.make_async_copy(
        x_hbm.at[pl.ds(row0, block_rows), pl.ds(pl.multiple_of(c * cols_core, LANES), cols_core)], xbuf, x_sem.at[0])
    x_copy.start()
    bo_copy = pltpu.make_async_copy(bo_hbm, bo_ref, x_sem.at[1])
    bo_copy.start()

    barrier = pltpu.get_barrier_semaphore()
    for where in (partner, to_xn, to_xp, to_yn, to_yp):
        pl.semaphore_signal(barrier, inc=1, device_id=where, device_id_type=MESH)
    pl.semaphore_wait(barrier, 5)

    def send(src, dst, send_sem, recv_sem, where):
        copy = pltpu.make_async_remote_copy(
            src_ref=src, dst_ref=dst, send_sem=send_sem, recv_sem=recv_sem, device_id=where, device_id_type=MESH)
        copy.start()

    def sent(shape_of, send_sem):
        pltpu.make_async_remote_copy(
            src_ref=shape_of, dst_ref=shape_of, send_sem=send_sem, recv_sem=send_sem, device_id=partner, device_id_type=MESH).wait_send()

    def arrived(dst, recv_sem):
        pltpu.make_async_remote_copy(
            src_ref=dst, dst_ref=dst, send_sem=recv_sem, recv_sem=recv_sem, device_id=partner, device_id_type=MESH).wait_recv()

    kv = p_ref.shape[2]
    ctx2 = k_ref.shape[1]
    position, sink_col = attention_setup(kv, heads, ctx2, sink_ref)

    def attend(b, s):
        attend_block((b * SUBS + s) * seqs, seqs, logit_scale, q_ref, k_ref, v_ref, lens, position, sink_col, p_ref.at[b, s])
        join(b, s)

    def join(b, s):
        send(p_ref.at[b, s, 1 - c], ra.at[b, s], a_send.at[0], a_recv.at[b, s], partner)

    def attend_both(b):
        @pl.loop(0, SUBS)
        def _(s):
            attend(b, s)

    def relay(s):
        arrived(ra.at[xo, s], a_recv.at[xo, s])
        merge_into(cb.at[0, s], (early_ref.at[s, c], ra.at[xo, s]), seqs)
        send(cb.at[0, s], rl.at[s], b_send.at[0], rl_recv.at[s], to_xn)

    def pass_on(s):
        arrived(ra.at[xn, s], a_recv.at[xn, s])
        arrived(rl.at[s], rl_recv.at[s])
        merge_into(cb.at[2, s], (p_ref.at[xn, s, c], ra.at[xn, s], rl.at[s]), seqs)
        send(cb.at[2, s], rm.at[s], b_send.at[0], rm_recv.at[s], to_xn)

    for s in range(SUBS):
        send(early_ref.at[s, 1 - c], ra.at[xo, s], a_send.at[0], a_recv.at[xo, s], partner)
    attend(xn, 0)
    for s in range(SUBS):
        relay(s)
    for s in range(1, SUBS):
        attend(xn, s)
    attend_both(xp)
    for s in range(SUBS):
        arrived(ra.at[xp, s], a_recv.at[xp, s])
        merge_into(cb.at[1, s], (p_ref.at[xp, s, c], ra.at[xp, s]), seqs)
        send(cb.at[1, s], rd.at[s], b_send.at[0], rd_recv.at[s], to_xp)
    for s in range(SUBS):
        pass_on(s)
    attend_both(x)
    for s in range(SUBS):
        arrived(ra.at[x, s], a_recv.at[x, s])
        merge_into(cb.at[3, s], (p_ref.at[x, s, c], ra.at[x, s]), seqs)
    sink = jnp.zeros((heads, LANES), jnp.float32)
    head_row = lax.broadcasted_iota(jnp.int32, sink.shape, 0)
    for h in range(heads):
        sink = jnp.where(head_row == h, sink_ref[c * heads + h], sink)
    for s in range(SUBS):
        arrived(rd.at[s], rd_recv.at[s])
        arrived(rm.at[s], rm_recv.at[s])
        parts = (cb.at[3, s], rd.at[s], rm.at[s])
        top, total, scales = merge_parts(parts, seqs)
        inverse = 1.0 / (pltpu.roll(total, HALF, 1) + jnp.exp(sink - top))
        columns = [[lane_column(scale * inverse, i) for scale in scales] for i in range(seqs)]
        outs = [out.astype(jnp.bfloat16).astype(jnp.float32) for out in weighted_sums(columns, parts, seqs)]
        for i in range(seqs):
            own_o[s, pl.ds(i * heads, heads), :] = outs[i]
        send(own_o.at[s], other_o.at[s], o_send.at[0], o_recv.at[s], partner)

    def head_rows(ref):
        columns = []
        for h in range(heads):
            columns.append(jnp.concatenate(
                [ref[s, pl.ds(h, seqs, stride=heads), :] for s in range(SUBS)], axis=0).astype(jnp.bfloat16))
        return jnp.concatenate(columns, axis=1)

    own_rows = head_rows(own_o)
    w_copies[0].wait()
    for q in range(SUBS):
        part = jnp.dot(own_rows, wbuf[0, :, pl.ds(q * cols_sub, cols_sub)], preferred_element_type=jnp.float32)
        for r in range(RING):
            z[q, r] = part[r * block_rows : (r + 1) * block_rows]
    for s in range(SUBS):
        arrived(other_o.at[s], o_recv.at[s])
    other_rows = head_rows(other_o)
    w_copies[1].wait()
    for q in range(SUBS):
        part = jnp.dot(other_rows, wbuf[1, :, pl.ds(q * cols_sub, cols_sub)], preferred_element_type=jnp.float32)
        for r in range(RING):
            z[q, r] += part[r * block_rows : (r + 1) * block_rows]
        send(z.at[q, yo], yrl.at[q], d_send.at[0], yrl_recv.at[q], to_yn)
        send(z.at[q, yp], yrd.at[q], d_send.at[0], yrd_recv.at[q], to_yp)
    for q in range(SUBS):
        arrived(yrl.at[q], yrl_recv.at[q])
        ym[q] = z[q, yn] + yrl[q]
        send(ym.at[q], yrm.at[q], d_send.at[0], yrm_recv.at[q], to_yn)
    chunk = g.shape[3:]
    sent(ra, a_send.at[0])
    sent(cb.at[pl.ds(0, 3)], b_send.at[0])
    sent(own_o, o_send.at[0])
    sent(g.reshape((-1,) + chunk).at[pl.ds(0, 3 * SUBS)], d_send.at[0])
    x_copy.wait()
    bo_copy.wait()
    bias_rows[...] = bo_ref[...].astype(jnp.float32)

    def store(q, xx, yy, core, value):
        rows = pl.ds(pl.multiple_of((xx * RING + yy) * block_rows, block_rows), block_rows)
        cols = pl.ds(pl.multiple_of(core * cols_core + q * cols_sub, LANES), cols_sub)
        out_ref[rows, cols] = value.astype(jnp.bfloat16)

    def slot(q, first, second):
        return (first, second) if q == 0 else (second, first)

    ahead = ((to_xn, to_xp), (to_yn, to_yp))
    first_now, first_n, first_p, first_o = (x, y), (xn, yn), (xp, yp), (xo, yo)

    pushes = []

    def push(q, first, second, where):
        xx, yy = slot(q, first, second)
        pushes.append(q)
        send(g.at[q, xx, yy], g.at[q, xx, yy], g_send.at[0], g_recv.at[q, xx, yy], where)

    def share(q, first, second, group):
        xx, yy = slot(q, first, second)
        send(g.at[q, xx, yy], gp.at[q, xx, yy], gp_send.at[0], gp_recv.at[group], partner)

    def receive(q, first, second):
        xx, yy = slot(q, first, second)
        arrived(g.at[q, xx, yy], g_recv.at[q, xx, yy])

    def keep(q, first, second):
        xx, yy = slot(q, first, second)
        store(q, xx, yy, c, g[q, xx, yy])

    for q in range(SUBS):
        arrived(yrd.at[q], yrd_recv.at[q])
        arrived(yrm.at[q], yrm_recv.at[q])
        first_row = (c * cols_core + q * cols_sub) // LANES
        bias = jnp.concatenate([bias_rows[pl.ds(first_row + t, 1), :] for t in range(cols_sub // LANES)], axis=1)
        summed = z[q, y] + yrd[q] + yrm[q]
        final = xbuf[:, pl.ds(q * cols_sub, cols_sub)].astype(jnp.float32) + summed + bias
        g[q, x, y] = final.astype(jnp.bfloat16).astype(jnp.float32)
        for axis in (q, 1 - q):
            for kind in range(2):
                push(q, first_now[q], first_now[1 - q], ahead[axis][kind])
        push(q, first_now[q], first_now[1 - q], dict(to_xn, **to_yn))
        share(q, first_now[q], first_now[1 - q], 0)

    def spread(q, first, forward, kinds):
        other = 1 - q
        receive(q, first, first_now[other])
        if forward:
            push(q, first, first_now[other], ahead[q][0])
        for kind in kinds:
            push(q, first, first_now[other], ahead[other][kind])
        share(q, first, first_now[other], 0)

    def settle(q, first, second, where, group):
        receive(q, first, second)
        for target in where:
            push(q, first, second, target)
        share(q, first, second, group)

    both = range(SUBS)
    along, onward = [ahead[1 - q][0] for q in both], [ahead[q][0] for q in both]
    diagonal = dict(to_xn, **to_yn)
    steps = [
        (lambda q: spread(q, first_p[q], True, (1,)), first_p, first_now),
        (lambda q: settle(q, first_now[q], first_p[1 - q], (along[q],), 0), first_now, first_p),
        (lambda q: spread(q, first_n[q], False, (0, 1)), first_n, first_now),
        (lambda q: settle(q, first_p[q], first_p[1 - q], (diagonal, along[q], onward[q]), 0), first_p, first_p),
        (lambda q: settle(q, first_now[q], first_n[1 - q], (), 0), first_now, first_n),
        (lambda q: spread(q, first_o[q], False, (1,)), first_o, first_now),
        (lambda q: settle(q, first_n[q], first_p[1 - q], (along[q],), 0), first_n, first_p),
        (lambda q: settle(q, first_p[q], first_n[1 - q], (), 0), first_p, first_n),
        (lambda q: settle(q, first_n[q], first_n[1 - q], (), 0), first_n, first_n),
        (lambda q: settle(q, first_now[q], first_o[1 - q], (), 0), first_now, first_o),
        (lambda q: settle(q, first_o[q], first_p[1 - q], (), 1), first_o, first_p),
        (lambda q: settle(q, first_p[q], first_o[1 - q], (), 1), first_p, first_o),
        (lambda q: settle(q, first_o[q], first_o[1 - q], (), 2), first_o, first_o),
        (lambda q: settle(q, first_o[q], first_n[1 - q], (), 1), first_o, first_n),
        (lambda q: settle(q, first_n[q], first_o[1 - q], (), 1), first_n, first_o),
    ]
    for q in both:
        keep(q, first_now[q], first_now[1 - q])
    for step_fn, first, second in steps:
        for q in both:
            step_fn(q)
        for q in both:
            keep(q, first[q], second[1 - q])
    blocks = [(first_now, first_now, 0)] + [(first, second, 0) for _, first, second in steps[:10]]
    blocks += [(first, second, 1 if first is not second else 2) for _, first, second in steps[10:]]
    for group in range(3):
        members = [(first, second) for first, second, which in blocks if which == group]
        arrived(gp.reshape((-1,) + chunk).at[pl.ds(0, SUBS * len(members))], gp_recv.at[group])
        for first, second in members:
            for q in both:
                xx, yy = slot(q, first[q], second[1 - q])
                store(q, xx, yy, 1 - c, gp[q, xx, yy])
    sent(g.reshape((-1,) + chunk).at[pl.ds(0, len(pushes))], g_send.at[0])
    sent(gp, gp_send.at[0])


def combine(early, queries, k_out, v_out, seq_lens, sinks, hidden, b_o, w_o):
    num_seqs, d_model = hidden.shape
    seqs = num_seqs // (RING * SUBS)
    kv = CORES
    heads = sinks.shape[0] // kv
    cols_core = d_model // CORES
    cols_sub = cols_core // SUBS
    block_rows = num_seqs // (RING * RING)
    part = (seqs + 1, heads, LANES)
    f32, bf16 = jnp.float32, jnp.bfloat16
    dma = pltpu.SemaphoreType.DMA
    vmem = pl.BlockSpec(memory_space=pltpu.VMEM)
    hbm = pl.BlockSpec(memory_space=pl.ANY)
    smem = pl.BlockSpec(memory_space=pltpu.SMEM)
    chunk = (block_rows, cols_sub)
    return pl.pallas_call(
        functools.partial(combine_kernel, seqs, LANES ** -0.5),
        out_shape=jax.ShapeDtypeStruct((num_seqs, d_model), bf16),
        in_specs=[vmem, vmem, vmem, vmem, smem, smem, hbm, hbm, hbm],
        out_specs=vmem,
        scratch_shapes=[
            pltpu.VMEM((RING, SUBS, kv) + part, f32),
            pltpu.VMEM(b_o.shape, bf16),
            pltpu.VMEM(b_o.shape, f32),
            pltpu.VMEM((RING, SUBS) + part, f32),
            pltpu.VMEM((RING, SUBS) + part, f32),
            pltpu.VMEM((SUBS,) + part, f32),
            pltpu.VMEM((SUBS,) + part, f32),
            pltpu.VMEM((SUBS,) + part, f32),
            pltpu.VMEM((SUBS, seqs * heads, LANES), f32),
            pltpu.VMEM((SUBS, seqs * heads, LANES), f32),
            pltpu.VMEM((2, w_o.shape[0] // 2, cols_core), bf16),
            pltpu.VMEM((block_rows, cols_core), bf16),
            pltpu.VMEM((SUBS, RING) + chunk, f32),
            pltpu.VMEM((SUBS,) + chunk, f32),
            pltpu.VMEM((SUBS,) + chunk, f32),
            pltpu.VMEM((SUBS,) + chunk, f32),
            pltpu.VMEM((SUBS,) + chunk, f32),
            pltpu.VMEM((SUBS, RING, RING) + chunk, f32),
            pltpu.VMEM((SUBS, RING, RING) + chunk, f32),
            dma((2,)), dma((2,)), dma((1,)), dma((RING, SUBS)), dma((1,)),
            dma((SUBS,)), dma((SUBS,)), dma((SUBS,)), dma((1,)), dma((SUBS,)),
            dma((1,)), dma((SUBS,)), dma((SUBS,)), dma((SUBS,)),
            dma((1,)), dma((SUBS, RING, RING)), dma((1,)), dma((3,)),
        ],
        compiler_params=pltpu.CompilerParams(collective_id=0, has_side_effects=True, vmem_limit_bytes=COMBINE_MIB * 2**20),
        cost_estimate=pl.CostEstimate(flops=2 * num_seqs // RING * w_o.shape[0] * cols_core, bytes_accessed=30 * 2**20, transcendentals=0),
        name="combine",
    )(early, queries, k_out, v_out, seq_lens, sinks, *(pltpu.with_memory_space_constraint(a, pltpu.HBM) for a in (hidden, b_o, w_o)))


def project_kernel(
    x_hbm, cos_hbm, sin_hbm, k_hbm, v_hbm, gain_hbm, w_hbm, bias_hbm,
    heads_ref, kbuf, vbuf,
    xbuf, cos, sin, gain, bias, hexp, wbuf, acc,
    in_sem, w_sem, cache_sem, send_sem, recv_sem,
):
    num_seqs, d_model = x_hbm.shape
    kv = w_hbm.shape[1]
    qkv = w_hbm.shape[2]
    tiles = qkv // LANES // CORES
    chunks, depth2, cols = wbuf.shape
    stride = heads_ref.shape[1] // (CORES * tiles)
    c = lax.axis_index("sp") % CORES
    partner = {"sp": lax.axis_index("sp") + 1 - 2 * c}
    w_rows = w_hbm.reshape(d_model * kv, qkv)
    first_col = pl.multiple_of(c * cols, LANES)

    def w_copy(chunk):
        return pltpu.make_async_copy(
            w_rows.at[pl.ds(chunk * depth2, depth2), pl.ds(first_col, cols)], wbuf.at[chunk], w_sem.at[chunk])

    small = [
        pltpu.make_async_copy(src, dst, in_sem.at[i])
        for i, (src, dst) in enumerate((
            (x_hbm, xbuf), (gain_hbm, gain), (cos_hbm, cos), (sin_hbm, sin), (bias_hbm, bias)))
    ]
    for copy in small:
        copy.start()
    for chunk in range(chunks):
        w_copy(chunk).start()
    barrier = pltpu.get_barrier_semaphore()
    pl.semaphore_signal(barrier, inc=1, device_id=partner, device_id_type=MESH)

    small[0].wait()
    small[1].wait()
    row = lax.broadcasted_iota(jnp.int32, (LANES, kv * LANES), 0)
    col = lax.broadcasted_iota(jnp.int32, (LANES, kv * LANES), 1)
    pick = (col == row * kv).astype(jnp.bfloat16)
    gains = gain[...].astype(jnp.float32)
    square = jnp.zeros((num_seqs, LANES), jnp.float32)
    for t in range(d_model // LANES):
        xt = xbuf[:, t * LANES : (t + 1) * LANES].astype(jnp.float32)
        square += xt * xt
    inv_rms = lax.rsqrt(jnp.sum(square, axis=-1, keepdims=True) / d_model + NORM_EPS)
    def spread_chunk(chunk):
        for t in range(chunk * pieces // kv, (chunk + 1) * pieces // kv):
            xt = xbuf[:, t * LANES : (t + 1) * LANES].astype(jnp.float32)
            ht = (xt * inv_rms * gains[t : t + 1]).astype(jnp.bfloat16)
            spread = jnp.dot(ht, pick, preferred_element_type=jnp.float32).astype(jnp.bfloat16)
            for k in range(kv):
                for j in range(kv):
                    piece = spread[:, j * LANES : (j + 1) * LANES]
                    hexp[t * kv + j, k * num_seqs : (k + 1) * num_seqs] = pltpu.roll(piece, k, 1) if k else piece

    pieces = depth2 // LANES
    for chunk in range(chunks):
        spread_chunk(chunk)
    cache_copies = [pltpu.make_async_copy(src, dst, cache_sem.at[i]) for i, (src, dst) in enumerate(((k_hbm, kbuf), (v_hbm, vbuf)))]

    for copy in cache_copies:
        copy.start()
    for chunk in range(chunks):
        w_copy(chunk).wait()
        lhs = jnp.concatenate([hexp[chunk * pieces + i] for i in range(pieces)], axis=1)
        for t in range(0, tiles, 2):
            part = slice(t * LANES, min(t + 2, tiles) * LANES)
            product = jnp.dot(lhs, wbuf[chunk, :, part], preferred_element_type=jnp.float32)
            acc[:, part] = acc[:, part] + product if chunk else product

    for copy in small[2:]:
        copy.wait()
    cos_t = jnp.transpose(jnp.concatenate([cos[...], cos[...]], axis=0))
    sin_t = jnp.transpose(jnp.concatenate([-sin[...], sin[...]], axis=0))
    pl.semaphore_wait(barrier, 1)

    def mine(k):
        rows = tiles * stride
        return heads_ref.at[k, pl.ds(pl.multiple_of(c * rows, 8), rows)]

    for k in range(kv):
        for j in range(tiles):
            tile = c * tiles + j
            value = acc[k * num_seqs : (k + 1) * num_seqs, j * LANES : (j + 1) * LANES]
            value += bias[k : k + 1, pl.ds(pl.multiple_of(tile * LANES, LANES), LANES)].astype(jnp.float32)
            turned = value * cos_t + pltpu.roll(value, HALF, 1) * sin_t
            value = jnp.where(jnp.full(value.shape, tile, jnp.int32) == CORES * tiles - 1, value, turned)
            heads_ref[k, pl.ds(pl.multiple_of(tile * stride, 8), num_seqs), :] = value.astype(jnp.bfloat16).astype(jnp.float32)
        pltpu.make_async_remote_copy(
            src_ref=mine(k), dst_ref=mine(k), send_sem=send_sem.at[k], recv_sem=recv_sem.at[k],
            device_id=partner, device_id_type=MESH).start()
    for copy in cache_copies:
        copy.wait()
    for k in range(kv):
        copy = pltpu.make_async_remote_copy(
            src_ref=mine(k), dst_ref=mine(k), send_sem=send_sem.at[k], recv_sem=recv_sem.at[k],
            device_id=partner, device_id_type=MESH)
        copy.wait_send()
        copy.wait_recv()


def project(hidden, cos_t, sin_t, k_cache, v_cache, gain, w_qkv, b_qkv):
    num_seqs, d_model = hidden.shape
    kv, qkv = w_qkv.shape[1:]
    tiles = qkv // LANES
    chunks = 4
    depth2 = d_model * kv // chunks
    f32, bf16 = jnp.float32, jnp.bfloat16
    dma = pltpu.SemaphoreType.DMA
    hbm = pl.BlockSpec(memory_space=pl.ANY)
    vmem = pl.BlockSpec(memory_space=pltpu.VMEM)
    operands = (hidden, cos_t, sin_t, k_cache, v_cache, gain, w_qkv, b_qkv)
    return pl.pallas_call(
        project_kernel,
        out_shape=(pltpu.VMEM((kv, tiles * (num_seqs + 8), LANES), f32), pltpu.VMEM(k_cache.shape, bf16), pltpu.VMEM(v_cache.shape, bf16)),
        in_specs=[hbm] * len(operands),
        out_specs=(vmem, vmem, vmem),
        scratch_shapes=[
            pltpu.VMEM(hidden.shape, bf16),
            pltpu.VMEM(cos_t.shape, f32),
            pltpu.VMEM(sin_t.shape, f32),
            pltpu.VMEM(gain.shape, bf16),
            pltpu.VMEM(b_qkv.shape, bf16),
            pltpu.VMEM((d_model * kv // LANES, kv * num_seqs, LANES), bf16),
            pltpu.VMEM((chunks, depth2, qkv // CORES), bf16),
            pltpu.VMEM((kv * num_seqs, qkv // CORES), f32),
            dma((5,)), dma((chunks,)), dma((2,)), dma((kv,)), dma((kv,)),
        ],
        compiler_params=pltpu.CompilerParams(collective_id=1, has_side_effects=True, vmem_limit_bytes=PROJECT_MIB * 2**20),
        cost_estimate=pl.CostEstimate(flops=2 * num_seqs * d_model * kv * qkv, bytes_accessed=24 * 2**20, transcendentals=0),
        name="project",
    )(*(pltpu.with_memory_space_constraint(a, pltpu.HBM) for a in operands))


def update_kernel(logit_scale, lens, sink_ref, heads_ref, k_in, v_in, kbuf, vbuf, k_out, v_out, early_ref, ko_sem, vo_sem):
    kv = heads_ref.shape[0]
    num_seqs, ctx2 = kbuf.shape[:2]
    blocks = ko_sem.shape[0]
    seqs = num_seqs // blocks
    stride = num_seqs + 8
    tiles = heads_ref.shape[1] // stride
    base = lax.axis_index("sp") * (ctx2 // kv)
    group = 16
    group_row = lax.broadcasted_iota(jnp.int32, (group, LANES), 0)

    def cache_write(hbm, buf, sem, block):
        rows = pl.ds(block * seqs, seqs)
        return pltpu.make_async_copy(buf.at[rows], hbm.at[rows], sem.at[block])

    @pl.loop(0, blocks)
    def _(block):
        found = []
        for i in range(seqs):
            b = block * seqs + i
            local = lens[b] - base
            here = jnp.logical_and(local >= 0, local < ctx2 // kv)
            place = jnp.where(here, local * kv, 0)
            start = pl.multiple_of(place // group * group, group)
            target = jnp.where(here, place - start, group)
            for n, buf in enumerate((kbuf, vbuf)):
                fresh = [heads_ref[k, pl.ds((tiles - 2 + n) * stride + b, 1), :] for k in range(kv)]
                found.append((buf, b, start, target, fresh, buf[b, pl.ds(start, group), :]))
        values = []
        for _, _, _, target, fresh, old in found:
            value = old.astype(jnp.float32)
            for k in range(kv):
                value = jnp.where(group_row == target + k, fresh[k], value)
            values.append(value.astype(jnp.bfloat16))
        for (buf, b, start, _, _, _), value in zip(found, values):
            buf[b, pl.ds(start, group), :] = value
        cache_write(k_out, kbuf, ko_sem, block).start()
        cache_write(v_out, vbuf, vo_sem, block).start()

    position, sink_col = attention_setup(kv, tiles - 2, ctx2, sink_ref)
    opposite = (lax.axis_index("sp") // CORES + RING // 2) % RING

    @pl.loop(0, SUBS)
    def _(s):
        attend_block((opposite * SUBS + s) * seqs, seqs, logit_scale, heads_ref, kbuf, vbuf, lens, position, sink_col, early_ref.at[s])

    @pl.loop(0, blocks)
    def _(block):
        cache_write(k_out, kbuf, ko_sem, block).wait()
        cache_write(v_out, vbuf, vo_sem, block).wait()


def update(seq_lens, sinks, heads_out, k_near, v_near):
    blocks = RING * SUBS
    hbm = pl.BlockSpec(memory_space=pl.ANY)
    vmem = pl.BlockSpec(memory_space=pltpu.VMEM)
    smem = pl.BlockSpec(memory_space=pltpu.SMEM)
    kv = heads_out.shape[0]
    heads = sinks.shape[0] // kv
    seqs = k_near.shape[0] // blocks
    near = pltpu.VMEM(k_near.shape, k_near.dtype)
    far = jax.ShapeDtypeStruct(k_near.shape, k_near.dtype)
    dma = pltpu.SemaphoreType.DMA
    return pl.pallas_call(
        functools.partial(update_kernel, LANES ** -0.5),
        out_shape=(near, near, far, far, pltpu.VMEM((SUBS, kv, seqs + 1, heads, LANES), jnp.float32)),
        in_specs=[smem, smem, vmem, vmem, vmem],
        out_specs=(vmem, vmem, hbm, hbm, vmem),
        scratch_shapes=[dma((blocks,)), dma((blocks,))],
        input_output_aliases={3: 0, 4: 1},
        compiler_params=pltpu.CompilerParams(vmem_limit_bytes=UPDATE_MIB * 2**20),
        cost_estimate=pl.CostEstimate(flops=10**6, bytes_accessed=10 * 2**20, transcendentals=0),
        name="update",
    )(seq_lens, sinks, heads_out, k_near, v_near)


def solution(mesh):
    cache_spec = P("dp", "sp", "tp", None)

    def block_step(hidden, seq_lens, rope_cos, rope_sin, k_cache, v_cache, norm_gain, w_qkv, b_qkv, sink_logits, w_o, b_o):
        num_seqs, ctx, kv, head_dim = k_cache.shape
        assert head_dim == LANES and mesh.shape["tp"] == RING and mesh.shape["sp"] == RING * CORES
        flat = (num_seqs, ctx * kv, head_dim)
        heads_out, k_near, v_near = project(
            hidden, rope_cos.T, rope_sin.T, k_cache.reshape(flat), v_cache.reshape(flat), norm_gain.reshape(-1, LANES), w_qkv, b_qkv)
        k_near, v_near, k_out, v_out, early = update(seq_lens, sink_logits, heads_out, k_near, v_near)
        out_hidden = combine(early, heads_out, k_near, v_near, seq_lens, sink_logits, hidden, b_o.reshape(-1, LANES), w_o)
        return out_hidden, k_out.reshape(k_cache.shape), v_out.reshape(v_cache.shape)

    return jax.shard_map(block_step, mesh=mesh, in_specs=(P("dp", None), P("dp"), P("dp", None), P("dp", None), cache_spec, cache_spec, P(None), P(None, "tp", None), P("tp", None), P("tp"), P("tp", None), P(None)), out_specs=(P("dp", None), cache_spec, cache_spec), check_vma=False)
```

```python
import functools

import jax
import jax.numpy as jnp
from jax import lax
from jax.experimental import pallas as pl
from jax.experimental.pallas import tpu as pltpu
from jax.sharding import PartitionSpec as P

NORM_EPS = 1e-5
MESH = pl.DeviceIdType.MESH
LANES = 128
HALF = LANES // 2
SUBS = 2
CORES = 2
PROJECT_MIB = 30
UPDATE_MIB = 4
COMBINE_MIB = 26
WAVE = 8
RING = 4


def lane_column(tile, index):
    return tile[:, index : index + 1]


def merge_parts(parts, seqs):
    stats = [part[seqs] for part in parts]
    top = functools.reduce(jnp.maximum, stats)
    scales = [jnp.exp(stat - top) for stat in stats]
    total = sum(pltpu.roll(scale, HALF, 1) * stat for scale, stat in zip(scales, stats))
    return top, total, scales


def weighted_sums(columns, parts, seqs):
    loaded = [[part[i] for part in parts] for i in range(seqs)]
    scaled = [[column * value for column, value in zip(cols, values)] for cols, values in zip(columns, loaded)]
    return [functools.reduce(jnp.add, terms) for terms in scaled]


def merge_into(dst, parts, seqs):
    top, total, scales = merge_parts(parts, seqs)
    columns = [[lane_column(scale, i) for scale in scales] for i in range(seqs)]
    sums = weighted_sums(columns, parts, seqs)
    lane = lax.broadcasted_iota(jnp.int32, top.shape, 1)
    stats = jnp.where(lane < HALF, top, total)
    for i in range(seqs):
        dst[i] = sums[i]
    dst[seqs] = stats


def attention_setup(kv, heads, ctx2, sink_ref):
    row = lax.broadcasted_iota(jnp.int32, (kv * heads, ctx2), 0)
    lane = lax.broadcasted_iota(jnp.int32, (kv * heads, ctx2), 1)
    base = lax.axis_index("sp") * (ctx2 // kv)
    position = jnp.where(lane % kv == row // heads, lane // kv + base, jnp.iinfo(jnp.int32).max)
    sinks = jnp.zeros((kv * heads, ctx2), jnp.float32)
    for i in range(kv * heads):
        sinks = jnp.where(row == i, sink_ref[i], sinks)
    return position, jnp.max(sinks, axis=-1, keepdims=True)


def attend_block(first, seqs, logit_scale, q_ref, k_ref, v_ref, lens, position, sink_col, dst):
    kv, _, heads, _ = dst.shape
    q_rows = kv * heads
    q_stride = q_ref.shape[1] // (heads + 2)
    lane = lax.broadcasted_iota(jnp.int32, (q_rows, LANES), 1)
    waves = [range(j, j + WAVE) for j in range(0, seqs, WAVE)]
    logits, tops, totals, weights, stats = {}, {}, {}, {}, jnp.zeros((q_rows, LANES), jnp.float32)
    for turn in range(len(waves) + 2):
        if turn < len(waves):
            for i in waves[turn]:
                q = jnp.concatenate([q_ref[k, pl.ds(first + i, heads, stride=q_stride), :] for k in range(kv)], axis=0).astype(jnp.bfloat16)
                logits[i] = lax.dot_general(q, k_ref[first + i], (((1,), (1,)), ((), ())), preferred_element_type=jnp.float32)
        if 0 <= turn - 1 < len(waves):
            members = waves[turn - 1]
            for i in members:
                logits[i] = jnp.where(position <= lens[first + i], logits[i] * logit_scale, -jnp.inf)
            for i in members:
                tops[i] = jnp.maximum(jnp.max(logits[i], axis=-1, keepdims=True), sink_col)
            for i in members:
                weights[i] = jnp.exp(logits[i] - tops[i])
            for i in members:
                totals[i] = jnp.sum(weights[i], axis=-1, keepdims=True)
        if 0 <= turn - 2:
            members = waves[turn - 2]
            numers = [
                jnp.dot(weights[i].astype(jnp.bfloat16), v_ref[first + i], preferred_element_type=jnp.float32) for i in members]
            for i, numer in zip(members, numers):
                for k in range(kv):
                    dst[k, i] = numer[k * heads : (k + 1) * heads]
                stats = jnp.where(lane == i, tops[i], jnp.where(lane == HALF + i, totals[i], stats))
    for k in range(kv):
        dst[k, seqs] = stats[k * heads : (k + 1) * heads]


def combine_kernel(
    seqs, logit_scale, early_ref, q_ref, k_ref, v_ref, lens, sink_ref, x_hbm, bo_hbm, wo_hbm, out_ref,
    p_ref, bo_ref, bias_rows, ra, cb, rl, rm, rd, own_o, other_o, wbuf, xbuf, z, yrl, ym, yrm, yrd, g, gp,
    w_sem, x_sem, a_send, a_recv, b_send, rl_recv, rm_recv, rd_recv, o_send, o_recv,
    d_send, yrl_recv, yrm_recv, yrd_recv, g_send, g_recv, gp_send, gp_recv,
):
    y = lax.axis_index("tp")
    sp = lax.axis_index("sp")
    x = sp // CORES
    c = sp % CORES
    step = 1 - 2 * c
    xn, xp, xo = (x + step + RING) % RING, (x - step + RING) % RING, (x + 2) % RING
    yn, yp, yo = (y + step + RING) % RING, (y - step + RING) % RING, (y + 2) % RING
    partner = {"sp": x * CORES + 1 - c}
    to_xn, to_xp = {"sp": xn * CORES + c}, {"sp": xp * CORES + c}
    to_yn, to_yp = {"tp": yn}, {"tp": yp}

    rows_half = wo_hbm.shape[0] // 2
    cols_core = wo_hbm.shape[1] // CORES
    cols_sub = cols_core // SUBS
    heads = p_ref.shape[4]
    block_rows = z.shape[2]

    w_copies = []
    for k in range(2):
        rows = (c if k == 0 else 1 - c) * rows_half
        copy = pltpu.make_async_copy(
            wo_hbm.at[pl.ds(pl.multiple_of(rows, LANES), rows_half), pl.ds(pl.multiple_of(c * cols_core, LANES), cols_core)],
            wbuf.at[k], w_sem.at[k])
        copy.start()
        w_copies.append(copy)
    row0 = pl.multiple_of((x * RING + y) * block_rows, block_rows)
    x_copy = pltpu.make_async_copy(
        x_hbm.at[pl.ds(row0, block_rows), pl.ds(pl.multiple_of(c * cols_core, LANES), cols_core)], xbuf, x_sem.at[0])
    x_copy.start()
    bo_copy = pltpu.make_async_copy(bo_hbm, bo_ref, x_sem.at[1])
    bo_copy.start()

    barrier = pltpu.get_barrier_semaphore()
    for where in (partner, to_xn, to_xp, to_yn, to_yp):
        pl.semaphore_signal(barrier, inc=1, device_id=where, device_id_type=MESH)
    pl.semaphore_wait(barrier, 5)

    def send(src, dst, send_sem, recv_sem, where):
        copy = pltpu.make_async_remote_copy(
            src_ref=src, dst_ref=dst, send_sem=send_sem, recv_sem=recv_sem, device_id=where, device_id_type=MESH)
        copy.start()

    def sent(shape_of, send_sem):
        pltpu.make_async_remote_copy(
            src_ref=shape_of, dst_ref=shape_of, send_sem=send_sem, recv_sem=send_sem, device_id=partner, device_id_type=MESH).wait_send()

    def arrived(dst, recv_sem):
        pltpu.make_async_remote_copy(
            src_ref=dst, dst_ref=dst, send_sem=recv_sem, recv_sem=recv_sem, device_id=partner, device_id_type=MESH).wait_recv()

    kv = p_ref.shape[2]
    ctx2 = k_ref.shape[1]
    position, sink_col = attention_setup(kv, heads, ctx2, sink_ref)

    def attend(b, s):
        attend_block((b * SUBS + s) * seqs, seqs, logit_scale, q_ref, k_ref, v_ref, lens, position, sink_col, p_ref.at[b, s])
        join(b, s)

    def join(b, s):
        send(p_ref.at[b, s, 1 - c], ra.at[b, s], a_send.at[0], a_recv.at[b, s], partner)

    def attend_both(b):
        @pl.loop(0, SUBS)
        def _(s):
            attend(b, s)

    def relay(s):
        arrived(ra.at[xo, s], a_recv.at[xo, s])
        merge_into(cb.at[0, s], (early_ref.at[s, c], ra.at[xo, s]), seqs)
        send(cb.at[0, s], rl.at[s], b_send.at[0], rl_recv.at[s], to_xn)

    def pass_on(s):
        arrived(ra.at[xn, s], a_recv.at[xn, s])
        arrived(rl.at[s], rl_recv.at[s])
        merge_into(cb.at[2, s], (p_ref.at[xn, s, c], ra.at[xn, s], rl.at[s]), seqs)
        send(cb.at[2, s], rm.at[s], b_send.at[0], rm_recv.at[s], to_xn)

    for s in range(SUBS):
        send(early_ref.at[s, 1 - c], ra.at[xo, s], a_send.at[0], a_recv.at[xo, s], partner)
    attend(xn, 0)
    for s in range(SUBS):
        relay(s)
    for s in range(1, SUBS):
        attend(xn, s)
    attend_both(xp)
    for s in range(SUBS):
        arrived(ra.at[xp, s], a_recv.at[xp, s])
        merge_into(cb.at[1, s], (p_ref.at[xp, s, c], ra.at[xp, s]), seqs)
        send(cb.at[1, s], rd.at[s], b_send.at[0], rd_recv.at[s], to_xp)
    for s in range(SUBS):
        pass_on(s)
    attend_both(x)
    for s in range(SUBS):
        arrived(ra.at[x, s], a_recv.at[x, s])
        merge_into(cb.at[3, s], (p_ref.at[x, s, c], ra.at[x, s]), seqs)
    sink = jnp.zeros((heads, LANES), jnp.float32)
    head_row = lax.broadcasted_iota(jnp.int32, sink.shape, 0)
    for h in range(heads):
        sink = jnp.where(head_row == h, sink_ref[c * heads + h], sink)
    for s in range(SUBS):
        arrived(rd.at[s], rd_recv.at[s])
        arrived(rm.at[s], rm_recv.at[s])
        parts = (cb.at[3, s], rd.at[s], rm.at[s])
        top, total, scales = merge_parts(parts, seqs)
        inverse = 1.0 / (pltpu.roll(total, HALF, 1) + jnp.exp(sink - top))
        columns = [[lane_column(scale * inverse, i) for scale in scales] for i in range(seqs)]
        outs = [out.astype(jnp.bfloat16).astype(jnp.float32) for out in weighted_sums(columns, parts, seqs)]
        for i in range(seqs):
            own_o[s, pl.ds(i * heads, heads), :] = outs[i]
        send(own_o.at[s], other_o.at[s], o_send.at[0], o_recv.at[s], partner)

    def head_rows(ref):
        columns = []
        for h in range(heads):
            columns.append(jnp.concatenate(
                [ref[s, pl.ds(h, seqs, stride=heads), :] for s in range(SUBS)], axis=0).astype(jnp.bfloat16))
        return jnp.concatenate(columns, axis=1)

    own_rows = head_rows(own_o)
    w_copies[0].wait()
    for q in range(SUBS):
        part = jnp.dot(own_rows, wbuf[0, :, pl.ds(q * cols_sub, cols_sub)], preferred_element_type=jnp.float32)
        for r in range(RING):
            z[q, r] = part[r * block_rows : (r + 1) * block_rows]
    for s in range(SUBS):
        arrived(other_o.at[s], o_recv.at[s])
    other_rows = head_rows(other_o)
    w_copies[1].wait()
    for q in range(SUBS):
        part = jnp.dot(other_rows, wbuf[1, :, pl.ds(q * cols_sub, cols_sub)], preferred_element_type=jnp.float32)
        for r in range(RING):
            z[q, r] += part[r * block_rows : (r + 1) * block_rows]
        send(z.at[q, yo], yrl.at[q], d_send.at[0], yrl_recv.at[q], to_yn)
        send(z.at[q, yp], yrd.at[q], d_send.at[0], yrd_recv.at[q], to_yp)
    for q in range(SUBS):
        arrived(yrl.at[q], yrl_recv.at[q])
        ym[q] = z[q, yn] + yrl[q]
        send(ym.at[q], yrm.at[q], d_send.at[0], yrm_recv.at[q], to_yn)
    chunk = g.shape[3:]
    sent(ra, a_send.at[0])
    sent(cb.at[pl.ds(0, 3)], b_send.at[0])
    sent(own_o, o_send.at[0])
    sent(g.reshape((-1,) + chunk).at[pl.ds(0, 3 * SUBS)], d_send.at[0])
    x_copy.wait()
    bo_copy.wait()
    bias_rows[...] = bo_ref[...].astype(jnp.float32)

    def store(q, xx, yy, core, value):
        rows = pl.ds(pl.multiple_of((xx * RING + yy) * block_rows, block_rows), block_rows)
        cols = pl.ds(pl.multiple_of(core * cols_core + q * cols_sub, LANES), cols_sub)
        out_ref[rows, cols] = value.astype(jnp.bfloat16)

    def slot(q, first, second):
        return (first, second) if q == 0 else (second, first)

    ahead = ((to_xn, to_xp), (to_yn, to_yp))
    first_now, first_n, first_p, first_o = (x, y), (xn, yn), (xp, yp), (xo, yo)

    pushes = []

    def push(q, first, second, where):
        xx, yy = slot(q, first, second)
        pushes.append(q)
        send(g.at[q, xx, yy], g.at[q, xx, yy], g_send.at[0], g_recv.at[q, xx, yy], where)

    def share(q, first, second, group):
        xx, yy = slot(q, first, second)
        send(g.at[q, xx, yy], gp.at[q, xx, yy], gp_send.at[0], gp_recv.at[group], partner)

    def receive(q, first, second):
        xx, yy = slot(q, first, second)
        arrived(g.at[q, xx, yy], g_recv.at[q, xx, yy])

    def keep(q, first, second):
        xx, yy = slot(q, first, second)
        store(q, xx, yy, c, g[q, xx, yy])

    for q in range(SUBS):
        arrived(yrd.at[q], yrd_recv.at[q])
        arrived(yrm.at[q], yrm_recv.at[q])
        first_row = (c * cols_core + q * cols_sub) // LANES
        bias = jnp.concatenate([bias_rows[pl.ds(first_row + t, 1), :] for t in range(cols_sub // LANES)], axis=1)
        summed = z[q, y] + yrd[q] + yrm[q]
        final = xbuf[:, pl.ds(q * cols_sub, cols_sub)].astype(jnp.float32) + summed + bias
        g[q, x, y] = final.astype(jnp.bfloat16).astype(jnp.float32)
        for axis in (q, 1 - q):
            for kind in range(2):
                push(q, first_now[q], first_now[1 - q], ahead[axis][kind])
        share(q, first_now[q], first_now[1 - q], 0)

    def spread(q, first, forward):
        other = 1 - q
        receive(q, first, first_now[other])
        if forward:
            push(q, first, first_now[other], ahead[q][0])
        for kind in range(2):
            push(q, first, first_now[other], ahead[other][kind])
        share(q, first, first_now[other], 0)

    def settle(q, first, second, where, group):
        receive(q, first, second)
        for target in where:
            push(q, first, second, target)
        share(q, first, second, group)

    both = range(SUBS)
    along = [ahead[1 - q][0] for q in both]
    diagonal = dict(to_xn, **to_yn)
    steps = [
        (lambda q: spread(q, first_p[q], True), first_p, first_now),
        (lambda q: spread(q, first_n[q], False), first_n, first_now),
        (lambda q: settle(q, first_now[q], first_p[1 - q], (along[q],), 0), first_now, first_p),
        (lambda q: settle(q, first_now[q], first_n[1 - q], (), 0), first_now, first_n),
        (lambda q: settle(q, first_p[q], first_p[1 - q], (diagonal, along[q]), 0), first_p, first_p),
        (lambda q: spread(q, first_o[q], False), first_o, first_now),
        (lambda q: settle(q, first_n[q], first_p[1 - q], (along[q],), 0), first_n, first_p),
        (lambda q: settle(q, first_p[q], first_n[1 - q], (), 0), first_p, first_n),
        (lambda q: settle(q, first_n[q], first_n[1 - q], (), 0), first_n, first_n),
        (lambda q: settle(q, first_now[q], first_o[1 - q], (), 0), first_now, first_o),
        (lambda q: settle(q, first_o[q], first_p[1 - q], (), 1), first_o, first_p),
        (lambda q: settle(q, first_o[q], first_n[1 - q], (), 1), first_o, first_n),
        (lambda q: settle(q, first_p[q], first_o[1 - q], (), 1), first_p, first_o),
        (lambda q: settle(q, first_n[q], first_o[1 - q], (), 1), first_n, first_o),
        (lambda q: settle(q, first_o[q], first_o[1 - q], (), 2), first_o, first_o),
    ]
    for q in both:
        keep(q, first_now[q], first_now[1 - q])
    for step_fn, first, second in steps:
        for q in both:
            step_fn(q)
        for q in both:
            keep(q, first[q], second[1 - q])
    blocks = [(first_now, first_now, 0)] + [(first, second, 0) for _, first, second in steps[:10]]
    blocks += [(first, second, 1) for _, first, second in steps[10:14]] + [(first_o, first_o, 2)]
    for group in range(3):
        members = [(first, second) for first, second, which in blocks if which == group]
        arrived(gp.reshape((-1,) + chunk).at[pl.ds(0, SUBS * len(members))], gp_recv.at[group])
        for first, second in members:
            for q in both:
                xx, yy = slot(q, first[q], second[1 - q])
                store(q, xx, yy, 1 - c, gp[q, xx, yy])
    sent(g.reshape((-1,) + chunk).at[pl.ds(0, len(pushes))], g_send.at[0])
    sent(gp, gp_send.at[0])


def combine(early, queries, k_out, v_out, seq_lens, sinks, hidden, b_o, w_o):
    num_seqs, d_model = hidden.shape
    seqs = num_seqs // (RING * SUBS)
    kv = CORES
    heads = sinks.shape[0] // kv
    cols_core = d_model // CORES
    cols_sub = cols_core // SUBS
    block_rows = num_seqs // (RING * RING)
    part = (seqs + 1, heads, LANES)
    f32, bf16 = jnp.float32, jnp.bfloat16
    dma = pltpu.SemaphoreType.DMA
    vmem = pl.BlockSpec(memory_space=pltpu.VMEM)
    hbm = pl.BlockSpec(memory_space=pl.ANY)
    smem = pl.BlockSpec(memory_space=pltpu.SMEM)
    chunk = (block_rows, cols_sub)
    return pl.pallas_call(
        functools.partial(combine_kernel, seqs, LANES ** -0.5),
        out_shape=jax.ShapeDtypeStruct((num_seqs, d_model), bf16),
        in_specs=[vmem, vmem, vmem, vmem, smem, smem, hbm, hbm, hbm],
        out_specs=vmem,
        scratch_shapes=[
            pltpu.VMEM((RING, SUBS, kv) + part, f32),
            pltpu.VMEM(b_o.shape, bf16),
            pltpu.VMEM(b_o.shape, f32),
            pltpu.VMEM((RING, SUBS) + part, f32),
            pltpu.VMEM((RING, SUBS) + part, f32),
            pltpu.VMEM((SUBS,) + part, f32),
            pltpu.VMEM((SUBS,) + part, f32),
            pltpu.VMEM((SUBS,) + part, f32),
            pltpu.VMEM((SUBS, seqs * heads, LANES), f32),
            pltpu.VMEM((SUBS, seqs * heads, LANES), f32),
            pltpu.VMEM((2, w_o.shape[0] // 2, cols_core), bf16),
            pltpu.VMEM((block_rows, cols_core), bf16),
            pltpu.VMEM((SUBS, RING) + chunk, f32),
            pltpu.VMEM((SUBS,) + chunk, f32),
            pltpu.VMEM((SUBS,) + chunk, f32),
            pltpu.VMEM((SUBS,) + chunk, f32),
            pltpu.VMEM((SUBS,) + chunk, f32),
            pltpu.VMEM((SUBS, RING, RING) + chunk, f32),
            pltpu.VMEM((SUBS, RING, RING) + chunk, f32),
            dma((2,)), dma((2,)), dma((1,)), dma((RING, SUBS)), dma((1,)),
            dma((SUBS,)), dma((SUBS,)), dma((SUBS,)), dma((1,)), dma((SUBS,)),
            dma((1,)), dma((SUBS,)), dma((SUBS,)), dma((SUBS,)),
            dma((1,)), dma((SUBS, RING, RING)), dma((1,)), dma((3,)),
        ],
        compiler_params=pltpu.CompilerParams(collective_id=0, has_side_effects=True, vmem_limit_bytes=COMBINE_MIB * 2**20),
        cost_estimate=pl.CostEstimate(flops=2 * num_seqs // RING * w_o.shape[0] * cols_core, bytes_accessed=30 * 2**20, transcendentals=0),
        name="combine",
    )(early, queries, k_out, v_out, seq_lens, sinks, *(pltpu.with_memory_space_constraint(a, pltpu.HBM) for a in (hidden, b_o, w_o)))


def project_kernel(
    x_hbm, cos_hbm, sin_hbm, k_hbm, v_hbm, gain_hbm, w_hbm, bias_hbm,
    heads_ref, kbuf, vbuf,
    xbuf, cos, sin, gain, bias, hexp, wbuf, acc,
    in_sem, w_sem, cache_sem, send_sem, recv_sem,
):
    num_seqs, d_model = x_hbm.shape
    kv = w_hbm.shape[1]
    qkv = w_hbm.shape[2]
    tiles = qkv // LANES // CORES
    chunks, depth2, cols = wbuf.shape
    stride = heads_ref.shape[1] // (CORES * tiles)
    c = lax.axis_index("sp") % CORES
    partner = {"sp": lax.axis_index("sp") + 1 - 2 * c}
    w_rows = w_hbm.reshape(d_model * kv, qkv)
    first_col = pl.multiple_of(c * cols, LANES)

    def w_copy(chunk):
        return pltpu.make_async_copy(
            w_rows.at[pl.ds(chunk * depth2, depth2), pl.ds(first_col, cols)], wbuf.at[chunk], w_sem.at[chunk])

    small = [
        pltpu.make_async_copy(src, dst, in_sem.at[i])
        for i, (src, dst) in enumerate((
            (x_hbm, xbuf), (gain_hbm, gain), (cos_hbm, cos), (sin_hbm, sin), (bias_hbm, bias)))
    ]
    for copy in small:
        copy.start()
    for chunk in range(chunks):
        w_copy(chunk).start()
    barrier = pltpu.get_barrier_semaphore()
    pl.semaphore_signal(barrier, inc=1, device_id=partner, device_id_type=MESH)

    small[0].wait()
    small[1].wait()
    row = lax.broadcasted_iota(jnp.int32, (LANES, kv * LANES), 0)
    col = lax.broadcasted_iota(jnp.int32, (LANES, kv * LANES), 1)
    pick = (col == row * kv).astype(jnp.bfloat16)
    gains = gain[...].astype(jnp.float32)
    square = jnp.zeros((num_seqs, LANES), jnp.float32)
    for t in range(d_model // LANES):
        xt = xbuf[:, t * LANES : (t + 1) * LANES].astype(jnp.float32)
        square += xt * xt
    inv_rms = lax.rsqrt(jnp.sum(square, axis=-1, keepdims=True) / d_model + NORM_EPS)
    def spread_chunk(chunk):
        for t in range(chunk * pieces // kv, (chunk + 1) * pieces // kv):
            xt = xbuf[:, t * LANES : (t + 1) * LANES].astype(jnp.float32)
            ht = (xt * inv_rms * gains[t : t + 1]).astype(jnp.bfloat16)
            spread = jnp.dot(ht, pick, preferred_element_type=jnp.float32).astype(jnp.bfloat16)
            for k in range(kv):
                for j in range(kv):
                    piece = spread[:, j * LANES : (j + 1) * LANES]
                    hexp[t * kv + j, k * num_seqs : (k + 1) * num_seqs] = pltpu.roll(piece, k, 1) if k else piece

    pieces = depth2 // LANES
    for chunk in range(chunks):
        spread_chunk(chunk)
    cache_copies = [pltpu.make_async_copy(src, dst, cache_sem.at[i]) for i, (src, dst) in enumerate(((k_hbm, kbuf), (v_hbm, vbuf)))]

    for copy in cache_copies:
        copy.start()
    for chunk in range(chunks):
        w_copy(chunk).wait()
        lhs = jnp.concatenate([hexp[chunk * pieces + i] for i in range(pieces)], axis=1)
        for t in range(0, tiles, 2):
            part = slice(t * LANES, min(t + 2, tiles) * LANES)
            product = jnp.dot(lhs, wbuf[chunk, :, part], preferred_element_type=jnp.float32)
            acc[:, part] = acc[:, part] + product if chunk else product

    for copy in small[2:]:
        copy.wait()
    cos_t = jnp.transpose(jnp.concatenate([cos[...], cos[...]], axis=0))
    sin_t = jnp.transpose(jnp.concatenate([-sin[...], sin[...]], axis=0))
    pl.semaphore_wait(barrier, 1)

    def mine(k):
        rows = tiles * stride
        return heads_ref.at[k, pl.ds(pl.multiple_of(c * rows, 8), rows)]

    for k in range(kv):
        for j in range(tiles):
            tile = c * tiles + j
            value = acc[k * num_seqs : (k + 1) * num_seqs, j * LANES : (j + 1) * LANES]
            value += bias[k : k + 1, pl.ds(pl.multiple_of(tile * LANES, LANES), LANES)].astype(jnp.float32)
            turned = value * cos_t + pltpu.roll(value, HALF, 1) * sin_t
            value = jnp.where(jnp.full(value.shape, tile, jnp.int32) == CORES * tiles - 1, value, turned)
            heads_ref[k, pl.ds(pl.multiple_of(tile * stride, 8), num_seqs), :] = value.astype(jnp.bfloat16).astype(jnp.float32)
        pltpu.make_async_remote_copy(
            src_ref=mine(k), dst_ref=mine(k), send_sem=send_sem.at[k], recv_sem=recv_sem.at[k],
            device_id=partner, device_id_type=MESH).start()
    for copy in cache_copies:
        copy.wait()
    for k in range(kv):
        copy = pltpu.make_async_remote_copy(
            src_ref=mine(k), dst_ref=mine(k), send_sem=send_sem.at[k], recv_sem=recv_sem.at[k],
            device_id=partner, device_id_type=MESH)
        copy.wait_send()
        copy.wait_recv()


def project(hidden, cos_t, sin_t, k_cache, v_cache, gain, w_qkv, b_qkv):
    num_seqs, d_model = hidden.shape
    kv, qkv = w_qkv.shape[1:]
    tiles = qkv // LANES
    chunks = 4
    depth2 = d_model * kv // chunks
    f32, bf16 = jnp.float32, jnp.bfloat16
    dma = pltpu.SemaphoreType.DMA
    hbm = pl.BlockSpec(memory_space=pl.ANY)
    vmem = pl.BlockSpec(memory_space=pltpu.VMEM)
    operands = (hidden, cos_t, sin_t, k_cache, v_cache, gain, w_qkv, b_qkv)
    return pl.pallas_call(
        project_kernel,
        out_shape=(pltpu.VMEM((kv, tiles * (num_seqs + 8), LANES), f32), pltpu.VMEM(k_cache.shape, bf16), pltpu.VMEM(v_cache.shape, bf16)),
        in_specs=[hbm] * len(operands),
        out_specs=(vmem, vmem, vmem),
        scratch_shapes=[
            pltpu.VMEM(hidden.shape, bf16),
            pltpu.VMEM(cos_t.shape, f32),
            pltpu.VMEM(sin_t.shape, f32),
            pltpu.VMEM(gain.shape, bf16),
            pltpu.VMEM(b_qkv.shape, bf16),
            pltpu.VMEM((d_model * kv // LANES, kv * num_seqs, LANES), bf16),
            pltpu.VMEM((chunks, depth2, qkv // CORES), bf16),
            pltpu.VMEM((kv * num_seqs, qkv // CORES), f32),
            dma((5,)), dma((chunks,)), dma((2,)), dma((kv,)), dma((kv,)),
        ],
        compiler_params=pltpu.CompilerParams(collective_id=1, has_side_effects=True, vmem_limit_bytes=PROJECT_MIB * 2**20),
        cost_estimate=pl.CostEstimate(flops=2 * num_seqs * d_model * kv * qkv, bytes_accessed=24 * 2**20, transcendentals=0),
        name="project",
    )(*(pltpu.with_memory_space_constraint(a, pltpu.HBM) for a in operands))


def update_kernel(logit_scale, lens, sink_ref, heads_ref, k_in, v_in, kbuf, vbuf, k_out, v_out, early_ref, ko_sem, vo_sem):
    kv = heads_ref.shape[0]
    num_seqs, ctx2 = kbuf.shape[:2]
    blocks = ko_sem.shape[0]
    seqs = num_seqs // blocks
    stride = num_seqs + 8
    tiles = heads_ref.shape[1] // stride
    base = lax.axis_index("sp") * (ctx2 // kv)
    group = 16
    group_row = lax.broadcasted_iota(jnp.int32, (group, LANES), 0)

    def cache_write(hbm, buf, sem, block):
        rows = pl.ds(block * seqs, seqs)
        return pltpu.make_async_copy(buf.at[rows], hbm.at[rows], sem.at[block])

    @pl.loop(0, blocks)
    def _(block):
        found = []
        for i in range(seqs):
            b = block * seqs + i
            local = lens[b] - base
            here = jnp.logical_and(local >= 0, local < ctx2 // kv)
            place = jnp.where(here, local * kv, 0)
            start = pl.multiple_of(place // group * group, group)
            target = jnp.where(here, place - start, group)
            for n, buf in enumerate((kbuf, vbuf)):
                fresh = [heads_ref[k, pl.ds((tiles - 2 + n) * stride + b, 1), :] for k in range(kv)]
                found.append((buf, b, start, target, fresh, buf[b, pl.ds(start, group), :]))
        values = []
        for _, _, _, target, fresh, old in found:
            value = old.astype(jnp.float32)
            for k in range(kv):
                value = jnp.where(group_row == target + k, fresh[k], value)
            values.append(value.astype(jnp.bfloat16))
        for (buf, b, start, _, _, _), value in zip(found, values):
            buf[b, pl.ds(start, group), :] = value
        cache_write(k_out, kbuf, ko_sem, block).start()
        cache_write(v_out, vbuf, vo_sem, block).start()

    position, sink_col = attention_setup(kv, tiles - 2, ctx2, sink_ref)
    opposite = (lax.axis_index("sp") // CORES + RING // 2) % RING

    @pl.loop(0, SUBS)
    def _(s):
        attend_block((opposite * SUBS + s) * seqs, seqs, logit_scale, heads_ref, kbuf, vbuf, lens, position, sink_col, early_ref.at[s])

    @pl.loop(0, blocks)
    def _(block):
        cache_write(k_out, kbuf, ko_sem, block).wait()
        cache_write(v_out, vbuf, vo_sem, block).wait()


def update(seq_lens, sinks, heads_out, k_near, v_near):
    blocks = RING * SUBS
    hbm = pl.BlockSpec(memory_space=pl.ANY)
    vmem = pl.BlockSpec(memory_space=pltpu.VMEM)
    smem = pl.BlockSpec(memory_space=pltpu.SMEM)
    kv = heads_out.shape[0]
    heads = sinks.shape[0] // kv
    seqs = k_near.shape[0] // blocks
    near = pltpu.VMEM(k_near.shape, k_near.dtype)
    far = jax.ShapeDtypeStruct(k_near.shape, k_near.dtype)
    dma = pltpu.SemaphoreType.DMA
    return pl.pallas_call(
        functools.partial(update_kernel, LANES ** -0.5),
        out_shape=(near, near, far, far, pltpu.VMEM((SUBS, kv, seqs + 1, heads, LANES), jnp.float32)),
        in_specs=[smem, smem, vmem, vmem, vmem],
        out_specs=(vmem, vmem, hbm, hbm, vmem),
        scratch_shapes=[dma((blocks,)), dma((blocks,))],
        input_output_aliases={3: 0, 4: 1},
        compiler_params=pltpu.CompilerParams(vmem_limit_bytes=UPDATE_MIB * 2**20),
        cost_estimate=pl.CostEstimate(flops=10**6, bytes_accessed=10 * 2**20, transcendentals=0),
        name="update",
    )(seq_lens, sinks, heads_out, k_near, v_near)


def solution(mesh):
    cache_spec = P("dp", "sp", "tp", None)

    def block_step(hidden, seq_lens, rope_cos, rope_sin, k_cache, v_cache, norm_gain, w_qkv, b_qkv, sink_logits, w_o, b_o):
        num_seqs, ctx, kv, head_dim = k_cache.shape
        assert head_dim == LANES and mesh.shape["tp"] == RING and mesh.shape["sp"] == RING * CORES
        flat = (num_seqs, ctx * kv, head_dim)
        heads_out, k_near, v_near = project(
            hidden, rope_cos.T, rope_sin.T, k_cache.reshape(flat), v_cache.reshape(flat), norm_gain.reshape(-1, LANES), w_qkv, b_qkv)
        k_near, v_near, k_out, v_out, early = update(seq_lens, sink_logits, heads_out, k_near, v_near)
        out_hidden = combine(early, heads_out, k_near, v_near, seq_lens, sink_logits, hidden, b_o.reshape(-1, LANES), w_o)
        return out_hidden, k_out.reshape(k_cache.shape), v_out.reshape(v_cache.shape)

    return jax.shard_map(block_step, mesh=mesh, in_specs=(P("dp", None), P("dp"), P("dp", None), P("dp", None), cache_spec, cache_spec, P(None), P(None, "tp", None), P("tp", None), P("tp"), P("tp", None), P(None)), out_specs=(P("dp", None), cache_spec, cache_spec), check_vma=False)
```
